32 devices in a mesh: dp: 8 (over z, y), fsdp: 4 (over x, core).
Axes of the slice: x: 2, y: 2, z: 4, core: 2. Of those that a mesh axis runs over, the one named last changes fastest.
Arguments:
- hidden_in: bfloat16 [2, 32, 256, 768], P(None, ('dp', 'fsdp')), may hold values from -6 to 6
- patches: bfloat16 [2, 32, 2048, 768], P(None, ('dp', 'fsdp')), may hold values from -6 to 6
- token_segments: int32 [2, 32, 256], P(None, ('dp', 'fsdp')), may hold values from 0 to 3, as said below
- patch_segments: int32 [2, 32, 2048], P(None, ('dp', 'fsdp')), may hold values from 0 to 3, as said below
- cotangent: bfloat16 [2, 32, 256, 768], P(None, ('dp', 'fsdp')), may hold values from -6 to 6
- attention_weights: float32 [8, 768, 768], P(None, 'fsdp', 'dp'), may hold values from -1.1547005 to 1.1547005
- attention_means: float32 [8, 768, 768], P(None, 'fsdp', 'dp'), may hold values from -40 to 40
- attention_squares: float32 [8, 768, 768], P(None, 'fsdp', 'dp'), may hold values from 131.072 to 1638.4
- inner_weights: float32 [2, 768, 2048], P(None, 'fsdp', 'dp'), may hold values from -0.21875 to 0.21875
- inner_means: float32 [2, 768, 2048], P(None, 'fsdp', 'dp'), may hold values from -40 to 40
- inner_squares: float32 [2, 768, 2048], P(None, 'fsdp', 'dp'), may hold values from 131.072 to 1638.4
- outer_weights: float32 [2048, 768], P('fsdp', 'dp'), may hold values from -0.125 to 0.125
- outer_means: float32 [2048, 768], P('fsdp', 'dp'), may hold values from -48 to 48
- outer_squares: float32 [2048, 768], P('fsdp', 'dp'), may hold values from 163.84 to 2457.6
- norm_gains: float32 [3, 768], P(None, 'fsdp'), may hold values from 0.25 to 1.75
- gain_means: float32 [3, 768], P(None, 'fsdp'), may hold values from -80 to 80
- gain_squares: float32 [3, 768], P(None, 'fsdp'), may hold values from 425.984 to 6881.28
Outputs:
- hidden_out: bfloat16 [2, 32, 256, 768], P(None, ('dp', 'fsdp'))
- hidden_grad: float32 [2, 32, 256, 768], P(None, ('dp', 'fsdp'))
- patch_grad: float32 [2, 32, 2048, 768], P(None, ('dp', 'fsdp'))
- attention_mean: float32 [8, 768, 768], P(None, 'fsdp', 'dp')
- attention_square: float32 [8, 768, 768], P(None, 'fsdp', 'dp')
- attention_master: float32 [8, 768, 768], P(None, 'fsdp', 'dp')
- attention_copy: bfloat16 [8, 768, 768], P(None, 'fsdp', 'dp')
- inner_mean: float32 [2, 768, 2048], P(None, 'fsdp', 'dp')
- inner_square: float32 [2, 768, 2048], P(None, 'fsdp', 'dp')
- inner_master: float32 [2, 768, 2048], P(None, 'fsdp', 'dp')
- inner_copy: bfloat16 [2, 768, 2048], P(None, 'fsdp', 'dp')
- outer_mean: float32 [2048, 768], P('fsdp', 'dp')
- outer_square: float32 [2048, 768], P('fsdp', 'dp')
- outer_master: float32 [2048, 768], P('fsdp', 'dp')
- outer_copy: bfloat16 [2048, 768], P('fsdp', 'dp')
- gain_mean: float32 [3, 768], P(None, 'fsdp')
- gain_square: float32 [3, 768], P(None, 'fsdp')
- gain_master: float32 [3, 768], P(None, 'fsdp')
- gain_copy: bfloat16 [3, 768], P(None, 'fsdp')
The draws below stay inside these ranges and needn't reach their ends.
Inputs may be any that keep to these rules, and one draw needn't show every extreme that they name: `token_segments`: along each row the ids never fall from one token to the next, and each of the 4 ids holds one token or more. `patch_segments`: along each row the ids never fall from one patch to the next, and each of the 4 ids holds one patch or more.
All inputs are finite; a program needn't handle non-finite values.
Results may differ from the reference program's by a relative error of at most 0.02.
The reference program's roundings to bfloat16 on the way count: a program that leaves them out, or rounds other values in their place, can miss the bound.
Values may be sent and summed in bfloat16 or wider, within the bound.
A program may use at most 320 MiB of HBM per device.

```python
import math
from functools import partial
import jax
import jax.numpy as jnp
from jax import lax

D = 768
HEADS = 12
HEAD = 64
FF = 2048
ROW = 256
PATCH = 2048
MB = 2
SEGS = 4
STEP = 10
ROWS = 32
TOKENS = 16384


def cut_row(row_key, length):
    boundary = jax.random.permutation(row_key, length - 1)[:SEGS - 1].astype(jnp.int32) + 1
    positions = jnp.arange(length, dtype=jnp.int32)
    return jnp.sum((positions[:, None] >= boundary[None, :]).astype(jnp.int32), axis=1).astype(jnp.int32)


def draw_token_segments(key, part):
    row_keys = jax.random.split(jax.random.fold_in(key, 11), MB * ROWS)
    drawn = jax.vmap(partial(cut_row, length=ROW))(row_keys)
    return drawn.reshape(MB, ROWS, ROW)


def draw_patch_segments(key, part):
    row_keys = jax.random.split(jax.random.fold_in(key, 23), MB * ROWS)
    drawn = jax.vmap(partial(cut_row, length=PATCH))(row_keys)
    return drawn.reshape(MB, ROWS, PATCH)


def draw_attention_weights(key, part):
    factors = jnp.array([1.4, 1.4, 1.0, 4.0, 1.4, 1.4, 1.0, 8.0], jnp.float32)[:, None, None]
    raw_values = jnp.clip(jax.random.normal(key, (8, D, D), jnp.float32), -4.0, 4.0)
    return raw_values * factors / math.sqrt(D)


def block_scale(stream_key, dims, shards, least, top_value):
    level, own = 1.0, jax.random.fold_in(stream_key, 6)
    for axis_at, parts in shards:
        draws = jnp.exp(jax.random.uniform(jax.random.fold_in(own, axis_at), (parts,), jnp.float32, least / len(shards), top_value / len(shards)))
        level = level * jnp.repeat(draws, dims[axis_at] // parts).reshape([-1 if axis == axis_at else 1 for axis in range(len(dims))])
    return level


def normal_values(key, dims, deviation, most, cuts=(), held_as=jnp.bfloat16):
    loudness = block_scale(key, dims, cuts, -0.22, 0.18) if cuts else 1.0
    values = jax.random.normal(key, dims, jnp.float32) * deviation * loudness
    return jnp.minimum(jnp.maximum(values, -most), most).astype(held_as)


def setup_inputs(seed: int = 0) -> dict:
    splits = jax.random.split(jax.random.key(seed), 18)
    hidden_in = normal_values(splits[0], (MB, ROWS, ROW, D), 1.0, 6.0, ((1, 32),))
    patches = normal_values(splits[1], (MB, ROWS, PATCH, D), 1.0, 6.0, ((1, 32),))
    token_segments = draw_token_segments(jax.random.fold_in(splits[17], 71), 0)
    patch_segments = draw_patch_segments(jax.random.fold_in(splits[17], 71), 0)
    cotangent = normal_values(splits[4], (MB, ROWS, ROW, D), 1.0, 6.0, ((1, 32),))
    attention_weights = draw_attention_weights(jax.random.fold_in(splits[17], 71), 0)
    attention_means = normal_values(splits[6], (8, D, D), (0.055 * TOKENS ** 0.5), 40.0, ((1, 4), (2, 8)), jnp.float32)
    attention_squares = jnp.clip(jnp.exp(math.log(1638.4) - 2.5257286 * jax.random.uniform(splits[7], (8, D, D), jnp.float32) ** block_scale(splits[7], (8, D, D), ((1, 4), (2, 8)), -0.2, 0.2)), 131.072, 1638.4)
    inner_weights = normal_values(splits[8], (2, D, FF), D ** -0.5, 0.21875, ((1, 4), (2, 8)), jnp.float32)
    inner_means = normal_values(splits[9], (2, D, FF), (0.055 * TOKENS ** 0.5), 40.0, ((1, 4), (2, 8)), jnp.float32)
    inner_squares = jnp.clip(jnp.exp(math.log(1638.4) - 2.5257286 * jax.random.uniform(splits[10], (2, D, FF), jnp.float32) ** block_scale(splits[10], (2, D, FF), ((1, 4), (2, 8)), -0.2, 0.2)), 131.072, 1638.4)
    outer_weights = normal_values(splits[11], (FF, D), FF ** -0.5, 0.125, ((0, 4), (1, 8)), jnp.float32)
    outer_means = normal_values(splits[12], (FF, D), (0.067 * TOKENS ** 0.5), 48.0, ((0, 4), (1, 8)), jnp.float32)
    outer_squares = jnp.clip(jnp.exp(math.log(2457.6) - 2.7080503 * jax.random.uniform(splits[13], (FF, D), jnp.float32) ** block_scale(splits[13], (FF, D), ((0, 4), (1, 8)), -0.2, 0.2)), 163.84, 2457.6)
    norm_gains = jnp.clip(1.0 + 0.15 * jax.random.normal(splits[14], (3, D), jnp.float32), 0.25, 1.75)
    gain_means = normal_values(splits[15], (3, D), (0.11 * TOKENS ** 0.5), 80.0, ((1, 4),), jnp.float32)
    gain_squares = jnp.clip(jnp.exp(math.log(6881.28) - 2.7821581 * jax.random.uniform(splits[16], (3, D), jnp.float32) ** block_scale(splits[16], (3, D), ((1, 4),), -0.2, 0.2)), 425.984, 6881.28)
    return dict(hidden_in=hidden_in, patches=patches, token_segments=token_segments, patch_segments=patch_segments, cotangent=cotangent, attention_weights=attention_weights, attention_means=attention_means, attention_squares=attention_squares, inner_weights=inner_weights, inner_means=inner_means, inner_squares=inner_squares, outer_weights=outer_weights, outer_means=outer_means, outer_squares=outer_squares, norm_gains=norm_gains, gain_means=gain_means, gain_squares=gain_squares)


@jax.custom_vjp
def low(v):
    return lax.optimization_barrier(v.astype(jnp.bfloat16)).astype(jnp.float32)

@jax.custom_vjp
def low_back(v):
    return v

def low_keep(v):
    return (low(v), None)

def low_pass(kept, grad):
    return (grad,)

def back_keep(v):
    return (v, None)

def back_low(kept, grad):
    return (low(grad),)
low.defvjp(low_keep, low_pass)
low_back.defvjp(back_keep, back_low)
epsilon = 1e-06
score_scale = 0.125
masked_value = -1000000000.0
beta_one = 0.9
beta_two = 0.95
adam_epsilon = 1e-08
decay_matrix = 0.1
rate_matrix = 0.1
rate_gain = 0.3
highest = lax.Precision.HIGHEST

def gelu_tanh(values):
    return 0.5 * values * (1.0 + jnp.tanh(0.7978845608028654 * (values + 0.044715 * values * values * values)))

def norm_rows(values, gain):
    inverse_rms = lax.rsqrt(lax.optimization_barrier(jnp.mean(values * values, axis=-1, keepdims=True)) + epsilon)
    return values * inverse_rms * gain

def softmax_rows(scores):
    row_maximum = lax.optimization_barrier(jnp.max(scores, axis=-1, keepdims=True))
    raised = jnp.exp(scores - row_maximum)
    return raised / lax.optimization_barrier(jnp.sum(raised, axis=-1, keepdims=True))

def attend(queries, key_heads, value_heads, allowed):
    scores = low_back(score_scale * jnp.einsum('qhe,khe->hqk', queries, key_heads, precision=highest))
    probabilities = low(softmax_rows(jnp.where(allowed[None], scores, masked_value)))
    mixture = jnp.einsum('hqk,khe->qhe', probabilities, value_heads, precision=highest)
    return low(low_back(mixture))

def layer_row(weights, hidden, patch_rows, token_ids, patch_ids):
    attention, inner_matrix, outer_matrix, gain_rows = weights
    length = hidden.shape[0]
    patch_count = patch_rows.shape[0]
    normed_one = low(norm_rows(hidden, gain_rows[0]))
    projected = low(low_back(jnp.einsum('nd,kde->kne', normed_one, attention[0:3], precision=highest)))
    heads_in = projected.reshape(3, length, HEADS, HEAD)
    places = jnp.arange(length)
    causal = (places[:, None] >= places[None, :]) & (token_ids[:, None] == token_ids[None, :])
    mixture_one = attend(heads_in[0], heads_in[1], heads_in[2], causal).reshape(length, D)
    after_one = hidden + low_back(jnp.dot(mixture_one, attention[3], precision=highest))
    normed_two = low(norm_rows(after_one, gain_rows[1]))
    cross_query = low(low_back(jnp.dot(normed_two, attention[4], precision=highest))).reshape(length, HEADS, HEAD)
    cross_pair = low(low_back(jnp.einsum('pd,kde->kpe', patch_rows, attention[5:7], precision=highest)))
    cross_pair = cross_pair.reshape(2, patch_count, HEADS, HEAD)
    matching = token_ids[:, None] == patch_ids[None, :]
    mixture_two = attend(cross_query, cross_pair[0], cross_pair[1], matching).reshape(length, D)
    after_two = after_one + low_back(jnp.dot(mixture_two, attention[7], precision=highest))
    normed_three = low(norm_rows(after_two, gain_rows[2]))
    gated = low_back(jnp.einsum('nd,kdf->knf', normed_three, inner_matrix, precision=highest))
    units = low(gelu_tanh(gated[0]) * gated[1])
    return after_two + low_back(jnp.dot(units, outer_matrix, precision=highest))

def adam_update(weight, mean_old, square_old, gradient, step_rate, decay_rate):
    mean_new = beta_one * mean_old + (1.0 - beta_one) * gradient
    square_new = beta_two * square_old + (1.0 - beta_two) * gradient * gradient
    corrected = mean_new / (1.0 - beta_one ** STEP) / (jnp.sqrt(square_new / (1.0 - beta_two ** STEP)) + adam_epsilon)
    master = weight - step_rate * (corrected + decay_rate * weight)
    return (mean_new, square_new, master, master.astype(jnp.bfloat16))

def reference(hidden_in, patches, token_segments, patch_segments, cotangent, attention_weights, attention_means, attention_squares, inner_weights, inner_means, inner_squares, outer_weights, outer_means, outer_squares, norm_gains, gain_means, gain_squares):
    count = MB * ROWS
    hidden_flat = hidden_in.astype(jnp.float32).reshape(count, ROW, D)
    patch_flat = patches.astype(jnp.float32).reshape(count, PATCH, D)
    token_flat = token_segments.reshape(count, ROW)
    patch_id_flat = patch_segments.reshape(count, PATCH)

    def forward(params, hidden_all, patch_all):
        rounded = (low(params[0]), low(params[1]), low(params[2]), low(params[3]))

        def one_row(items):
            return layer_row(rounded, items[0], items[1], items[2], items[3])
        return lax.map(jax.checkpoint(one_row), (hidden_all, patch_all, token_flat, patch_id_flat))
    params = (attention_weights, inner_weights, outer_weights, norm_gains)
    output, pullback = jax.vjp(forward, params, hidden_flat, patch_flat)
    gradients, hidden_grad, patch_grad = pullback(cotangent.astype(jnp.float32).reshape(count, ROW, D))
    attention_new = adam_update(attention_weights, attention_means, attention_squares, gradients[0], rate_matrix, decay_matrix)
    inner_new = adam_update(inner_weights, inner_means, inner_squares, gradients[1], rate_matrix, decay_matrix)
    outer_new = adam_update(outer_weights, outer_means, outer_squares, gradients[2], rate_matrix, decay_matrix)
    gain_new = adam_update(norm_gains, gain_means, gain_squares, gradients[3], rate_gain, 0.0)
    return (output.reshape(MB, ROWS, ROW, D).astype(jnp.bfloat16), hidden_grad.reshape(MB, ROWS, ROW, D), patch_grad.reshape(MB, ROWS, PATCH, D), attention_new[0], attention_new[1], attention_new[2], attention_new[3], inner_new[0], inner_new[1], inner_new[2], inner_new[3], outer_new[0], outer_new[1], outer_new[2], outer_new[3], gain_new[0], gain_new[1], gain_new[2], gain_new[3])
```

```python
import functools

import jax
import jax.numpy as jnp
from jax import lax
from jax.experimental import pallas as pl
from jax.experimental.pallas import tpu as pltpu
from jax.sharding import PartitionSpec as P

D = 768
HEADS = 12
HEAD = 64
PAIR = 2 * HEAD
PAIRS = HEADS // 2
STEP = 10
SEGS = 4

epsilon = 1e-06
score_scale = 0.125
masked_value = -1000000000.0
beta_one = 0.9
beta_two = 0.95
adam_epsilon = 1e-08
decay_matrix = 0.1
rate_matrix = 0.1
rate_gain = 0.3
f32 = jnp.float32
bf16 = jnp.bfloat16
BOTH = ("dp", "fsdp")


def gelu_tanh(values):
    return (
        0.5
        * values
        * (1.0 + jnp.tanh(0.7978845608028654 * (values + 0.044715 * values * values * values)))
    )


def dot_nn(a, b):
    return lax.dot_general(a, b, (((1,), (0,)), ((), ())), preferred_element_type=f32)


def dot_nt(a, b):
    return lax.dot_general(a, b, (((1,), (1,)), ((), ())), preferred_element_type=f32)


def dot_tn(a, b):
    return lax.dot_general(a, b, (((0,), (0,)), ((), ())), preferred_element_type=f32)


def norm_forward(values, gain):
    inverse_rms = lax.rsqrt(jnp.mean(values * values, axis=-1, keepdims=True) + epsilon)
    unit_rows = values * inverse_rms
    return ((unit_rows * gain.astype(f32)).astype(bf16), unit_rows, inverse_rms)


def norm_backward(grad_rows, gain, unit_rows, inverse_rms):
    grad_unit = grad_rows * gain.astype(f32)
    grad_values = inverse_rms * (
        grad_unit - unit_rows * jnp.mean(grad_unit * unit_rows, axis=-1, keepdims=True)
    )
    return (grad_values, jnp.sum(grad_rows * unit_rows, axis=0))


def head_half(block, half):
    lane = lax.broadcasted_iota(jnp.int32, block.shape, 1)
    keep = (lane < HEAD) if half == 0 else (lane >= HEAD)
    return jnp.where(keep, block, jnp.zeros_like(block))


def three_parts(column):
    high = column.astype(bf16).astype(f32)
    rest = column - high
    middle = rest.astype(bf16).astype(f32)
    low = rest - middle
    return high, middle, low


def stat_lanes(base, column, first):
    lane = lax.broadcasted_iota(jnp.int32, base.shape, 1)
    for place, part in enumerate(three_parts(column)):
        base = jnp.where(lane == first + place, -part, base)
    return base


def key_marks(key_ids, stats):
    lane = lax.broadcasted_iota(jnp.int32, (key_ids.shape[0], 128), 1)
    marks = lane == key_ids
    if stats:
        marks = marks | ((lane >= SEGS) & (lane < SEGS + 3))
    return jnp.where(marks, 1.0, 0.0).astype(bf16)


def query_bias(query_ids):
    lane = lax.broadcasted_iota(jnp.int32, (query_ids.shape[0], 128), 1)
    return jnp.where((lane == query_ids) | (lane >= SEGS), 0.0, masked_value)


def softmax_columns(scores):
    top = jnp.max(scores, axis=0, keepdims=True)
    raised = jnp.exp(scores - top)
    return raised, top, jnp.sum(raised, axis=0, keepdims=True)


def finish_forward(halves, tops, sums, o_ref, lse_ref):
    mixed = jnp.concatenate([h / s for h, s in zip(halves, sums)], axis=0)
    o_ref[0] = mixed.T.astype(bf16)
    rows = [t + jnp.log(s) for t, s in zip(tops, sums)]
    pad = jnp.zeros((6, rows[0].shape[1]), f32)
    lse_ref[0, 0] = jnp.concatenate(rows + [pad], axis=0)


def cross_forward_kernel(q_ref, k_ref, v_ref, qid_ref, kid_ref, o_ref, lse_ref):
    marked = jnp.concatenate([k_ref[0], key_marks(kid_ref[0], False)], axis=1)
    bias = query_bias(qid_ref[0]).astype(bf16)
    query = q_ref[0] * jnp.asarray(score_scale, bf16)
    values = v_ref[0].T
    halves, tops, sums = [], [], []
    for half in range(2):
        extended = jnp.concatenate([head_half(query, half), bias], axis=1)
        raised, top, total = softmax_columns(dot_nt(marked, extended))
        halves.append(dot_nn(values[half * HEAD : (half + 1) * HEAD], raised.astype(bf16)))
        tops.append(top)
        sums.append(total)
    finish_forward(halves, tops, sums, o_ref, lse_ref)


def causal_mask(qid_ref, kid_ref):
    length = kid_ref.shape[1]
    key = lax.broadcasted_iota(jnp.int32, (length, length), 0)
    query = lax.broadcasted_iota(jnp.int32, (length, length), 1)
    return (key <= query) & (kid_ref[0] == qid_ref[0])


def self_forward_kernel(q_ref, k_ref, v_ref, qid_ref, kid_ref, o_ref, lse_ref):
    allowed = causal_mask(qid_ref, kid_ref)
    query = q_ref[0] * jnp.asarray(score_scale, bf16)
    key = k_ref[0]
    values = v_ref[0].T
    halves, tops, sums = [], [], []
    for half in range(2):
        scores = jnp.where(allowed, dot_nt(key, head_half(query, half)), masked_value)
        raised, top, total = softmax_columns(scores)
        halves.append(dot_nn(values[half * HEAD : (half + 1) * HEAD], raised.astype(bf16)))
        tops.append(top)
        sums.append(total)
    finish_forward(halves, tops, sums, o_ref, lse_ref)


def backward_pair(q_ref, k_ref, v_ref, o_ref, do_ref, lse_ref, marked, bias, allowed,
                  dq_ref, dk_ref, dv_ref):
    query, grad = q_ref[0], do_ref[0]
    scaled = query * jnp.asarray(score_scale, bf16)
    key_turned = k_ref[0].T
    length = query.shape[0]
    lse_columns = lse_ref[0, 0].T
    product = o_ref[0].astype(f32) * grad.astype(f32)
    ones = key_marks(jnp.full((v_ref.shape[1], 1), -1, jnp.int32), True)
    valued = jnp.concatenate([v_ref[0], ones], axis=1)
    probs, grads, turned = [], [], []
    for half in range(2):
        stats = stat_lanes(bias, lse_columns[:, half : half + 1], SEGS).astype(bf16)
        scores = dot_nt(marked, jnp.concatenate([head_half(scaled, half), stats], axis=1))
        if allowed is not None:
            scores = jnp.where(allowed, scores, masked_value)
        weight = jnp.exp(scores)
        inner = jnp.sum(head_half(product, half), axis=1, keepdims=True)
        delta = stat_lanes(jnp.zeros((length, 128), f32), inner, SEGS).astype(bf16)
        shifted = dot_nt(valued, jnp.concatenate([head_half(grad, half), delta], axis=1))
        grad_scores = (weight * shifted).astype(bf16)
        probs.append(weight.astype(bf16))
        grads.append(grad_scores)
        turned.append(dot_nn(key_turned[half * HEAD : (half + 1) * HEAD], grad_scores))
    dq_ref[0] = (score_scale * jnp.concatenate(turned, axis=0)).T.astype(bf16)
    dv_ref[0] = dot_nn(
        jnp.concatenate(probs, axis=1),
        jnp.concatenate([head_half(grad, 0), head_half(grad, 1)], axis=0),
    ).astype(bf16)
    dk_ref[0] = dot_nn(
        jnp.concatenate(grads, axis=1),
        jnp.concatenate([head_half(scaled, 0), head_half(scaled, 1)], axis=0),
    ).astype(bf16)


def cross_backward_kernel(q_ref, k_ref, v_ref, o_ref, do_ref, lse_ref, qid_ref, kid_ref,
                          dq_ref, dk_ref, dv_ref):
    marked = jnp.concatenate([k_ref[0], key_marks(kid_ref[0], True)], axis=1)
    backward_pair(q_ref, k_ref, v_ref, o_ref, do_ref, lse_ref, marked, query_bias(qid_ref[0]),
                  None, dq_ref, dk_ref, dv_ref)


def self_backward_kernel(q_ref, k_ref, v_ref, o_ref, do_ref, lse_ref, qid_ref, kid_ref,
                         dq_ref, dk_ref, dv_ref):
    length = k_ref.shape[1]
    ones = key_marks(jnp.full((length, 1), -1, jnp.int32), True)
    marked = jnp.concatenate([k_ref[0], ones], axis=1)
    backward_pair(q_ref, k_ref, v_ref, o_ref, do_ref, lse_ref, marked,
                  jnp.zeros((length, 128), f32), causal_mask(qid_ref, kid_ref),
                  dq_ref, dk_ref, dv_ref)


def pair_spec(length, offset):
    return pl.BlockSpec((1, length, PAIR), lambda row, pair: (row, 0, offset + pair))


def row_spec(shape):
    return pl.BlockSpec((1,) + shape, lambda row, pair: (row, 0, 0))


def stat_spec(length):
    return pl.BlockSpec((1, 1, 8, length), lambda row, pair: (row, pair, 0, 0))


def cost(rows, queries, keys, products):
    elements = rows * HEADS * queries * keys
    return pl.CostEstimate(
        flops=2 * elements * 256 * products // 2,
        transcendentals=elements,
        bytes_accessed=rows * (queries + keys) * D * 2 * 3,
    )


def attend_forward(kernel, queries, keys, offsets, query_ids, key_ids, query_shape):
    rows, length = queries.shape[:2]
    count = keys.shape[1]
    return pl.pallas_call(
        kernel,
        grid=(rows, PAIRS),
        in_specs=[
            pair_spec(length, 0),
            pair_spec(count, offsets[0]),
            pair_spec(count, offsets[1]),
            row_spec(query_shape),
            row_spec((count, 1)),
        ],
        out_specs=[pair_spec(length, 0), stat_spec(length)],
        out_shape=[
            jax.ShapeDtypeStruct((rows, length, D), bf16),
            jax.ShapeDtypeStruct((rows, PAIRS, 8, length), f32),
        ],
        cost_estimate=cost(rows, length, count, 2),
    )(queries, keys, keys, query_ids, key_ids)


def attend_backward(kernel, queries, keys, offsets, mixed, grad, lse, query_ids, key_ids,
                    query_shape):
    rows, length = grad.shape[:2]
    count = keys.shape[1]
    return pl.pallas_call(
        kernel,
        grid=(rows, PAIRS),
        in_specs=[
            pair_spec(length, 0),
            pair_spec(count, offsets[0]),
            pair_spec(count, offsets[1]),
            pair_spec(length, 0),
            pair_spec(length, 0),
            stat_spec(length),
            row_spec(query_shape),
            row_spec((count, 1)),
        ],
        out_specs=[pair_spec(length, 0), pair_spec(count, 0), pair_spec(count, 0)],
        out_shape=[
            jax.ShapeDtypeStruct((rows, length, D), bf16),
            jax.ShapeDtypeStruct((rows, count, D), bf16),
            jax.ShapeDtypeStruct((rows, count, D), bf16),
        ],
        cost_estimate=cost(rows, length, count, 5),
    )(queries, keys, keys, mixed, grad, lse, query_ids, key_ids)


def gather_weights(attention, inner, outer):
    turned = lax.all_gather(jnp.swapaxes(attention, 1, 2), BOTH, axis=0, tiled=False)
    heads = lax.axis_size("dp"), lax.axis_size("fsdp")
    turned = turned.reshape(heads + turned.shape[1:])
    full_attention = jnp.transpose(turned, (2, 0, 3, 1, 4)).reshape(8, D, D)
    wide = lax.all_gather(inner, BOTH, axis=0, tiled=False)
    wide = wide.reshape(heads + wide.shape[1:])
    full_inner = jnp.transpose(wide, (2, 1, 3, 0, 4)).reshape(2, D, -1)
    tall = lax.all_gather(outer.T, BOTH, axis=0, tiled=False)
    tall = tall.reshape(heads + tall.shape[1:])
    full_outer = jnp.transpose(tall, (0, 2, 1, 3)).reshape(D, -1)
    return full_attention, full_inner, full_outer


def scatter_grads(attention, inner, outer):
    across, within = lax.axis_size("dp"), lax.axis_size("fsdp")
    blocks = attention.reshape(8, across, D // across, within, D // within)
    blocks = jnp.transpose(blocks, (1, 3, 0, 2, 4))
    blocks = blocks.reshape((across * within,) + blocks.shape[2:])
    own_attention = lax.psum_scatter(blocks, BOTH, scatter_dimension=0, tiled=False)
    blocks = inner.reshape(2, within, D // within, across, inner.shape[2] // across)
    blocks = jnp.transpose(blocks, (3, 1, 0, 2, 4))
    blocks = blocks.reshape((across * within,) + blocks.shape[2:])
    own_inner = lax.psum_scatter(blocks, BOTH, scatter_dimension=0, tiled=False)
    blocks = outer.reshape(across, D // across, within, outer.shape[1] // within)
    blocks = jnp.transpose(blocks, (0, 2, 1, 3))
    blocks = blocks.reshape((across * within,) + blocks.shape[2:])
    own_outer = lax.psum_scatter(blocks, BOTH, scatter_dimension=0, tiled=False)
    return (
        jnp.swapaxes(own_attention, 1, 2).astype(f32),
        own_inner.astype(f32),
        own_outer.T.astype(f32),
    )


def adam_update(weight, mean_old, square_old, gradient, step_rate, decay_rate):
    mean_new = beta_one * mean_old + (1.0 - beta_one) * gradient
    square_new = beta_two * square_old + (1.0 - beta_two) * gradient * gradient
    corrected = (
        mean_new
        / (1.0 - beta_one**STEP)
        / (jnp.sqrt(square_new / (1.0 - beta_two**STEP)) + adam_epsilon)
    )
    master = weight - step_rate * (corrected + decay_rate * weight)
    return (mean_new, square_new, master, master.astype(bf16))


def on_device(
    hidden_in,
    patches,
    token_segments,
    patch_segments,
    cotangent,
    attention_weights,
    attention_means,
    attention_squares,
    inner_weights,
    inner_means,
    inner_squares,
    outer_weights,
    outer_means,
    outer_squares,
    norm_gains,
    gain_means,
    gain_squares,
):
    rows, _, length, _ = hidden_in.shape
    count = patches.shape[2]
    tokens = rows * length
    weights, inner, outer = gather_weights(
        attention_weights.astype(bf16), inner_weights.astype(bf16), outer_weights.astype(bf16)
    )
    gains = lax.all_gather(norm_gains.astype(bf16), "fsdp", axis=1, tiled=True)

    initial = hidden_in.reshape(tokens, D).astype(f32)
    patch_rows = patches.reshape(rows * count, D)
    token_rows = token_segments.reshape(rows, 1, length)
    token_columns = token_segments.reshape(rows, length, 1)
    patch_columns = patch_segments.reshape(rows, count, 1)

    normed_one, unit_one, rms_one = norm_forward(initial, gains[0])
    packed = dot_nt(normed_one, weights[0:3].reshape(3 * D, D)).astype(bf16)
    packed = packed.reshape(rows, length, 3 * D)
    mixture_one, lse_one = attend_forward(
        self_forward_kernel, packed, packed, (PAIRS, 2 * PAIRS), token_rows, token_columns,
        (1, length),
    )
    mixed_one = mixture_one.reshape(tokens, D)
    after_one = initial + dot_nt(mixed_one, weights[3])
    normed_two, unit_two, rms_two = norm_forward(after_one, gains[1])
    cross_query = dot_nt(normed_two, weights[4]).astype(bf16).reshape(rows, length, D)
    cross_pair = dot_nt(patch_rows, weights[5:7].reshape(2 * D, D)).astype(bf16)
    cross_pair = cross_pair.reshape(rows, count, 2 * D)
    mixture_two, lse_two = attend_forward(
        cross_forward_kernel, cross_query, cross_pair, (0, PAIRS), token_columns, patch_columns,
        (length, 1),
    )
    mixed_two = mixture_two.reshape(tokens, D)
    after_two = after_one + dot_nt(mixed_two, weights[7])
    normed_three, unit_three, rms_three = norm_forward(after_two, gains[2])
    gate = dot_nn(normed_three, inner[0])
    up = dot_nn(normed_three, inner[1])
    units = (gelu_tanh(gate) * up).astype(bf16)
    hidden_out = (after_two + dot_nt(units, outer)).astype(bf16)

    grad_low = cotangent.reshape(tokens, D)
    grad_final = grad_low.astype(f32)
    grad_outer = dot_tn(grad_low, units).astype(bf16)
    grad_units = dot_nn(grad_low, outer)
    activation, gelu_back = jax.vjp(gelu_tanh, gate)
    grad_gate = gelu_back(grad_units * up)[0].astype(bf16)
    grad_up = (grad_units * activation).astype(bf16)
    grad_inner = jnp.stack(
        [dot_tn(normed_three, grad_gate).astype(bf16), dot_tn(normed_three, grad_up).astype(bf16)]
    )
    grad_normed = dot_nt(grad_gate, inner[0]) + dot_nt(grad_up, inner[1])
    grad_from_three, gain_three = norm_backward(grad_normed, gains[2], unit_three, rms_three)
    grad_two = grad_final + grad_from_three
    branch_two = grad_two.astype(bf16)
    grad_mixture_two = dot_nn(branch_two, weights[7]).astype(bf16).reshape(rows, length, D)
    grad_cq, grad_ck, grad_cv = attend_backward(
        cross_backward_kernel, cross_query, cross_pair, (0, PAIRS), mixture_two,
        grad_mixture_two, lse_two, token_columns, patch_columns, (length, 1),
    )
    grad_cq = grad_cq.reshape(tokens, D)
    grad_ck = grad_ck.reshape(rows * count, D)
    grad_cv = grad_cv.reshape(rows * count, D)
    patch_grad = dot_nn(grad_ck, weights[5]) + dot_nn(grad_cv, weights[6])
    grad_from_two, gain_two = norm_backward(
        dot_nn(grad_cq, weights[4]), gains[1], unit_two, rms_two
    )
    grad_one = grad_two + grad_from_two
    branch_one = grad_one.astype(bf16)
    grad_mixture_one = dot_nn(branch_one, weights[3]).astype(bf16).reshape(rows, length, D)
    grad_q, grad_k, grad_v = attend_backward(
        self_backward_kernel, packed, packed, (PAIRS, 2 * PAIRS), mixture_one,
        grad_mixture_one, lse_one, token_rows, token_columns, (1, length),
    )
    grad_q = grad_q.reshape(tokens, D)
    grad_k = grad_k.reshape(tokens, D)
    grad_v = grad_v.reshape(tokens, D)
    grad_normed_one = (
        dot_nn(grad_q, weights[0]) + dot_nn(grad_k, weights[1]) + dot_nn(grad_v, weights[2])
    )
    grad_from_one, gain_one = norm_backward(grad_normed_one, gains[0], unit_one, rms_one)
    hidden_grad = grad_one + grad_from_one
    grad_attention = jnp.stack(
        [
            dot_tn(grad_q, normed_one).astype(bf16),
            dot_tn(grad_k, normed_one).astype(bf16),
            dot_tn(grad_v, normed_one).astype(bf16),
            dot_tn(branch_one, mixed_one).astype(bf16),
            dot_tn(grad_cq, normed_two).astype(bf16),
            dot_tn(grad_ck, patch_rows).astype(bf16),
            dot_tn(grad_cv, patch_rows).astype(bf16),
            dot_tn(branch_two, mixed_two).astype(bf16),
        ]
    )
    own_attention, own_inner, own_outer = scatter_grads(grad_attention, grad_inner, grad_outer)
    gain_totals = lax.psum(jnp.stack([gain_one, gain_two, gain_three]), BOTH)
    width = norm_gains.shape[1]
    own_gains = lax.dynamic_slice_in_dim(
        gain_totals, lax.axis_index("fsdp") * width, width, axis=1
    )

    attention_new = adam_update(
        attention_weights, attention_means, attention_squares, own_attention,
        rate_matrix, decay_matrix,
    )
    inner_new = adam_update(
        inner_weights, inner_means, inner_squares, own_inner, rate_matrix, decay_matrix
    )
    outer_new = adam_update(
        outer_weights, outer_means, outer_squares, own_outer, rate_matrix, decay_matrix
    )
    gain_new = adam_update(norm_gains, gain_means, gain_squares, own_gains, rate_gain, 0.0)
    return (
        hidden_out.reshape(hidden_in.shape),
        hidden_grad.reshape(hidden_in.shape),
        patch_grad.reshape(patches.shape),
        *attention_new,
        *inner_new,
        *outer_new,
        *gain_new,
    )


def solution(mesh):
    rows = P(None, BOTH, None, None)
    ids = P(None, BOTH, None)
    matrix = P(None, "fsdp", "dp")
    down = P("fsdp", "dp")
    gain = P(None, "fsdp")
    return jax.shard_map(
        on_device,
        mesh=mesh,
        in_specs=(rows, rows, ids, ids, rows) + (matrix,) * 6 + (down,) * 3 + (gain,) * 3,
        out_specs=(rows, rows, rows) + (matrix,) * 8 + (down,) * 4 + (gain,) * 4,
        check_vma=False,
    )
```

```python
import functools

import jax
import jax.numpy as jnp
from jax import lax
from jax.experimental import pallas as pl
from jax.experimental.pallas import tpu as pltpu
from jax.sharding import PartitionSpec as P

D = 768
HEADS = 12
HEAD = 64
PAIR = 2 * HEAD
PAIRS = HEADS // 2
STEP = 10
SEGS = 4

epsilon = 1e-06
score_scale = 0.125
masked_value = -1000000000.0
beta_one = 0.9
beta_two = 0.95
adam_epsilon = 1e-08
decay_matrix = 0.1
rate_matrix = 0.1
rate_gain = 0.3
f32 = jnp.float32
bf16 = jnp.bfloat16
BOTH = ("dp", "fsdp")


def gelu_tanh(values):
    return (
        0.5
        * values
        * (1.0 + jnp.tanh(0.7978845608028654 * (values + 0.044715 * values * values * values)))
    )


def dot_nn(a, b):
    return lax.dot_general(a, b, (((1,), (0,)), ((), ())), preferred_element_type=f32)


def dot_nt(a, b):
    return lax.dot_general(a, b, (((1,), (1,)), ((), ())), preferred_element_type=f32)


def dot_tn(a, b):
    return lax.dot_general(a, b, (((0,), (0,)), ((), ())), preferred_element_type=f32)


def norm_forward(values, gain):
    inverse_rms = lax.rsqrt(jnp.mean(values * values, axis=-1, keepdims=True) + epsilon)
    unit_rows = values * inverse_rms
    return ((unit_rows * gain.astype(f32)).astype(bf16), unit_rows, inverse_rms)


def norm_backward(grad_rows, gain, unit_rows, inverse_rms):
    grad_unit = grad_rows * gain.astype(f32)
    grad_values = inverse_rms * (
        grad_unit - unit_rows * jnp.mean(grad_unit * unit_rows, axis=-1, keepdims=True)
    )
    return (grad_values, jnp.sum(grad_rows * unit_rows, axis=0))


def head_half(block, half):
    lane = lax.broadcasted_iota(jnp.int32, block.shape, 1)
    keep = (lane < HEAD) if half == 0 else (lane >= HEAD)
    return jnp.where(keep, block, jnp.zeros_like(block))


def three_parts(column):
    high = column.astype(bf16).astype(f32)
    rest = column - high
    middle = rest.astype(bf16).astype(f32)
    low = rest - middle
    return high, middle, low


def stat_lanes(base, column, first):
    lane = lax.broadcasted_iota(jnp.int32, base.shape, 1)
    for place, part in enumerate(three_parts(column)):
        base = jnp.where(lane == first + place, -part, base)
    return base


def key_marks(key_ids, stats):
    lane = lax.broadcasted_iota(jnp.int32, (key_ids.shape[0], 128), 1)
    marks = lane == key_ids
    if stats:
        marks = marks | ((lane >= SEGS) & (lane < SEGS + 3))
    return jnp.where(marks, 1.0, 0.0).astype(bf16)


def query_bias(query_ids):
    lane = lax.broadcasted_iota(jnp.int32, (query_ids.shape[0], 128), 1)
    return jnp.where((lane == query_ids) | (lane >= SEGS), 0.0, masked_value)


def softmax_columns(scores):
    top = jnp.max(scores, axis=0, keepdims=True)
    raised = jnp.exp(scores - top)
    return raised, top, jnp.sum(raised, axis=0, keepdims=True)


def finish_forward(halves, tops, sums, o_ref, lse_ref):
    mixed = jnp.concatenate([h / s for h, s in zip(halves, sums)], axis=0)
    o_ref[0] = mixed.T.astype(bf16)
    rows = [t + jnp.log(s) for t, s in zip(tops, sums)]
    pad = jnp.zeros((6, rows[0].shape[1]), f32)
    lse_ref[0, 0] = jnp.concatenate(rows + [pad], axis=0)


def cross_forward_kernel(q_ref, k_ref, v_ref, qid_ref, kid_ref, o_ref, lse_ref):
    marked = jnp.concatenate([k_ref[0], key_marks(kid_ref[0], False)], axis=1)
    bias = query_bias(qid_ref[0]).astype(bf16)
    query = q_ref[0] * jnp.asarray(score_scale, bf16)
    values = v_ref[0].T
    halves, tops, sums = [], [], []
    for half in range(2):
        extended = jnp.concatenate([head_half(query, half), bias], axis=1)
        raised, top, total = softmax_columns(dot_nt(marked, extended))
        halves.append(dot_nn(values[half * HEAD : (half + 1) * HEAD], raised.astype(bf16)))
        tops.append(top)
        sums.append(total)
    finish_forward(halves, tops, sums, o_ref, lse_ref)


def causal_mask(qid_ref, kid_ref):
    length = kid_ref.shape[1]
    key = lax.broadcasted_iota(jnp.int32, (length, length), 0)
    query = lax.broadcasted_iota(jnp.int32, (length, length), 1)
    return (key <= query) & (kid_ref[0] == qid_ref[0])


def self_forward_kernel(q_ref, k_ref, v_ref, qid_ref, kid_ref, o_ref, lse_ref):
    allowed = causal_mask(qid_ref, kid_ref)
    query = q_ref[0] * jnp.asarray(score_scale, bf16)
    key = k_ref[0]
    values = v_ref[0].T
    halves, tops, sums = [], [], []
    for half in range(2):
        scores = jnp.where(allowed, dot_nt(key, head_half(query, half)), masked_value)
        raised, top, total = softmax_columns(scores)
        halves.append(dot_nn(values[half * HEAD : (half + 1) * HEAD], raised.astype(bf16)))
        tops.append(top)
        sums.append(total)
    finish_forward(halves, tops, sums, o_ref, lse_ref)


def backward_pair(q_ref, k_ref, v_ref, o_ref, do_ref, lse_ref, marked, bias, allowed,
                  dq_ref, dk_ref, dv_ref):
    query, grad = q_ref[0], do_ref[0]
    scaled = query * jnp.asarray(score_scale, bf16)
    key_turned = k_ref[0].T
    length = query.shape[0]
    lse_columns = lse_ref[0, 0].T
    product = o_ref[0].astype(f32) * grad.astype(f32)
    ones = key_marks(jnp.full((v_ref.shape[1], 1), -1, jnp.int32), True)
    valued = jnp.concatenate([v_ref[0], ones], axis=1)
    probs, grads, turned = [], [], []
    for half in range(2):
        stats = stat_lanes(bias, lse_columns[:, half : half + 1], SEGS).astype(bf16)
        scores = dot_nt(marked, jnp.concatenate([head_half(scaled, half), stats], axis=1))
        if allowed is not None:
            scores = jnp.where(allowed, scores, masked_value)
        weight = jnp.exp(scores)
        inner = jnp.sum(head_half(product, half), axis=1, keepdims=True)
        delta = stat_lanes(jnp.zeros((length, 128), f32), inner, SEGS).astype(bf16)
        shifted = dot_nt(valued, jnp.concatenate([head_half(grad, half), delta], axis=1))
        grad_scores = (weight * shifted).astype(bf16)
        probs.append(weight.astype(bf16))
        grads.append(grad_scores)
        turned.append(dot_nn(key_turned[half * HEAD : (half + 1) * HEAD], grad_scores))
    dq_ref[0] = (score_scale * jnp.concatenate(turned, axis=0)).T.astype(bf16)
    dv_ref[0] = dot_nn(
        jnp.concatenate(probs, axis=1),
        jnp.concatenate([head_half(grad, 0), head_half(grad, 1)], axis=0),
    ).astype(bf16)
    dk_ref[0] = dot_nn(
        jnp.concatenate(grads, axis=1),
        jnp.concatenate([head_half(scaled, 0), head_half(scaled, 1)], axis=0),
    ).astype(bf16)


def cross_backward_kernel(q_ref, k_ref, v_ref, o_ref, do_ref, lse_ref, qid_ref, kid_ref,
                          dq_ref, dk_ref, dv_ref):
    marked = jnp.concatenate([k_ref[0], key_marks(kid_ref[0], True)], axis=1)
    backward_pair(q_ref, k_ref, v_ref, o_ref, do_ref, lse_ref, marked, query_bias(qid_ref[0]),
                  None, dq_ref, dk_ref, dv_ref)


def self_backward_kernel(q_ref, k_ref, v_ref, o_ref, do_ref, lse_ref, qid_ref, kid_ref,
                         dq_ref, dk_ref, dv_ref):
    length = k_ref.shape[1]
    ones = key_marks(jnp.full((length, 1), -1, jnp.int32), True)
    marked = jnp.concatenate([k_ref[0], ones], axis=1)
    backward_pair(q_ref, k_ref, v_ref, o_ref, do_ref, lse_ref, marked,
                  jnp.zeros((length, 128), f32), causal_mask(qid_ref, kid_ref),
                  dq_ref, dk_ref, dv_ref)


def pair_spec(length, offset):
    return pl.BlockSpec((1, length, PAIR), lambda row, pair: (row, 0, offset + pair))


def row_spec(shape):
    return pl.BlockSpec((1,) + shape, lambda row, pair: (row, 0, 0))


def stat_spec(length):
    return pl.BlockSpec((1, 1, 8, length), lambda row, pair: (row, pair, 0, 0))


def cost(rows, queries, keys, products):
    elements = rows * HEADS * queries * keys
    return pl.CostEstimate(
        flops=2 * elements * 256 * products // 2,
        transcendentals=elements,
        bytes_accessed=rows * (queries + keys) * D * 2 * 3,
    )


def attend_forward(kernel, queries, keys, offsets, query_ids, key_ids, query_shape):
    rows, length = queries.shape[:2]
    count = keys.shape[1]
    return pl.pallas_call(
        kernel,
        grid=(rows, PAIRS),
        in_specs=[
            pair_spec(length, 0),
            pair_spec(count, offsets[0]),
            pair_spec(count, offsets[1]),
            row_spec(query_shape),
            row_spec((count, 1)),
        ],
        out_specs=[pair_spec(length, 0), stat_spec(length)],
        out_shape=[
            jax.ShapeDtypeStruct((rows, length, D), bf16),
            jax.ShapeDtypeStruct((rows, PAIRS, 8, length), f32),
        ],
        cost_estimate=cost(rows, length, count, 2),
    )(queries, keys, keys, query_ids, key_ids)


def attend_backward(kernel, queries, keys, offsets, mixed, grad, lse, query_ids, key_ids,
                    query_shape):
    rows, length = grad.shape[:2]
    count = keys.shape[1]
    return pl.pallas_call(
        kernel,
        grid=(rows, PAIRS),
        in_specs=[
            pair_spec(length, 0),
            pair_spec(count, offsets[0]),
            pair_spec(count, offsets[1]),
            pair_spec(length, 0),
            pair_spec(length, 0),
            stat_spec(length),
            row_spec(query_shape),
            row_spec((count, 1)),
        ],
        out_specs=[pair_spec(length, 0), pair_spec(count, 0), pair_spec(count, 0)],
        out_shape=[
            jax.ShapeDtypeStruct((rows, length, D), bf16),
            jax.ShapeDtypeStruct((rows, count, D), bf16),
            jax.ShapeDtypeStruct((rows, count, D), bf16),
        ],
        cost_estimate=cost(rows, length, count, 5),
    )(queries, keys, keys, mixed, grad, lse, query_ids, key_ids)


def gather_weights(attention, inner, outer):
    turned = lax.all_gather(jnp.swapaxes(attention, 1, 2), BOTH, axis=0, tiled=False)
    heads = lax.axis_size("dp"), lax.axis_size("fsdp")
    turned = turned.reshape(heads + turned.shape[1:])
    full_attention = jnp.transpose(turned, (2, 0, 3, 1, 4)).reshape(8, D, D)
    wide = lax.all_gather(inner, BOTH, axis=0, tiled=False)
    wide = wide.reshape(heads + wide.shape[1:])
    full_inner = jnp.transpose(wide, (2, 1, 3, 0, 4)).reshape(2, D, -1)
    tall = lax.all_gather(outer.T, BOTH, axis=0, tiled=False)
    tall = tall.reshape(heads + tall.shape[1:])
    full_outer = jnp.transpose(tall, (0, 2, 1, 3)).reshape(D, -1)
    return full_attention, full_inner, full_outer


def scatter_grads(attention, inner, outer):
    across, within = lax.axis_size("dp"), lax.axis_size("fsdp")
    blocks = attention.reshape(8, across, D // across, within, D // within)
    blocks = jnp.transpose(blocks, (1, 3, 0, 2, 4))
    blocks = blocks.reshape((across * within,) + blocks.shape[2:])
    own_attention = lax.psum_scatter(blocks, BOTH, scatter_dimension=0, tiled=False)
    blocks = inner.reshape(2, within, D // within, across, inner.shape[2] // across)
    blocks = jnp.transpose(blocks, (3, 1, 0, 2, 4))
    blocks = blocks.reshape((across * within,) + blocks.shape[2:])
    own_inner = lax.psum_scatter(blocks, BOTH, scatter_dimension=0, tiled=False)
    blocks = outer.reshape(across, D // across, within, outer.shape[1] // within)
    blocks = jnp.transpose(blocks, (0, 2, 1, 3))
    blocks = blocks.reshape((across * within,) + blocks.shape[2:])
    own_outer = lax.psum_scatter(blocks, BOTH, scatter_dimension=0, tiled=False)
    return (
        jnp.swapaxes(own_attention, 1, 2).astype(f32),
        own_inner.astype(f32),
        own_outer.T.astype(f32),
    )


MESH = pl.DeviceIdType.MESH
PIECES = 3


def where_am_i():
    across, within = lax.axis_index("dp"), lax.axis_index("fsdp")
    return across // 2, across % 2, within // 2, within % 2


def device_at(z, y, x, core):
    return (2 * z + y, 2 * x + core)


def aligned(value, unit):
    return pl.multiple_of(value * unit, unit)


def block_of(refs, widths, z, y, x, half):
    attention, inner, outer = refs
    down, side, deep = widths
    place = 2 * z + y
    pair = 2 * (D // 4)
    return (
        attention.at[
            pl.ds(4 * half, 4), pl.ds(aligned(place, down), down), pl.ds(aligned(x, pair), pair)
        ],
        inner.at[half, pl.ds(aligned(x, pair), pair), pl.ds(aligned(place, side), side)],
        outer.at[
            pl.ds(aligned(2 * place + half, down // 2), down // 2),
            pl.ds(aligned(x, 2 * deep), 2 * deep),
        ],
    )


def greet(neighbours):
    barrier = pltpu.get_barrier_semaphore()
    for device, present in neighbours:
        def signal(device=device):
            pl.semaphore_signal(barrier, inc=1, device_id=device, device_id_type=MESH)
        if present is None:
            signal()
        else:
            pl.when(present)(signal)
    expected = 0
    for _, present in neighbours:
        expected = expected + (1 if present is None else jnp.where(present, 1, 0))
    pl.semaphore_wait(barrier, expected)


def neighbours_of(depth, z, y, x, core):
    return (
        (device_at(z, y, x, 1 - core), None),
        (device_at(z, y, 1 - x, core), None),
        (device_at(z, 1 - y, x, core), None),
        (device_at(z - 1, y, x, core), z > 0),
        (device_at(z + 1, y, x, core), z < depth - 1),
    )


RIGHT, LEFT, TO_Y, TO_X, TO_CORE = range(5)


def gather_kernel(depth, widths, a_ref, i_ref, o_ref, wa, wi, wo, pair_a, pair_i, pair_o,
                  got_a, got_i, got_o, swap_send, swap_recv, own_sem, send_sem, recv_sem):
    z, y, x, core = where_am_i()
    other = 1 - core
    greet(neighbours_of(depth, z, y, x, core))
    full = (wa, wi, wo)
    down = widths[0]
    swaps = [
        pltpu.make_async_remote_copy(
            src_ref=src, dst_ref=dst, send_sem=swap_send.at[n], recv_sem=swap_recv.at[n],
            device_id=device_at(z, y, x, other), device_id_type=MESH)
        for n, (src, dst) in enumerate((
            (a_ref.at[pl.ds(4 * other, 4)], got_a),
            (i_ref.at[other], got_i),
            (o_ref.at[pl.ds(aligned(other, down // 2), down // 2)], got_o),
        ))
    ]
    for swap in swaps:
        swap.start()
    width, deep = a_ref.shape[2], o_ref.shape[1]
    tall = i_ref.shape[1]
    for swap in swaps:
        swap.wait_recv()
    for me in range(2):
        @pl.when(core == me)
        def _(me=me):
            mine, theirs = me, 1 - me
            pair_a[:, :, mine * width : (mine + 1) * width] = a_ref[4 * me : 4 * me + 4]
            pair_a[:, :, theirs * width : (theirs + 1) * width] = got_a[...]
            pair_i[mine * tall : (mine + 1) * tall] = i_ref[me]
            pair_i[theirs * tall : (theirs + 1) * tall] = got_i[...]
            half = down // 2
            pair_o[:, mine * deep : (mine + 1) * deep] = o_ref[me * half : (me + 1) * half]
            pair_o[:, theirs * deep : (theirs + 1) * deep] = got_o[...]

    pairs = (pair_a, pair_i, pair_o)

    def index(bz, by, bx):
        return (2 * bz + by) * 2 + bx

    def copy(piece, bz, by, bx, kind, own=False):
        target = {
            RIGHT: device_at(z + 1, y, x, core),
            LEFT: device_at(z - 1, y, x, core),
            TO_Y: device_at(z, 1 - y, x, core),
            TO_X: device_at(z, y, 1 - x, core),
            TO_CORE: device_at(z, y, x, other),
        }[kind]
        place = block_of(full, widths, bz, by, bx, core)[piece]
        slot = index(bz, by, bx)
        return pltpu.make_async_remote_copy(
            src_ref=pairs[piece] if own else place, dst_ref=place,
            send_sem=send_sem.at[piece, kind, slot], recv_sem=recv_sem.at[piece, 0, slot]
            if kind != TO_CORE else recv_sem.at[piece, 1, slot],
            device_id=target, device_id_type=MESH)

    def arrive(piece, bz, by, bx, half):
        place = block_of(full, widths, bz, by, bx, half)[piece]
        which = 0 if half is core else 1
        pltpu.make_async_remote_copy(
            src_ref=place, dst_ref=place, send_sem=send_sem.at[piece, 0, 0],
            recv_sem=recv_sem.at[piece, which, index(bz, by, bx)],
            device_id=device_at(z, y, x, other), device_id_type=MESH).wait_recv()

    owns = [
        pltpu.make_async_copy(pairs[n], block_of(full, widths, z, y, x, core)[n], own_sem.at[n])
        for n in range(PIECES)
    ]

    def launch_own(kind):
        for n in range(PIECES):
            copy(n, z, y, x, kind, True).start()

    pl.when(z < depth - 1)(lambda: launch_own(RIGHT))
    pl.when(z > 0)(lambda: launch_own(LEFT))
    for n in range(PIECES):
        copy(n, z, y, x, TO_Y, True).start()
        copy(n, z, y, x, TO_X, True).start()
    for n in range(PIECES):
        copy(n, z, y, x, TO_CORE, True).start()
        owns[n].start()

    FIRST, LATER = (0,), (1, 2)

    def from_z(bz, kind, further):
        for n in range(PIECES):
            arrive(n, bz, y, x, core)
            pl.when(further)(lambda n=n: copy(n, bz, y, x, kind).start())
            copy(n, bz, y, x, TO_Y).start()
            copy(n, bz, y, x, TO_X).start()
            copy(n, bz, y, x, TO_CORE).start()

    def from_sides(bz):
        for n in FIRST:
            arrive(n, bz, 1 - y, x, core)
            copy(n, bz, 1 - y, x, TO_X).start()
            copy(n, bz, 1 - y, x, TO_CORE).start()
        for n in LATER:
            arrive(n, bz, y, 1 - x, core)
            copy(n, bz, y, 1 - x, TO_Y).start()
            copy(n, bz, y, 1 - x, TO_CORE).start()
        for n in FIRST:
            arrive(n, bz, y, 1 - x, core)
            copy(n, bz, y, 1 - x, TO_CORE).start()
        for n in LATER:
            arrive(n, bz, 1 - y, x, core)
            copy(n, bz, 1 - y, x, TO_CORE).start()

    def from_corner(bz):
        for n in range(PIECES):
            arrive(n, bz, 1 - y, 1 - x, core)
            copy(n, bz, 1 - y, 1 - x, TO_CORE).start()

    def both_ways(step, action):
        pl.when(z - step >= 0)(lambda: action(z - step))
        pl.when(z + step < depth)(lambda: action(z + step))

    for step in range(1, depth):
        pl.when(z - step >= 0)(lambda: from_z(z - step, RIGHT, z < depth - 1))
        pl.when(z + step < depth)(lambda: from_z(z + step, LEFT, z > 0))
        if step == 1:
            from_sides(z)
        else:
            both_ways(step - 1, from_sides)
    both_ways(depth - 1, from_sides)
    from_corner(z)
    for step in range(1, depth):
        both_ways(step, from_corner)

    for swap in swaps:
        swap.wait_send()
    for own in owns:
        own.wait()
    for n in range(PIECES):
        @pl.loop(0, depth)
        def _(bz, n=n):
            for by in range(2):
                for bx in range(2):
                    arrive(n, bz, by, bx, other)
                    copy(n, bz, by, bx, TO_CORE).wait_send()
            copy(n, bz, y, x, TO_Y).wait_send()
            copy(n, bz, y, x, TO_X).wait_send()
            if n in FIRST:
                copy(n, bz, 1 - y, x, TO_X).wait_send()
            else:
                copy(n, bz, y, 1 - x, TO_Y).wait_send()
            pl.when((bz <= z) & (z < depth - 1))(lambda: copy(n, bz, y, x, RIGHT).wait_send())
            pl.when((bz >= z) & (z > 0))(lambda: copy(n, bz, y, x, LEFT).wait_send())


def gather_blocks(attention, inner, outer):
    depth = lax.axis_size("dp") // 2
    down, width = attention.shape[1:]
    tall, side = inner.shape[1:]
    deep = outer.shape[1]
    chips = depth * 4
    hbm = pl.BlockSpec(memory_space=pl.ANY)
    vmem = pl.BlockSpec(memory_space=pltpu.VMEM)
    across, within = lax.axis_size("dp"), lax.axis_size("fsdp")
    return pl.pallas_call(
        functools.partial(gather_kernel, depth, (down, side, deep)),
        out_shape=(
            jax.ShapeDtypeStruct((8, across * down, within * width), bf16),
            jax.ShapeDtypeStruct((2, within * tall, across * side), bf16),
            jax.ShapeDtypeStruct((across * down, within * deep), bf16),
        ),
        in_specs=[vmem] * 3,
        out_specs=(hbm,) * 3,
        scratch_shapes=[
            pltpu.VMEM((4, down, 2 * width), bf16),
            pltpu.VMEM((2 * tall, side), bf16),
            pltpu.VMEM((down // 2, 2 * deep), bf16),
            pltpu.VMEM((4, down, width), bf16),
            pltpu.VMEM((tall, side), bf16),
            pltpu.VMEM((down // 2, deep), bf16),
            pltpu.SemaphoreType.DMA((PIECES,)),
            pltpu.SemaphoreType.DMA((PIECES,)),
            pltpu.SemaphoreType.DMA((PIECES,)),
            pltpu.SemaphoreType.DMA((PIECES, 5, chips)),
            pltpu.SemaphoreType.DMA((PIECES, 2, chips)),
        ],
        compiler_params=pltpu.CompilerParams(collective_id=0, has_side_effects=True),
    )(attention, inner, outer)


def scatter_order(depth):
    return sorted(range(depth), key=lambda place: (-abs(2 * place - depth + 1), -place))


def add_rows(target, sources):
    def total(at):
        value = sources[0][at].astype(f32)
        for source in sources[1:]:
            value = value + source[at].astype(f32)
        target[at] = value.astype(target.dtype)

    if len(target.shape) == 3:
        @pl.loop(0, target.shape[0])
        def _(k):
            total((k,))
    else:
        slab = 16
        @pl.loop(0, target.shape[0] // slab)
        def _(k):
            total((pl.ds(aligned(k, slab), slab),))


def scatter_kernel(depth, widths, ga, gi, go, gain_ref,
                   own_a, own_i, own_o, gain_out,
                   acc_a, acc_i, acc_o, swap_a, swap_i, swap_o, one_a, one_i, one_o,
                   two_a, two_i, two_o, line_a, line_i, line_o, sum_a, sum_i, sum_o,
                   out_a, out_i, out_o, in_a, in_i, in_o, gain_buf,
                   load_sem, swap_send, swap_recv, one_send, one_recv, two_send, two_recv,
                   line_send, line_recv, end_send, end_recv, gain_send, gain_recv):
    z, y, x, core = where_am_i()
    other = 1 - core
    greet(neighbours_of(depth, z, y, x, core))
    full = (ga, gi, go)
    acc, swapped = (acc_a, acc_i, acc_o), (swap_a, swap_i, swap_o)
    first, second = (one_a, one_i, one_o), (two_a, two_i, two_o)
    line, sums = (line_a, line_i, line_o), (sum_a, sum_i, sum_o)
    outs, ins = (out_a, out_i, out_o), (in_a, in_i, in_o)
    order = scatter_order(depth)
    partner = device_at(z, y, x, other)

    def index(bz, by, bx):
        return (2 * bz + by) * 2 + bx

    def load(n, bz, by, bx):
        slot = index(bz, by, bx)
        return pltpu.make_async_copy(
            block_of(full, widths, bz, by, bx, core)[n], acc[n].at[slot], load_sem.at[n, slot])

    def remote(src, dst, send, recv, device):
        return pltpu.make_async_remote_copy(
            src_ref=src, dst_ref=dst, send_sem=send, recv_sem=recv,
            device_id=device, device_id_type=MESH)

    def swap(n, bz, by, bx):
        slot = index(bz, by, bx)
        return remote(block_of(full, widths, bz, by, bx, other)[n], swapped[n].at[slot],
                      swap_send.at[n, slot], swap_recv.at[n, slot], partner)

    def side(n, stage):
        over_x = (n == 0) == (stage == 0)
        return device_at(z, y, 1 - x, core) if over_x else device_at(z, 1 - y, x, core)

    def stage_one(n, bz, place):
        far = index(bz, place, 1 - x) if n == 0 else index(bz, 1 - y, place)
        slot = 2 * bz + place
        return remote(acc[n].at[far], first[n].at[slot], one_send.at[n, slot],
                      one_recv.at[n, slot], side(n, 0))

    def stage_two(n, bz):
        far = index(bz, 1 - y, x) if n == 0 else index(bz, y, 1 - x)
        return remote(acc[n].at[far], second[n].at[bz], two_send.at[n, bz], two_recv.at[n, bz],
                      side(n, 1))

    def along(n, bz, way):
        device = device_at(z + 1, y, x, core) if way == 0 else device_at(z - 1, y, x, core)
        return remote(acc[n].at[index(bz, y, x)], line[n].at[way, bz],
                      line_send.at[n, way, bz], line_recv.at[n, way, bz], device)

    gain_buf[0] = gain_ref[...]
    hops = (partner, device_at(z, y, 1 - x, core), device_at(z, 1 - y, x, core))

    def gain_hop(step):
        return remote(gain_buf.at[2 * step], gain_buf.at[2 * step + 1], gain_send.at[step],
                      gain_recv.at[step], hops[step])

    def gain_line(way):
        device = device_at(z + 1, y, x, core) if way == 0 else device_at(z - 1, y, x, core)
        return remote(gain_buf.at[7 + way], gain_buf.at[9 + way], gain_send.at[3 + way],
                      gain_recv.at[3 + way], device)

    gain_hop(0).start()

    def far_first(n):
        if n == 0:
            return ((1 - y, 1 - x), (y, 1 - x), (1 - y, x), (y, x))
        return ((1 - y, 1 - x), (1 - y, x), (y, 1 - x), (y, x))

    for bz in order:
        for n in range(PIECES):
            for by, bx in far_first(n):
                swap(n, bz, by, bx).start()
                load(n, bz, by, bx).start()

    def join(n, bz, by, bx, extra=()):
        load(n, bz, by, bx).wait()
        swap(n, bz, by, bx).wait_recv()
        slot = index(bz, by, bx)
        add_rows(acc[n].at[slot], (acc[n].at[slot], swapped[n].at[slot]) + extra)

    def send_first(bz):
        for n in range(PIECES):
            for place in ((1 - y, y) if n == 0 else (1 - x, x)):
                if n == 0:
                    join(n, bz, place, 1 - x)
                else:
                    join(n, bz, 1 - y, place)
                stage_one(n, bz, place).start()

    def send_second(bz):
        for n in range(PIECES):
            place = 1 - y if n == 0 else 1 - x
            stage_one(n, bz, place).wait_recv()
            slot = 2 * bz + place
            if n == 0:
                join(n, bz, place, x, (first[n].at[slot],))
            else:
                join(n, bz, y, place, (first[n].at[slot],))
            stage_two(n, bz).start()

    def finish(bz):
        for n in range(PIECES):
            place = y if n == 0 else x
            stage_one(n, bz, place).wait_recv()
            stage_two(n, bz).wait_recv()
            slot = index(bz, y, x)
            arrived = (first[n].at[2 * bz + place], second[n].at[bz])
            load(n, bz, y, x).wait()
            swap(n, bz, y, x).wait_recv()
            base = (acc[n].at[slot], swapped[n].at[slot]) + arrived
            before, after = z > 0, z < depth - 1

            @pl.when(z < bz)
            def _(n=n, base=base, slot=slot):
                @pl.when(before)
                def _():
                    along(n, bz, 0).wait_recv()
                    add_rows(acc[n].at[slot], base + (line[n].at[0, bz],))
                @pl.when(z == 0)
                def _():
                    add_rows(acc[n].at[slot], base)
                along(n, bz, 0).start()

            @pl.when(z > bz)
            def _(n=n, base=base, slot=slot):
                @pl.when(after)
                def _():
                    along(n, bz, 1).wait_recv()
                    add_rows(acc[n].at[slot], base + (line[n].at[1, bz],))
                @pl.when(z == depth - 1)
                def _():
                    add_rows(acc[n].at[slot], base)
                along(n, bz, 1).start()

            @pl.when(z == bz)
            def _(n=n, base=base):
                add_rows(sums[n], base)
                @pl.when(before)
                def _():
                    along(n, bz, 0).wait_recv()
                    add_rows(sums[n], (sums[n], line[n].at[0, bz]))
                @pl.when(after)
                def _():
                    along(n, bz, 1).wait_recv()
                    add_rows(sums[n], (sums[n], line[n].at[1, bz]))

    steps = [(send_first, send_second, finish)[lag] for lag in range(3)]
    for turn in range(len(order) + 2):
        for lag in range(3):
            if 0 <= turn - lag < len(order):
                steps[lag](order[turn - lag])
        if turn < 3:
            gain_hop(turn).wait_recv()
            gain_buf[2 * turn + 2] = gain_buf[2 * turn] + gain_buf[2 * turn + 1]
            if turn < 2:
                gain_hop(turn + 1).start()

    gain_out[...] = gain_buf[6]

    @pl.when(z > 0)
    def _():
        gain_line(0).wait_recv()
        gain_out[...] = gain_out[...] + gain_buf[9]

    @pl.when(z < depth - 1)
    def _():
        gain_buf[7] = gain_out[...]
        gain_line(0).start()
        gain_line(1).wait_recv()

    @pl.when((z > 0) & (z < depth - 1))
    def _():
        gain_buf[8] = gain_buf[6] + gain_buf[10]

    @pl.when(z == depth - 1)
    def _():
        gain_buf[8] = gain_buf[6]

    @pl.when(z > 0)
    def _():
        gain_line(1).start()

    @pl.when(z < depth - 1)
    def _():
        gain_out[...] = gain_out[...] + gain_buf[10]

    width, tall, deep = own_a.shape[2], own_i.shape[1], own_o.shape[1]
    half = widths[0] // 2
    for me in range(2):
        @pl.when(core == me)
        def _(me=me):
            far = 1 - me
            for k in range(4):
                out_a[k] = sum_a[k, :, far * width : (far + 1) * width]
                own_a[4 * me + k] = sum_a[k, :, me * width : (me + 1) * width]
            out_i[...] = sum_i[far * tall : (far + 1) * tall]
            own_i[me] = sum_i[me * tall : (me + 1) * tall]
            out_o[...] = sum_o[:, far * deep : (far + 1) * deep]
            own_o[me * half : (me + 1) * half] = sum_o[:, me * deep : (me + 1) * deep]
    ends = [remote(outs[n], ins[n], end_send.at[n], end_recv.at[n], partner)
            for n in range(PIECES)]
    for end in ends:
        end.start()
    for end in ends:
        end.wait_recv()
    for me in range(2):
        @pl.when(core == me)
        def _(me=me):
            far = 1 - me
            own_a[4 * far : 4 * far + 4] = in_a[...]
            own_i[far] = in_i[...]
            own_o[far * half : (far + 1) * half] = in_o[...]

    for end in ends:
        end.wait_send()
    for step in range(3):
        gain_hop(step).wait_send()
    pl.when(z < depth - 1)(lambda: gain_line(0).wait_send())
    pl.when(z > 0)(lambda: gain_line(1).wait_send())
    for n in range(PIECES):
        @pl.loop(0, depth)
        def _(bz, n=n):
            for by in range(2):
                for bx in range(2):
                    swap(n, bz, by, bx).wait_send()
            for place in range(2):
                stage_one(n, bz, place).wait_send()
            stage_two(n, bz).wait_send()
            pl.when(z < bz)(lambda: along(n, bz, 0).wait_send())
            pl.when(z > bz)(lambda: along(n, bz, 1).wait_send())


def scatter_blocks(attention, inner, outer, gains):
    across, within = lax.axis_size("dp"), lax.axis_size("fsdp")
    depth, chips = across // 2, across * 2
    down, width = D // across, D // within
    tall, side, deep = width, inner.shape[2] // across, outer.shape[1] // within
    pieces = ((4, down, 2 * width), (2 * tall, side), (down // 2, 2 * deep))
    ends = ((4, down, width), (tall, side), (down // 2, deep))
    hbm = pl.BlockSpec(memory_space=pl.ANY)
    vmem = pl.BlockSpec(memory_space=pltpu.VMEM)
    wave = pltpu.SemaphoreType.DMA

    def buffers(lead, kind=bf16, shapes=pieces):
        return [pltpu.VMEM(tuple(lead) + shape, kind) for shape in shapes]

    return pl.pallas_call(
        functools.partial(scatter_kernel, depth, (down, side, deep)),
        out_shape=(
            jax.ShapeDtypeStruct((8, down, width), f32),
            jax.ShapeDtypeStruct((2, tall, side), f32),
            jax.ShapeDtypeStruct((down, deep), f32),
            jax.ShapeDtypeStruct(gains.shape, f32),
        ),
        in_specs=[hbm] * 3 + [vmem],
        out_specs=(vmem,) * 4,
        scratch_shapes=[
            *buffers((chips,)), *buffers((chips,)), *buffers((2 * depth,)), *buffers((depth,)),
            *buffers((2, depth)), *buffers((), f32), *buffers((), f32, ends),
            *buffers((), f32, ends),
            pltpu.VMEM((11,) + gains.shape, f32),
            wave((PIECES, chips)), wave((PIECES, chips)), wave((PIECES, chips)),
            wave((PIECES, 2 * depth)), wave((PIECES, 2 * depth)),
            wave((PIECES, depth)), wave((PIECES, depth)),
            wave((PIECES, 2, depth)), wave((PIECES, 2, depth)),
            wave((PIECES,)), wave((PIECES,)), wave((5,)), wave((5,)),
        ],
        compiler_params=pltpu.CompilerParams(
            collective_id=1, has_side_effects=True, vmem_limit_bytes=60 * 1024 * 1024
        ),
    )(attention, inner, outer, gains)


def tile_aligned(down, width, side, deep):
    return (
        lax.axis_size("fsdp") == 4
        and lax.axis_size("dp") % 2 == 0
        and down % 32 == 0
        and (2 * width) % 128 == 0
        and side % 128 == 0
        and (2 * deep) % 128 == 0
    )


def adam_update(weight, mean_old, square_old, gradient, step_rate, decay_rate):
    mean_new = beta_one * mean_old + (1.0 - beta_one) * gradient
    square_new = beta_two * square_old + (1.0 - beta_two) * gradient * gradient
    corrected = (
        mean_new
        / (1.0 - beta_one**STEP)
        / (jnp.sqrt(square_new / (1.0 - beta_two**STEP)) + adam_epsilon)
    )
    master = weight - step_rate * (corrected + decay_rate * weight)
    return (mean_new, square_new, master, master.astype(bf16))


def on_device(
    hidden_in,
    patches,
    token_segments,
    patch_segments,
    cotangent,
    attention_weights,
    attention_means,
    attention_squares,
    inner_weights,
    inner_means,
    inner_squares,
    outer_weights,
    outer_means,
    outer_squares,
    norm_gains,
    gain_means,
    gain_squares,
):
    rows, _, length, _ = hidden_in.shape
    count = patches.shape[2]
    tokens = rows * length
    width, down = attention_weights.shape[1:]
    whole_tiles = tile_aligned(down, width, inner_weights.shape[2], outer_weights.shape[0])
    if whole_tiles:
        weights, inner, outer = gather_blocks(
            jnp.swapaxes(attention_weights, 1, 2).astype(bf16),
            inner_weights.astype(bf16),
            outer_weights.T.astype(bf16),
        )
    else:
        weights, inner, outer = gather_weights(
            attention_weights.astype(bf16), inner_weights.astype(bf16), outer_weights.astype(bf16)
        )
    gains = lax.all_gather(norm_gains.astype(bf16), "fsdp", axis=1, tiled=True)

    initial = hidden_in.reshape(tokens, D).astype(f32)
    patch_rows = patches.reshape(rows * count, D)
    token_rows = token_segments.reshape(rows, 1, length)
    token_columns = token_segments.reshape(rows, length, 1)
    patch_columns = patch_segments.reshape(rows, count, 1)

    normed_one, unit_one, rms_one = norm_forward(initial, gains[0])
    packed = dot_nt(normed_one, weights[0:3].reshape(3 * D, D)).astype(bf16)
    packed = packed.reshape(rows, length, 3 * D)
    mixture_one, lse_one = attend_forward(
        self_forward_kernel, packed, packed, (PAIRS, 2 * PAIRS), token_rows, token_columns,
        (1, length),
    )
    mixed_one = mixture_one.reshape(tokens, D)
    after_one = initial + dot_nt(mixed_one, weights[3])
    normed_two, unit_two, rms_two = norm_forward(after_one, gains[1])
    cross_query = dot_nt(normed_two, weights[4]).astype(bf16).reshape(rows, length, D)
    cross_pair = dot_nt(patch_rows, weights[5:7].reshape(2 * D, D)).astype(bf16)
    cross_pair = cross_pair.reshape(rows, count, 2 * D)
    mixture_two, lse_two = attend_forward(
        cross_forward_kernel, cross_query, cross_pair, (0, PAIRS), token_columns, patch_columns,
        (length, 1),
    )
    mixed_two = mixture_two.reshape(tokens, D)
    after_two = after_one + dot_nt(mixed_two, weights[7])
    normed_three, unit_three, rms_three = norm_forward(after_two, gains[2])
    gate = dot_nn(normed_three, inner[0])
    up = dot_nn(normed_three, inner[1])
    units = (gelu_tanh(gate) * up).astype(bf16)
    hidden_out = (after_two + dot_nt(units, outer)).astype(bf16)

    grad_low = cotangent.reshape(tokens, D)
    grad_final = grad_low.astype(f32)
    grad_outer = dot_tn(grad_low, units).astype(bf16)
    grad_units = dot_nn(grad_low, outer)
    activation, gelu_back = jax.vjp(gelu_tanh, gate)
    grad_gate = gelu_back(grad_units * up)[0].astype(bf16)
    grad_up = (grad_units * activation).astype(bf16)
    grad_inner = jnp.stack(
        [dot_tn(normed_three, grad_gate).astype(bf16), dot_tn(normed_three, grad_up).astype(bf16)]
    )
    grad_normed = dot_nt(grad_gate, inner[0]) + dot_nt(grad_up, inner[1])
    grad_from_three, gain_three = norm_backward(grad_normed, gains[2], unit_three, rms_three)
    grad_two = grad_final + grad_from_three
    branch_two = grad_two.astype(bf16)
    grad_mixture_two = dot_nn(branch_two, weights[7]).astype(bf16).reshape(rows, length, D)
    grad_cq, grad_ck, grad_cv = attend_backward(
        cross_backward_kernel, cross_query, cross_pair, (0, PAIRS), mixture_two,
        grad_mixture_two, lse_two, token_columns, patch_columns, (length, 1),
    )
    grad_cq = grad_cq.reshape(tokens, D)
    grad_ck = grad_ck.reshape(rows * count, D)
    grad_cv = grad_cv.reshape(rows * count, D)
    patch_grad = dot_nn(grad_ck, weights[5]) + dot_nn(grad_cv, weights[6])
    grad_from_two, gain_two = norm_backward(
        dot_nn(grad_cq, weights[4]), gains[1], unit_two, rms_two
    )
    grad_one = grad_two + grad_from_two
    branch_one = grad_one.astype(bf16)
    grad_mixture_one = dot_nn(branch_one, weights[3]).astype(bf16).reshape(rows, length, D)
    grad_q, grad_k, grad_v = attend_backward(
        self_backward_kernel, packed, packed, (PAIRS, 2 * PAIRS), mixture_one,
        grad_mixture_one, lse_one, token_rows, token_columns, (1, length),
    )
    grad_q = grad_q.reshape(tokens, D)
    grad_k = grad_k.reshape(tokens, D)
    grad_v = grad_v.reshape(tokens, D)
    grad_normed_one = (
        dot_nn(grad_q, weights[0]) + dot_nn(grad_k, weights[1]) + dot_nn(grad_v, weights[2])
    )
    grad_from_one, gain_one = norm_backward(grad_normed_one, gains[0], unit_one, rms_one)
    hidden_grad = grad_one + grad_from_one
    grad_attention = jnp.stack(
        [
            dot_tn(grad_q, normed_one).astype(bf16),
            dot_tn(grad_k, normed_one).astype(bf16),
            dot_tn(grad_v, normed_one).astype(bf16),
            dot_tn(branch_one, mixed_one).astype(bf16),
            dot_tn(grad_cq, normed_two).astype(bf16),
            dot_tn(grad_ck, patch_rows).astype(bf16),
            dot_tn(grad_cv, patch_rows).astype(bf16),
            dot_tn(branch_two, mixed_two).astype(bf16),
        ]
    )
    gain_grads = jnp.stack([gain_one, gain_two, gain_three])
    if whole_tiles:
        own_attention, own_inner, own_outer, gain_totals = scatter_blocks(
            grad_attention, grad_inner, grad_outer, jnp.pad(gain_grads, ((0, 5), (0, 0)))
        )
        own_attention = jnp.swapaxes(own_attention, 1, 2)
        own_outer = own_outer.T
        gain_totals = gain_totals[:3]
    else:
        own_attention, own_inner, own_outer = scatter_grads(
            grad_attention, grad_inner, grad_outer
        )
        gain_totals = lax.psum(gain_grads, BOTH)
    width = norm_gains.shape[1]
    own_gains = lax.dynamic_slice_in_dim(
        gain_totals, lax.axis_index("fsdp") * width, width, axis=1
    )

    attention_new = adam_update(
        attention_weights, attention_means, attention_squares, own_attention,
        rate_matrix, decay_matrix,
    )
    inner_new = adam_update(
        inner_weights, inner_means, inner_squares, own_inner, rate_matrix, decay_matrix
    )
    outer_new = adam_update(
        outer_weights, outer_means, outer_squares, own_outer, rate_matrix, decay_matrix
    )
    gain_new = adam_update(norm_gains, gain_means, gain_squares, own_gains, rate_gain, 0.0)
    return (
        hidden_out.reshape(hidden_in.shape),
        hidden_grad.reshape(hidden_in.shape),
        patch_grad.reshape(patches.shape),
        *attention_new,
        *inner_new,
        *outer_new,
        *gain_new,
    )


def solution(mesh):
    rows = P(None, BOTH, None, None)
    ids = P(None, BOTH, None)
    matrix = P(None, "fsdp", "dp")
    down = P("fsdp", "dp")
    gain = P(None, "fsdp")
    return jax.shard_map(
        on_device,
        mesh=mesh,
        in_specs=(rows, rows, ids, ids, rows) + (matrix,) * 6 + (down,) * 3 + (gain,) * 3,
        out_specs=(rows, rows, rows) + (matrix,) * 8 + (down,) * 4 + (gain,) * 4,
        check_vma=False,
    )
```

```python
import functools

import jax
import jax.numpy as jnp
from jax import lax
from jax.experimental import pallas as pl
from jax.experimental.pallas import tpu as pltpu
from jax.sharding import PartitionSpec as P

D = 768
HEADS = 12
HEAD = 64
PAIR = 2 * HEAD
PAIRS = HEADS // 2
STEP = 10
SEGS = 4

epsilon = 1e-06
score_scale = 0.125
masked_value = -1000000000.0
beta_one = 0.9
beta_two = 0.95
adam_epsilon = 1e-08
decay_matrix = 0.1
rate_matrix = 0.1
rate_gain = 0.3
f32 = jnp.float32
bf16 = jnp.bfloat16
BOTH = ("dp", "fsdp")


def gelu_tanh(values):
    return (
        0.5
        * values
        * (1.0 + jnp.tanh(0.7978845608028654 * (values + 0.044715 * values * values * values)))
    )


def dot_nn(a, b):
    return lax.dot_general(a, b, (((1,), (0,)), ((), ())), preferred_element_type=f32)


def dot_nt(a, b):
    return lax.dot_general(a, b, (((1,), (1,)), ((), ())), preferred_element_type=f32)


def dot_tn(a, b):
    return lax.dot_general(a, b, (((0,), (0,)), ((), ())), preferred_element_type=f32)


def norm_forward(values, gain):
    inverse_rms = lax.rsqrt(jnp.mean(values * values, axis=-1, keepdims=True) + epsilon)
    unit_rows = values * inverse_rms
    return ((unit_rows * gain.astype(f32)).astype(bf16), unit_rows, inverse_rms)


def norm_backward(grad_rows, gain, unit_rows, inverse_rms):
    grad_unit = grad_rows * gain.astype(f32)
    grad_values = inverse_rms * (
        grad_unit - unit_rows * jnp.mean(grad_unit * unit_rows, axis=-1, keepdims=True)
    )
    return (grad_values, jnp.sum(grad_rows * unit_rows, axis=0))


def head_half(block, half):
    lane = lax.broadcasted_iota(jnp.int32, block.shape, 1)
    keep = (lane < HEAD) if half == 0 else (lane >= HEAD)
    return jnp.where(keep, block, jnp.zeros_like(block))


def three_parts(column):
    high = column.astype(bf16).astype(f32)
    rest = column - high
    middle = rest.astype(bf16).astype(f32)
    low = rest - middle
    return high, middle, low


def stat_lanes(base, column, first):
    lane = lax.broadcasted_iota(jnp.int32, base.shape, 1)
    for place, part in enumerate(three_parts(column)):
        base = jnp.where(lane == first + place, -part, base)
    return base


def key_marks(key_ids, stats):
    lane = lax.broadcasted_iota(jnp.int32, (key_ids.shape[0], 128), 1)
    marks = lane == key_ids
    if stats:
        marks = marks | ((lane >= SEGS) & (lane < SEGS + 3))
    return jnp.where(marks, 1.0, 0.0).astype(bf16)


def query_bias(query_ids):
    lane = lax.broadcasted_iota(jnp.int32, (query_ids.shape[0], 128), 1)
    return jnp.where((lane == query_ids) | (lane >= SEGS), 0.0, masked_value)


def softmax_columns(scores):
    top = jnp.max(scores, axis=0, keepdims=True)
    raised = jnp.exp(scores - top)
    return raised, top, jnp.sum(raised, axis=0, keepdims=True)


def finish_forward(halves, tops, sums, o_ref, lse_ref):
    mixed = jnp.concatenate([h / s for h, s in zip(halves, sums)], axis=0)
    o_ref[0] = mixed.T.astype(bf16)
    rows = [t + jnp.log(s) for t, s in zip(tops, sums)]
    pad = jnp.zeros((6, rows[0].shape[1]), f32)
    lse_ref[0, 0] = jnp.concatenate(rows + [pad], axis=0)


def cross_forward_kernel(rider, q_ref, c_ref, wk_ref, wv_ref, qid_ref, kid_ref, *refs):
    (o_ref, lse_ref, k_ref, v_ref) = rider.board(refs, 4)
    key = dot_nt(c_ref[0], wk_ref[0]).astype(bf16)
    value = dot_nt(c_ref[0], wv_ref[0]).astype(bf16)
    k_ref[0], v_ref[0] = key, value
    marked = jnp.concatenate([key, key_marks(kid_ref[0], False)], axis=1)
    bias = query_bias(qid_ref[0]).astype(bf16)
    query = q_ref[0] * jnp.asarray(score_scale, bf16)
    values = value.T
    halves, tops, sums = [], [], []
    for half in range(2):
        extended = jnp.concatenate([head_half(query, half), bias], axis=1)
        raised, top, total = softmax_columns(dot_nt(marked, extended))
        halves.append(dot_nn(values[half * HEAD : (half + 1) * HEAD], raised.astype(bf16)))
        tops.append(top)
        sums.append(total)
    finish_forward(halves, tops, sums, o_ref, lse_ref)


def causal_mask(qid_ref, kid_ref):
    length = kid_ref.shape[1]
    key = lax.broadcasted_iota(jnp.int32, (length, length), 0)
    query = lax.broadcasted_iota(jnp.int32, (length, length), 1)
    return (key <= query) & (kid_ref[0] == qid_ref[0])


def self_forward_kernel(q_ref, k_ref, v_ref, qid_ref, kid_ref, o_ref, lse_ref):
    allowed = causal_mask(qid_ref, kid_ref)
    query = q_ref[0] * jnp.asarray(score_scale, bf16)
    key = k_ref[0]
    values = v_ref[0].T
    halves, tops, sums = [], [], []
    for half in range(2):
        scores = jnp.where(allowed, dot_nt(key, head_half(query, half)), masked_value)
        raised, top, total = softmax_columns(scores)
        halves.append(dot_nn(values[half * HEAD : (half + 1) * HEAD], raised.astype(bf16)))
        tops.append(top)
        sums.append(total)
    finish_forward(halves, tops, sums, o_ref, lse_ref)


def backward_pair(q_ref, k_ref, v_ref, o_ref, do_ref, lse_ref, marked, bias, allowed,
                  dq_ref, dk_ref, dv_ref):
    query, grad = q_ref[0], do_ref[0]
    scaled = query * jnp.asarray(score_scale, bf16)
    key_turned = k_ref[0].T
    length = query.shape[0]
    lse_columns = lse_ref[0, 0].T
    product = o_ref[0].astype(f32) * grad.astype(f32)
    ones = key_marks(jnp.full((v_ref.shape[1], 1), -1, jnp.int32), True)
    valued = jnp.concatenate([v_ref[0], ones], axis=1)
    probs, grads, turned = [], [], []
    for half in range(2):
        stats = stat_lanes(bias, lse_columns[:, half : half + 1], SEGS).astype(bf16)
        scores = dot_nt(marked, jnp.concatenate([head_half(scaled, half), stats], axis=1))
        if allowed is not None:
            scores = jnp.where(allowed, scores, masked_value)
        weight = jnp.exp(scores)
        inner = jnp.sum(head_half(product, half), axis=1, keepdims=True)
        delta = stat_lanes(jnp.zeros((length, 128), f32), inner, SEGS).astype(bf16)
        shifted = dot_nt(valued, jnp.concatenate([head_half(grad, half), delta], axis=1))
        grad_scores = (weight * shifted).astype(bf16)
        probs.append(weight.astype(bf16))
        grads.append(grad_scores)
        turned.append(dot_nn(key_turned[half * HEAD : (half + 1) * HEAD], grad_scores))
    dq_ref[0] = (score_scale * jnp.concatenate(turned, axis=0)).T.astype(bf16)
    dv_ref[0] = dot_nn(
        jnp.concatenate(probs, axis=1),
        jnp.concatenate([head_half(grad, 0), head_half(grad, 1)], axis=0),
    ).astype(bf16)
    dk_ref[0] = dot_nn(
        jnp.concatenate(grads, axis=1),
        jnp.concatenate([head_half(scaled, 0), head_half(scaled, 1)], axis=0),
    ).astype(bf16)


def cross_backward_kernel(rider, q_ref, k_ref, v_ref, o_ref, do_ref, lse_ref, qid_ref, kid_ref,
                          *refs):
    dq_ref, dk_ref, dv_ref = rider.board(refs, 3)
    marked = jnp.concatenate([k_ref[0], key_marks(kid_ref[0], True)], axis=1)
    backward_pair(q_ref, k_ref, v_ref, o_ref, do_ref, lse_ref, marked, query_bias(qid_ref[0]),
                  None, dq_ref, dk_ref, dv_ref)


def self_backward_kernel(rider, q_ref, k_ref, v_ref, o_ref, do_ref, lse_ref, qid_ref, kid_ref,
                         *refs):
    dq_ref, dk_ref, dv_ref = rider.board(refs, 3)
    length = k_ref.shape[1]
    ones = key_marks(jnp.full((length, 1), -1, jnp.int32), True)
    marked = jnp.concatenate([k_ref[0], ones], axis=1)
    backward_pair(q_ref, k_ref, v_ref, o_ref, do_ref, lse_ref, marked,
                  jnp.zeros((length, 128), f32), causal_mask(qid_ref, kid_ref),
                  dq_ref, dk_ref, dv_ref)


def pair_spec(length, offset):
    return pl.BlockSpec((1, length, PAIR), lambda row, pair: (row, 0, offset + pair))


def row_spec(shape):
    return pl.BlockSpec((1,) + shape, lambda row, pair: (row, 0, 0))


def stat_spec(length):
    return pl.BlockSpec((1, 1, 8, length), lambda row, pair: (row, pair, 0, 0))


def cost(rows, queries, keys, products):
    elements = rows * HEADS * queries * keys
    return pl.CostEstimate(
        flops=2 * elements * 256 * products // 2,
        transcendentals=elements,
        bytes_accessed=rows * (queries + keys) * D * 2 * 3,
    )


class Rider:
    def __init__(self, sizes, names, kind, number):
        self.sizes, self.names, self.kind, self.number = sizes, names, kind, number

    def board(self, refs, outputs):
        count = len(self.names)
        theirs, mine, scratch = refs[:count], refs[count : count + outputs], refs[count + outputs :]
        if count:
            ends, scratch = scratch[:count], scratch[count:]
            build = gather_stages if self.kind == "gather" else scatter_stages
            stages = build(self.sizes, self.names, theirs, ends, scratch)
            steps = pl.num_programs(0) * pl.num_programs(1)
            step = pl.program_id(0) * pl.num_programs(1) + pl.program_id(1)
            run_stages(stages, step, steps)
        return mine

    def in_specs(self):
        return [VMEM if self.kind == "gather" else HBM] * len(self.names)

    def out_specs(self):
        return [HBM if self.kind == "gather" else VMEM] * len(self.names)

    def out_shape(self):
        if self.kind == "gather":
            return [jax.ShapeDtypeStruct(self.sizes.full(n), bf16) for n in self.names]
        return [jax.ShapeDtypeStruct(self.sizes.shard(n), f32) for n in self.names]

    def scratch(self):
        if not self.names:
            return []
        build = gather_scratch if self.kind == "gather" else scatter_scratch
        return build(self.sizes, self.names)

    def params(self):
        if not self.names:
            return pltpu.CompilerParams()
        return pltpu.CompilerParams(
            collective_id=self.number, has_side_effects=True, vmem_limit_bytes=60 * 1024 * 1024
        )


def self_forward(packed, query_ids, key_ids):
    rows, length = packed.shape[:2]
    return pl.pallas_call(
        self_forward_kernel,
        grid=(rows, PAIRS),
        in_specs=[
            pair_spec(length, 0),
            pair_spec(length, PAIRS),
            pair_spec(length, 2 * PAIRS),
            row_spec((1, length)),
            row_spec((length, 1)),
        ],
        out_specs=[pair_spec(length, 0), stat_spec(length)],
        out_shape=[
            jax.ShapeDtypeStruct((rows, length, D), bf16),
            jax.ShapeDtypeStruct((rows, PAIRS, 8, length), f32),
        ],
        cost_estimate=cost(rows, length, length, 2),
        name="self_forward",
    )(packed, packed, packed, query_ids, key_ids)


def cross_forward(rider, queries, patches, projections, query_ids, key_ids, shards):
    rows, length = queries.shape[:2]
    count = patches.shape[1]

    def slab(which):
        return pl.BlockSpec((1, PAIR, D), lambda row, pair: (which, pair, 0))

    return pl.pallas_call(
        functools.partial(cross_forward_kernel, rider),
        grid=(rows, PAIRS),
        in_specs=[
            pair_spec(length, 0),
            row_spec((count, D)),
            slab(1),
            slab(2),
            row_spec((length, 1)),
            row_spec((count, 1)),
        ]
        + rider.in_specs(),
        out_specs=[
            pair_spec(length, 0), stat_spec(length), pair_spec(count, 0), pair_spec(count, 0),
        ]
        + rider.out_specs(),
        out_shape=[
            jax.ShapeDtypeStruct((rows, length, D), bf16),
            jax.ShapeDtypeStruct((rows, PAIRS, 8, length), f32),
            jax.ShapeDtypeStruct((rows, count, D), bf16),
            jax.ShapeDtypeStruct((rows, count, D), bf16),
        ]
        + rider.out_shape(),
        scratch_shapes=rider.scratch(),
        compiler_params=rider.params(),
        cost_estimate=cost(rows, length, count, 4),
        name="cross_forward",
    )(queries, patches, projections, projections, query_ids, key_ids, *shards)


def attend_backward(kernel, rider, queries, keys, values, offsets, mixed, grad, lse, query_ids,
                    key_ids, query_shape, fulls, name):
    rows, length = grad.shape[:2]
    count = keys.shape[1]
    return pl.pallas_call(
        functools.partial(kernel, rider),
        grid=(rows, PAIRS),
        in_specs=[
            pair_spec(length, 0),
            pair_spec(count, offsets[0]),
            pair_spec(count, offsets[1]),
            pair_spec(length, 0),
            pair_spec(length, 0),
            stat_spec(length),
            row_spec(query_shape),
            row_spec((count, 1)),
        ]
        + rider.in_specs(),
        out_specs=[pair_spec(length, 0), pair_spec(count, 0), pair_spec(count, 0)]
        + rider.out_specs(),
        out_shape=[
            jax.ShapeDtypeStruct((rows, length, D), bf16),
            jax.ShapeDtypeStruct((rows, count, D), bf16),
            jax.ShapeDtypeStruct((rows, count, D), bf16),
        ]
        + rider.out_shape(),
        scratch_shapes=rider.scratch(),
        compiler_params=rider.params(),
        cost_estimate=cost(rows, length, count, 5),
        name=name,
    )(queries, keys, values, mixed, grad, lse, query_ids, key_ids, *fulls)


def gather_weights(attention, inner, outer):
    turned = lax.all_gather(jnp.swapaxes(attention, 1, 2), BOTH, axis=0, tiled=False)
    heads = lax.axis_size("dp"), lax.axis_size("fsdp")
    turned = turned.reshape(heads + turned.shape[1:])
    full_attention = jnp.transpose(turned, (2, 0, 3, 1, 4)).reshape(8, D, D)
    wide = lax.all_gather(inner, BOTH, axis=0, tiled=False)
    wide = wide.reshape(heads + wide.shape[1:])
    full_inner = jnp.transpose(wide, (2, 1, 3, 0, 4)).reshape(2, D, -1)
    tall = lax.all_gather(outer.T, BOTH, axis=0, tiled=False)
    tall = tall.reshape(heads + tall.shape[1:])
    full_outer = jnp.transpose(tall, (0, 2, 1, 3)).reshape(D, -1)
    return full_attention, full_inner, full_outer


def scatter_grads(attention, inner, outer):
    across, within = lax.axis_size("dp"), lax.axis_size("fsdp")
    blocks = attention.reshape(8, across, D // across, within, D // within)
    blocks = jnp.transpose(blocks, (1, 3, 0, 2, 4))
    blocks = blocks.reshape((across * within,) + blocks.shape[2:])
    own_attention = lax.psum_scatter(blocks, BOTH, scatter_dimension=0, tiled=False)
    blocks = inner.reshape(2, within, D // within, across, inner.shape[2] // across)
    blocks = jnp.transpose(blocks, (3, 1, 0, 2, 4))
    blocks = blocks.reshape((across * within,) + blocks.shape[2:])
    own_inner = lax.psum_scatter(blocks, BOTH, scatter_dimension=0, tiled=False)
    blocks = outer.reshape(across, D // across, within, outer.shape[1] // within)
    blocks = jnp.transpose(blocks, (0, 2, 1, 3))
    blocks = blocks.reshape((across * within,) + blocks.shape[2:])
    own_outer = lax.psum_scatter(blocks, BOTH, scatter_dimension=0, tiled=False)
    return (
        jnp.swapaxes(own_attention, 1, 2).astype(f32),
        own_inner.astype(f32),
        own_outer.T.astype(f32),
    )


MESH = pl.DeviceIdType.MESH
RIGHT, LEFT, TO_Y, TO_X, TO_CORE = range(5)


def where_am_i():
    across, within = lax.axis_index("dp"), lax.axis_index("fsdp")
    return across // 2, across % 2, within // 2, within % 2


def device_at(z, y, x, core):
    return (2 * z + y, 2 * x + core)


def aligned(value, unit):
    return pl.multiple_of(value * unit, unit)


class Sizes:
    def __init__(self, down, width, side, deep):
        self.down, self.width, self.side, self.deep = down, width, side, deep
        self.across, self.within = D // down, D // width
        self.depth = self.across // 2
        self.chips = self.across * self.within // 2

    def shard(self, name):
        return {
            "low": (4, self.down, self.width),
            "high": (4, self.down, self.width),
            "inner": (2, self.width, self.side),
            "outer": (self.down, self.deep),
        }[name]

    def full(self, name):
        return {
            "low": (4, D, D),
            "high": (4, D, D),
            "inner": (2, D, self.across * self.side),
            "outer": (D, self.within * self.deep),
        }[name]

    def piece(self, name):
        return {
            "low": (self.down, 2 * self.width),
            "high": (self.down, 2 * self.width),
            "inner": (self.width, self.side),
            "outer": (self.down // 2, self.deep),
        }[name]

    def part(self, name):
        return {
            "low": (2, self.down, self.width),
            "high": (2, self.down, self.width),
            "inner": (self.width, self.side),
            "outer": (self.down // 2, self.deep),
        }[name]

    def place(self, name, ref, cut, z, y, x, half):
        place = 2 * z + y
        if name == "inner":
            return ref.at[
                half,
                pl.ds(aligned(2 * x + cut, self.width), self.width),
                pl.ds(aligned(place, self.side), self.side),
            ]
        if name == "outer":
            return ref.at[
                pl.ds(aligned(2 * place + half, self.down // 2), self.down // 2),
                pl.ds(aligned(2 * x + cut, self.deep), self.deep),
            ]
        return ref.at[
            2 * half + cut,
            pl.ds(aligned(place, self.down), self.down),
            pl.ds(aligned(x, 2 * self.width), 2 * self.width),
        ]

    def share(self, name, ref, half):
        if name == "inner":
            return ref.at[half]
        if name == "outer":
            return ref.at[pl.ds(aligned(half, self.down // 2), self.down // 2)]
        return ref.at[pl.ds(2 * half, 2)]


def greet(depth):
    z, y, x, core = where_am_i()
    barrier = pltpu.get_barrier_semaphore()

    def signal(device):
        pl.semaphore_signal(barrier, inc=1, device_id=device, device_id_type=MESH)

    signal(device_at(z, y, x, 1 - core))
    signal(device_at(z, y, 1 - x, core))
    signal(device_at(z, 1 - y, x, core))
    pl.when(z > 0)(lambda: signal(device_at(z - 1, y, x, core)))
    pl.when(z < depth - 1)(lambda: signal(device_at(z + 1, y, x, core)))
    pl.semaphore_wait(barrier, 3 + jnp.where(z > 0, 1, 0) + jnp.where(z < depth - 1, 1, 0))


def chip_index(bz, by, bx):
    return (2 * bz + by) * 2 + bx


def remote(src, dst, send, recv, device):
    return pltpu.make_async_remote_copy(
        src_ref=src, dst_ref=dst, send_sem=send, recv_sem=recv, device_id=device,
        device_id_type=MESH)


def gather_scratch(sizes, names):
    wave = pltpu.SemaphoreType.DMA
    count, pieces = len(names), 2 * len(names)
    return (
        [pltpu.VMEM((2,) + sizes.piece(name), bf16) for name in names]
        + [pltpu.VMEM(sizes.part(name), bf16) for name in names]
        + [wave((count,)), wave((count,)), wave((pieces,)), wave((pieces, 5, sizes.chips)),
           wave((pieces, 2, sizes.chips))]
    )


def gather_stages(sizes, names, shards, fulls, scratch):
    count, depth = len(names), sizes.depth
    pairs, got = scratch[:count], scratch[count : 2 * count]
    swap_send, swap_recv, own_sem, send_sem, recv_sem = scratch[2 * count :]
    z, y, x, core = where_am_i()
    other = 1 - core
    pieces = [(n, cut) for cut in range(2) for n in range(count)]

    def place(piece, bz, by, bx, half):
        n, cut = pieces[piece]
        return sizes.place(names[n], fulls[n], cut, bz, by, bx, half)

    def swap(n):
        return remote(sizes.share(names[n], shards[n], other), got[n], swap_send.at[n],
                      swap_recv.at[n], device_at(z, y, x, other))

    def merge(n, me):
        if names[n] in ("low", "high"):
            width = sizes.width
            for part, source in ((me, shards[n][2 * me : 2 * me + 2]), (1 - me, got[n][...])):
                pairs[n][:, :, part * width : (part + 1) * width] = source
        else:
            half = sizes.down // 2
            mine = shards[n][me] if names[n] == "inner" else shards[n][me * half : (me + 1) * half]
            pairs[n][me] = mine
            pairs[n][1 - me] = got[n][...]

    def copy(piece, bz, by, bx, kind, own=False):
        target = {
            RIGHT: device_at(z + 1, y, x, core),
            LEFT: device_at(z - 1, y, x, core),
            TO_Y: device_at(z, 1 - y, x, core),
            TO_X: device_at(z, y, 1 - x, core),
            TO_CORE: device_at(z, y, x, other),
        }[kind]
        spot = place(piece, bz, by, bx, core)
        n, cut = pieces[piece]
        slot = chip_index(bz, by, bx)
        return remote(pairs[n].at[cut] if own else spot, spot, send_sem.at[piece, kind, slot],
                      recv_sem.at[piece, 1 if kind == TO_CORE else 0, slot], target)

    def arrive(piece, bz, by, bx, from_core=False):
        spot = place(piece, bz, by, bx, other if from_core else core)
        remote(spot, spot, send_sem.at[piece, 0, 0],
               recv_sem.at[piece, 1 if from_core else 0, chip_index(bz, by, bx)],
               device_at(z, y, x, other)).wait_recv()

    def keep(piece):
        n, cut = pieces[piece]
        return pltpu.make_async_copy(pairs[n].at[cut], place(piece, z, y, x, core),
                                     own_sem.at[piece])

    every = range(len(pieces))
    first, later = every[:count], every[count:]

    def launch(kind):
        for piece in every:
            copy(piece, z, y, x, kind, True).start()

    def begin():
        greet(depth)
        for n in range(count):
            swap(n).start()

    def send_own():
        for n in range(count):
            swap(n).wait_recv()
        for me in range(2):
            @pl.when(core == me)
            def _(me=me):
                for n in range(count):
                    merge(n, me)
        pl.when(z < depth - 1)(lambda: launch(RIGHT))
        pl.when(z > 0)(lambda: launch(LEFT))
        for piece in every:
            copy(piece, z, y, x, TO_Y, True).start()
            copy(piece, z, y, x, TO_X, True).start()
        for piece in every:
            copy(piece, z, y, x, TO_CORE, True).start()
            keep(piece).start()

    def from_z(bz, kind, further):
        for piece in every:
            arrive(piece, bz, y, x)
            pl.when(further)(lambda piece=piece: copy(piece, bz, y, x, kind).start())
            copy(piece, bz, y, x, TO_Y).start()
            copy(piece, bz, y, x, TO_X).start()
            copy(piece, bz, y, x, TO_CORE).start()

    def from_sides(bz):
        for early, late in zip(first, later):
            arrive(early, bz, 1 - y, x)
            copy(early, bz, 1 - y, x, TO_X).start()
            copy(early, bz, 1 - y, x, TO_CORE).start()
            arrive(late, bz, y, 1 - x)
            copy(late, bz, y, 1 - x, TO_Y).start()
            copy(late, bz, y, 1 - x, TO_CORE).start()
        for early, late in zip(first, later):
            arrive(early, bz, y, 1 - x)
            copy(early, bz, y, 1 - x, TO_CORE).start()
            arrive(late, bz, 1 - y, x)
            copy(late, bz, 1 - y, x, TO_CORE).start()

    def from_corner(bz):
        for piece in every:
            arrive(piece, bz, 1 - y, 1 - x)
            copy(piece, bz, 1 - y, 1 - x, TO_CORE).start()

    def both_ways(step, action):
        if step == 0:
            action(z)
            return
        pl.when(z - step >= 0)(lambda: action(z - step))
        pl.when(z + step < depth)(lambda: action(z + step))

    def line(step):
        pl.when(z - step >= 0)(lambda: from_z(z - step, RIGHT, z < depth - 1))
        pl.when(z + step < depth)(lambda: from_z(z + step, LEFT, z > 0))

    def end():
        for n in range(count):
            swap(n).wait_send()
        for piece in every:
            keep(piece).wait()

            @pl.loop(0, depth)
            def _(bz, piece=piece):
                for by in range(2):
                    for bx in range(2):
                        arrive(piece, bz, by, bx, True)
                        copy(piece, bz, by, bx, TO_CORE).wait_send()
                copy(piece, bz, y, x, TO_Y).wait_send()
                copy(piece, bz, y, x, TO_X).wait_send()
                if piece in first:
                    copy(piece, bz, 1 - y, x, TO_X).wait_send()
                else:
                    copy(piece, bz, y, 1 - x, TO_Y).wait_send()
                pl.when((bz <= z) & (z < depth - 1))(
                    lambda: copy(piece, bz, y, x, RIGHT).wait_send())
                pl.when((bz >= z) & (z > 0))(lambda: copy(piece, bz, y, x, LEFT).wait_send())

    stages = [begin, send_own]
    for step in range(1, depth):
        stages.append(functools.partial(line, step))
        stages.append(functools.partial(both_ways, step - 1, from_sides))
    stages.append(functools.partial(both_ways, depth - 1, from_sides))
    for step in range(depth):
        stages.append(functools.partial(both_ways, step, from_corner))
    stages.append(end)
    return stages


def add_rows(target, sources):
    slab = 48

    def total(k):
        at = pl.ds(aligned(k, slab), slab)
        value = sources[0][at].astype(f32)
        for source in sources[1:]:
            value = value + source[at].astype(f32)
        target[at] = value.astype(target.dtype)

    pl.loop(0, target.shape[0] // slab)(total)


def scatter_scratch(sizes, names):
    wave = pltpu.SemaphoreType.DMA
    count, pieces, depth, chips = len(names), 2 * len(names), sizes.depth, sizes.chips

    def buffers(lead, kind):
        return [pltpu.VMEM(lead + (2,) + sizes.piece(name), kind) for name in names]

    return (
        buffers((chips,), bf16) + buffers((chips,), bf16) + buffers((2 * depth,), bf16)
        + buffers((depth,), bf16) + buffers((2, depth), bf16) + buffers((), f32)
        + [pltpu.VMEM(sizes.part(name), f32) for name in names]
        + [pltpu.VMEM(sizes.part(name), f32) for name in names]
        + [wave((pieces, chips))] * 3 + [wave((pieces, 2 * depth))] * 2
        + [wave((pieces, depth))] * 2 + [wave((pieces, 2, depth))] * 2 + [wave((count,))] * 2
    )


def scatter_stages(sizes, names, fulls, owns, scratch):
    count, depth = len(names), sizes.depth
    acc, swapped, first, second, line, sums, outs, ins = (
        scratch[k * count : (k + 1) * count] for k in range(8)
    )
    (load_sem, swap_send, swap_recv, one_send, one_recv, two_send, two_recv, line_send,
     line_recv, end_send, end_recv) = scratch[8 * count :]
    z, y, x, core = where_am_i()
    other = 1 - core
    partner = device_at(z, y, x, other)
    over_x, over_y = device_at(z, y, 1 - x, core), device_at(z, 1 - y, x, core)
    pieces = [(n, cut) for cut in range(2) for n in range(count)]
    every = range(len(pieces))
    order = sorted(range(depth), key=lambda spot: (-abs(2 * spot - depth + 1), -spot))

    def at(buffers, piece, *index):
        n, cut = pieces[piece]
        return buffers[n].at[(*index, cut)]

    def block(piece, bz, by, bx, half):
        n, cut = pieces[piece]
        return sizes.place(names[n], fulls[n], cut, bz, by, bx, half)

    def load(piece, bz, by, bx):
        slot = chip_index(bz, by, bx)
        return pltpu.make_async_copy(block(piece, bz, by, bx, core), at(acc, piece, slot),
                                     load_sem.at[piece, slot])

    def swap(piece, bz, by, bx):
        slot = chip_index(bz, by, bx)
        return remote(block(piece, bz, by, bx, other), at(swapped, piece, slot),
                      swap_send.at[piece, slot], swap_recv.at[piece, slot], partner)

    def turned(piece):
        return pieces[piece][1] == 1

    def stage_one(piece, bz, spot):
        if turned(piece):
            far, device = chip_index(bz, 1 - y, spot), over_y
        else:
            far, device = chip_index(bz, spot, 1 - x), over_x
        slot = 2 * bz + spot
        return remote(at(acc, piece, far), at(first, piece, slot), one_send.at[piece, slot],
                      one_recv.at[piece, slot], device)

    def stage_two(piece, bz):
        if turned(piece):
            far, device = chip_index(bz, y, 1 - x), over_x
        else:
            far, device = chip_index(bz, 1 - y, x), over_y
        return remote(at(acc, piece, far), at(second, piece, bz), two_send.at[piece, bz],
                      two_recv.at[piece, bz], device)

    def along(piece, bz, way):
        device = device_at(z + 1, y, x, core) if way == 0 else device_at(z - 1, y, x, core)
        return remote(at(acc, piece, chip_index(bz, y, x)), at(line, piece, way, bz),
                      line_send.at[piece, way, bz], line_recv.at[piece, way, bz], device)

    def begin():
        greet(depth)
        for bz in order:
            for flip_y, flip_x in ((1, 1), (0, 1), (1, 0), (0, 0)):
                for piece in every:
                    if turned(piece):
                        flip_y, flip_x = flip_x, flip_y
                    by = 1 - y if flip_y else y
                    bx = 1 - x if flip_x else x
                    swap(piece, bz, by, bx).start()
                    load(piece, bz, by, bx).start()
                    if turned(piece):
                        flip_y, flip_x = flip_x, flip_y

    def join(piece, bz, by, bx, extra=()):
        load(piece, bz, by, bx).wait()
        swap(piece, bz, by, bx).wait_recv()
        mine = at(acc, piece, chip_index(bz, by, bx))
        add_rows(mine, (mine, at(swapped, piece, chip_index(bz, by, bx))) + extra)

    def send_first(bz):
        for far in range(2):
            for piece in every:
                if turned(piece):
                    spot = x if far else 1 - x
                    join(piece, bz, 1 - y, spot)
                else:
                    spot = y if far else 1 - y
                    join(piece, bz, spot, 1 - x)
                stage_one(piece, bz, spot).start()

    def send_second(bz):
        for piece in every:
            spot = 1 - x if turned(piece) else 1 - y
            stage_one(piece, bz, spot).wait_recv()
            arrived = (at(first, piece, 2 * bz + spot),)
            if turned(piece):
                join(piece, bz, y, spot, arrived)
            else:
                join(piece, bz, spot, x, arrived)
            stage_two(piece, bz).start()

    def gathered(piece, bz):
        spot = x if turned(piece) else y
        stage_one(piece, bz, spot).wait_recv()
        stage_two(piece, bz).wait_recv()
        load(piece, bz, y, x).wait()
        swap(piece, bz, y, x).wait_recv()
        mine = at(acc, piece, chip_index(bz, y, x))
        return mine, (mine, at(swapped, piece, chip_index(bz, y, x)),
                      at(first, piece, 2 * bz + spot), at(second, piece, bz))

    def pass_on(bz, level, way):
        for piece in every:
            mine, base = gathered(piece, bz)
            if level > 0:
                along(piece, bz, way).wait_recv()
                base = base + (at(line, piece, way, bz),)
            add_rows(mine, base)
            along(piece, bz, way).start()

    def pass_level(bz, level):
        if level < bz:
            pl.when(z == level)(lambda: pass_on(bz, level, 0))
        if depth - 1 - level > bz:
            pl.when(z == depth - 1 - level)(lambda: pass_on(bz, level, 1))

    def finish(bz):
        @pl.when(z == bz)
        def _():
            ways = ((0,) if bz > 0 else ()) + ((1,) if bz < depth - 1 else ())
            for piece in every:
                n, cut = pieces[piece]
                _, base = gathered(piece, bz)
                for way in ways:
                    along(piece, bz, way).wait_recv()
                add_rows(sums[n].at[cut], base + tuple(at(line, piece, way, bz) for way in ways))

    def exchange(n):
        return remote(outs[n], ins[n], end_send.at[n], end_recv.at[n], partner)

    width, half = sizes.width, sizes.down // 2

    def hand_over():
        for me in range(2):
            @pl.when(core == me)
            def _(me=me):
                far = 1 - me
                for n, name in enumerate(names):
                    if name == "inner":
                        outs[n][...] = sums[n][far]
                        owns[n][me] = sums[n][me]
                    elif name == "outer":
                        outs[n][...] = sums[n][far]
                        owns[n][me * half : (me + 1) * half] = sums[n][me]
                    else:
                        outs[n][...] = sums[n][:, :, far * width : (far + 1) * width]
                        owns[n][2 * me : 2 * me + 2] = sums[n][:, :, me * width : (me + 1) * width]
        for n in range(count):
            exchange(n).start()

    def end():
        for n in range(count):
            exchange(n).wait_recv()
        for me in range(2):
            @pl.when(core == me)
            def _(me=me):
                far = 1 - me
                for n, name in enumerate(names):
                    if name == "inner":
                        owns[n][far] = ins[n][...]
                    elif name == "outer":
                        owns[n][far * half : (far + 1) * half] = ins[n][...]
                    else:
                        owns[n][2 * far : 2 * far + 2] = ins[n][...]
        for n in range(count):
            exchange(n).wait_send()
        for piece in every:
            @pl.loop(0, depth)
            def _(bz, piece=piece):
                for by in range(2):
                    for bx in range(2):
                        swap(piece, bz, by, bx).wait_send()
                for spot in range(2):
                    stage_one(piece, bz, spot).wait_send()
                stage_two(piece, bz).wait_send()
                pl.when(z < bz)(lambda: along(piece, bz, 0).wait_send())
                pl.when(z > bz)(lambda: along(piece, bz, 1).wait_send())

    stages = [begin]
    for turn in range(2 * depth + 1):
        if turn < depth:
            stages.append(functools.partial(send_first, order[turn]))
        if 0 <= turn - 1 < depth:
            stages.append(functools.partial(send_second, order[turn - 1]))
        passes = [
            functools.partial(pass_level, order[turn - 2 - level], level)
            for level in range(depth - 1)
            if 0 <= turn - 2 - level < depth
        ]
        if passes:
            stages.append(functools.partial(in_turn, passes))
    stages.append(functools.partial(in_turn, [functools.partial(finish, bz) for bz in order]))
    return stages + [hand_over, end]


def in_turn(actions):
    for action in actions:
        action()


def run_stages(stages, step, steps):
    for number in range(steps):
        mine = [s for k, s in enumerate(stages) if k * steps // len(stages) == number]
        if mine:
            @pl.when(step == number)
            def _(mine=mine):
                for stage in mine:
                    stage()


HBM = pl.BlockSpec(memory_space=pl.ANY)
VMEM = pl.BlockSpec(memory_space=pltpu.VMEM)


def gather_kernel(sizes, names, *refs):
    count = len(names)
    for stage in gather_stages(sizes, names, refs[:count], refs[count : 2 * count],
                               refs[2 * count :]):
        stage()


def gather_blocks(sizes, names, shards):
    return pl.pallas_call(
        functools.partial(gather_kernel, sizes, names),
        out_shape=[jax.ShapeDtypeStruct(sizes.full(name), bf16) for name in names],
        in_specs=[VMEM] * len(names),
        out_specs=[HBM] * len(names),
        scratch_shapes=gather_scratch(sizes, names),
        compiler_params=pltpu.CompilerParams(collective_id=0, has_side_effects=True),
        name="gather_blocks",
    )(*shards)


def gain_stages(depth, gain_ref, gain_out, buf, send, recv):
    z, y, x, core = where_am_i()
    hops = (device_at(z, y, x, 1 - core), device_at(z, y, 1 - x, core),
            device_at(z, 1 - y, x, core))

    def hop(step):
        return remote(buf.at[2 * step], buf.at[2 * step + 1], send.at[step], recv.at[step],
                      hops[step])

    def line(way):
        device = device_at(z + 1, y, x, core) if way == 0 else device_at(z - 1, y, x, core)
        return remote(buf.at[7 + way], buf.at[9 + way], send.at[3 + way], recv.at[3 + way],
                      device)

    def begin():
        buf[0] = gain_ref[...]
        hop(0).start()

    def turn(step):
        hop(step).wait_recv()
        buf[2 * step + 2] = buf[2 * step] + buf[2 * step + 1]
        if step < 2:
            hop(step + 1).start()

    def rightward():
        gain_out[...] = buf[6]

        @pl.when(z > 0)
        def _():
            line(0).wait_recv()
            gain_out[...] = gain_out[...] + buf[9]

        @pl.when(z < depth - 1)
        def _():
            buf[7] = gain_out[...]
            line(0).start()

    def leftward():
        buf[8] = buf[6]

        @pl.when(z < depth - 1)
        def _():
            line(1).wait_recv()
            gain_out[...] = gain_out[...] + buf[10]
            buf[8] = buf[6] + buf[10]

        pl.when(z > 0)(lambda: line(1).start())

    def end():
        for step in range(3):
            hop(step).wait_send()
        pl.when(z < depth - 1)(lambda: line(0).wait_send())
        pl.when(z > 0)(lambda: line(1).wait_send())

    return [begin] + [functools.partial(turn, step) for step in range(3)] + [
        rightward, leftward, end]


def scatter_kernel(sizes, names, *refs):
    count = len(names)
    fulls, gain_ref = refs[:count], refs[count]
    owns, gain_out = refs[count + 1 : 2 * count + 1], refs[2 * count + 1]
    gain_scratch, scratch = refs[2 * count + 2 : 2 * count + 5], refs[2 * count + 5 :]
    stages = scatter_stages(sizes, names, fulls, owns, scratch)
    gains = gain_stages(sizes.depth, gain_ref, gain_out, *gain_scratch)
    stages[0]()
    for number, stage in enumerate(stages[1:]):
        stage()
        if number < len(gains):
            gains[number]()


def scatter_blocks(sizes, names, fulls, gains):
    wave = pltpu.SemaphoreType.DMA
    return pl.pallas_call(
        functools.partial(scatter_kernel, sizes, names),
        out_shape=[jax.ShapeDtypeStruct(sizes.shard(name), f32) for name in names]
        + [jax.ShapeDtypeStruct(gains.shape, f32)],
        in_specs=[HBM] * len(names) + [VMEM],
        out_specs=[VMEM] * (len(names) + 1),
        scratch_shapes=[pltpu.VMEM((11,) + gains.shape, f32), wave((5,)), wave((5,))]
        + scatter_scratch(sizes, names),
        compiler_params=pltpu.CompilerParams(
            collective_id=1, has_side_effects=True, vmem_limit_bytes=60 * 1024 * 1024
        ),
        name="scatter_blocks",
    )(*fulls, gains)


def tile_aligned(down, width, side, deep):
    return (
        lax.axis_size("fsdp") == 4
        and lax.axis_size("dp") % 2 == 0
        and down % 96 == 0
        and width % 48 == 0
        and (2 * width) % 128 == 0
        and side % 128 == 0
        and deep % 128 == 0
    )


def adam_update(weight, mean_old, square_old, gradient, step_rate, decay_rate):
    mean_new = beta_one * mean_old + (1.0 - beta_one) * gradient
    square_new = beta_two * square_old + (1.0 - beta_two) * gradient * gradient
    corrected = (
        mean_new
        / (1.0 - beta_one**STEP)
        / (jnp.sqrt(square_new / (1.0 - beta_two**STEP)) + adam_epsilon)
    )
    master = weight - step_rate * (corrected + decay_rate * weight)
    return (mean_new, square_new, master, master.astype(bf16))


def on_device(
    hidden_in,
    patches,
    token_segments,
    patch_segments,
    cotangent,
    attention_weights,
    attention_means,
    attention_squares,
    inner_weights,
    inner_means,
    inner_squares,
    outer_weights,
    outer_means,
    outer_squares,
    norm_gains,
    gain_means,
    gain_squares,
):
    rows, _, length, _ = hidden_in.shape
    count = patches.shape[2]
    tokens = rows * length
    width, down = attention_weights.shape[1:]
    side, deep = inner_weights.shape[2], outer_weights.shape[0]
    direct = tile_aligned(down, width, side, deep)
    low_inner, low_outer = inner_weights.astype(bf16), outer_weights.astype(bf16)
    if direct:
        sizes = Sizes(down, width, side, deep)
        turned = jnp.swapaxes(attention_weights, 1, 2).astype(bf16)
        low, high = gather_blocks(sizes, ("low", "high"), (turned[:4], turned[4:]))
        rest, rest_shards = ("inner", "outer"), (low_inner, low_outer.T)
        late = ("high",)
    else:
        sizes = None
        weights, inner, outer = gather_weights(
            attention_weights.astype(bf16), low_inner, low_outer
        )
        low, high = weights[:4], weights[4:]
        rest, rest_shards, late = (), (), ()
    gains = lax.all_gather(norm_gains.astype(bf16), "fsdp", axis=1, tiled=True)

    initial = hidden_in.reshape(tokens, D).astype(f32)
    patch_rows = patches.reshape(rows * count, D)
    token_rows = token_segments.reshape(rows, 1, length)
    token_columns = token_segments.reshape(rows, length, 1)
    patch_columns = patch_segments.reshape(rows, count, 1)

    normed_one, unit_one, rms_one = norm_forward(initial, gains[0])
    packed = dot_nt(normed_one, low[0:3].reshape(3 * D, D)).astype(bf16)
    packed = packed.reshape(rows, length, 3 * D)
    mixture_one, lse_one = self_forward(packed, token_rows, token_columns)
    mixed_one = mixture_one.reshape(tokens, D)
    after_one = initial + dot_nt(mixed_one, low[3])
    normed_two, unit_two, rms_two = norm_forward(after_one, gains[1])
    cross_query = dot_nt(normed_two, high[0]).astype(bf16).reshape(rows, length, D)
    mixture_two, lse_two, cross_key, cross_value, *arrived = cross_forward(
        Rider(sizes, rest, "gather", 2), cross_query, patches.reshape(rows, count, D), high,
        token_columns, patch_columns, rest_shards,
    )
    if direct:
        inner, outer = arrived
    mixed_two = mixture_two.reshape(tokens, D)
    after_two = after_one + dot_nt(mixed_two, high[3])
    normed_three, unit_three, rms_three = norm_forward(after_two, gains[2])
    gate = dot_nn(normed_three, inner[0])
    up = dot_nn(normed_three, inner[1])
    units = (gelu_tanh(gate) * up).astype(bf16)
    hidden_out = (after_two + dot_nt(units, outer)).astype(bf16)

    grad_low = cotangent.reshape(tokens, D)
    grad_final = grad_low.astype(f32)
    grad_outer = dot_tn(grad_low, units).astype(bf16)
    grad_units = dot_nn(grad_low, outer)
    activation, gelu_back = jax.vjp(gelu_tanh, gate)
    grad_gate = gelu_back(grad_units * up)[0].astype(bf16)
    grad_up = (grad_units * activation).astype(bf16)
    grad_inner = jnp.stack(
        [dot_tn(normed_three, grad_gate).astype(bf16), dot_tn(normed_three, grad_up).astype(bf16)]
    )
    grad_normed = dot_nt(grad_gate, inner[0]) + dot_nt(grad_up, inner[1])
    grad_from_three, gain_three = norm_backward(grad_normed, gains[2], unit_three, rms_three)
    grad_two = grad_final + grad_from_three
    branch_two = grad_two.astype(bf16)
    grad_mixture_two = dot_nn(branch_two, high[3]).astype(bf16).reshape(rows, length, D)
    grad_cq, grad_ck, grad_cv, *summed_rest = attend_backward(
        cross_backward_kernel, Rider(sizes, rest, "scatter", 3), cross_query, cross_key,
        cross_value, (0, 0), mixture_two, grad_mixture_two, lse_two, token_columns,
        patch_columns, (length, 1), (grad_inner, grad_outer) if direct else (),
        "cross_backward",
    )
    grad_cq = grad_cq.reshape(tokens, D)
    grad_ck = grad_ck.reshape(rows * count, D)
    grad_cv = grad_cv.reshape(rows * count, D)
    grad_high = jnp.stack(
        [
            dot_tn(grad_cq, normed_two).astype(bf16),
            dot_tn(grad_ck, patch_rows).astype(bf16),
            dot_tn(grad_cv, patch_rows).astype(bf16),
            dot_tn(branch_two, mixed_two).astype(bf16),
        ]
    )
    patch_grad = dot_nn(grad_ck, high[1]) + dot_nn(grad_cv, high[2])
    grad_from_two, gain_two = norm_backward(
        dot_nn(grad_cq, high[0]), gains[1], unit_two, rms_two
    )
    grad_one = grad_two + grad_from_two
    branch_one = grad_one.astype(bf16)
    grad_mixture_one = dot_nn(branch_one, low[3]).astype(bf16).reshape(rows, length, D)
    grad_q, grad_k, grad_v, *summed_late = attend_backward(
        self_backward_kernel, Rider(sizes, late, "scatter", 4), packed, packed, packed,
        (PAIRS, 2 * PAIRS), mixture_one, grad_mixture_one, lse_one, token_rows, token_columns,
        (1, length), (grad_high,) if direct else (), "self_backward",
    )
    grad_q = grad_q.reshape(tokens, D)
    grad_k = grad_k.reshape(tokens, D)
    grad_v = grad_v.reshape(tokens, D)
    grad_normed_one = dot_nn(grad_q, low[0]) + dot_nn(grad_k, low[1]) + dot_nn(grad_v, low[2])
    grad_from_one, gain_one = norm_backward(grad_normed_one, gains[0], unit_one, rms_one)
    hidden_grad = grad_one + grad_from_one
    grad_first = jnp.stack(
        [
            dot_tn(grad_q, normed_one).astype(bf16),
            dot_tn(grad_k, normed_one).astype(bf16),
            dot_tn(grad_v, normed_one).astype(bf16),
            dot_tn(branch_one, mixed_one).astype(bf16),
        ]
    )
    gain_grads = jnp.stack([gain_one, gain_two, gain_three])
    if direct:
        own_inner, own_outer = summed_rest
        own_low, gain_totals = scatter_blocks(
            sizes, ("low",), (grad_first,), jnp.pad(gain_grads, ((0, 5), (0, 0)))
        )
        own_attention = jnp.swapaxes(jnp.concatenate([own_low, summed_late[0]]), 1, 2)
        own_outer = own_outer.T
        gain_totals = gain_totals[:3]
    else:
        own_attention, own_inner, own_outer = scatter_grads(
            jnp.concatenate([grad_first, grad_high]), grad_inner, grad_outer
        )
        gain_totals = lax.psum(gain_grads, BOTH)
    width = norm_gains.shape[1]
    own_gains = lax.dynamic_slice_in_dim(
        gain_totals, lax.axis_index("fsdp") * width, width, axis=1
    )

    attention_new = adam_update(
        attention_weights, attention_means, attention_squares, own_attention,
        rate_matrix, decay_matrix,
    )
    inner_new = adam_update(
        inner_weights, inner_means, inner_squares, own_inner, rate_matrix, decay_matrix
    )
    outer_new = adam_update(
        outer_weights, outer_means, outer_squares, own_outer, rate_matrix, decay_matrix
    )
    gain_new = adam_update(norm_gains, gain_means, gain_squares, own_gains, rate_gain, 0.0)
    return (
        hidden_out.reshape(hidden_in.shape),
        hidden_grad.reshape(hidden_in.shape),
        patch_grad.reshape(patches.shape),
        *attention_new,
        *inner_new,
        *outer_new,
        *gain_new,
    )


def solution(mesh):
    rows = P(None, BOTH, None, None)
    ids = P(None, BOTH, None)
    matrix = P(None, "fsdp", "dp")
    down = P("fsdp", "dp")
    gain = P(None, "fsdp")
    return jax.shard_map(
        on_device,
        mesh=mesh,
        in_specs=(rows, rows, ids, ids, rows) + (matrix,) * 6 + (down,) * 3 + (gain,) * 3,
        out_specs=(rows, rows, rows) + (matrix,) * 8 + (down,) * 4 + (gain,) * 4,
        check_vma=False,
    )
```

```python
import functools

import jax
import jax.numpy as jnp
from jax import lax
from jax.experimental import pallas as pl
from jax.experimental.pallas import tpu as pltpu
from jax.sharding import PartitionSpec as P

D = 768
HEADS = 12
HEAD = 64
PAIR = 2 * HEAD
PAIRS = HEADS // 2
STEP = 10
SEGS = 4

epsilon = 1e-06
score_scale = 0.125
masked_value = -1000000000.0
beta_one = 0.9
beta_two = 0.95
adam_epsilon = 1e-08
decay_matrix = 0.1
rate_matrix = 0.1
rate_gain = 0.3
f32 = jnp.float32
bf16 = jnp.bfloat16
BOTH = ("dp", "fsdp")


def gelu_tanh(values):
    return (
        0.5
        * values
        * (1.0 + jnp.tanh(0.7978845608028654 * (values + 0.044715 * values * values * values)))
    )


def dot_nn(a, b):
    return lax.dot_general(a, b, (((1,), (0,)), ((), ())), preferred_element_type=f32)


def dot_nt(a, b):
    return lax.dot_general(a, b, (((1,), (1,)), ((), ())), preferred_element_type=f32)


def dot_tn(a, b):
    return lax.dot_general(a, b, (((0,), (0,)), ((), ())), preferred_element_type=f32)


def norm_forward(values, gain):
    inverse_rms = lax.rsqrt(jnp.mean(values * values, axis=-1, keepdims=True) + epsilon)
    unit_rows = values * inverse_rms
    return ((unit_rows * gain.astype(f32)).astype(bf16), unit_rows, inverse_rms)


def norm_backward(grad_rows, gain, unit_rows, inverse_rms):
    grad_unit = grad_rows * gain.astype(f32)
    grad_values = inverse_rms * (
        grad_unit - unit_rows * jnp.mean(grad_unit * unit_rows, axis=-1, keepdims=True)
    )
    return (grad_values, jnp.sum(grad_rows * unit_rows, axis=0))


def head_half(block, half):
    lane = lax.broadcasted_iota(jnp.int32, block.shape, 1)
    keep = (lane < HEAD) if half == 0 else (lane >= HEAD)
    return jnp.where(keep, block, jnp.zeros_like(block))


def three_parts(column):
    high = column.astype(bf16).astype(f32)
    rest = column - high
    middle = rest.astype(bf16).astype(f32)
    low = rest - middle
    return high, middle, low


def stat_lanes(base, column, first):
    lane = lax.broadcasted_iota(jnp.int32, base.shape, 1)
    for place, part in enumerate(three_parts(column)):
        base = jnp.where(lane == first + place, -part, base)
    return base


def key_marks(key_ids, stats):
    lane = lax.broadcasted_iota(jnp.int32, (key_ids.shape[0], 128), 1)
    marks = lane == key_ids
    if stats:
        marks = marks | ((lane >= SEGS) & (lane < SEGS + 3))
    return jnp.where(marks, 1.0, 0.0).astype(bf16)


def query_bias(query_ids):
    lane = lax.broadcasted_iota(jnp.int32, (query_ids.shape[0], 128), 1)
    return jnp.where((lane == query_ids) | (lane >= SEGS), 0.0, masked_value)


def softmax_columns(scores):
    top = jnp.max(scores, axis=0, keepdims=True)
    raised = jnp.exp(scores - top)
    return raised, top, jnp.sum(raised, axis=0, keepdims=True)


def finish_forward(halves, tops, sums, o_ref, lse_ref):
    mixed = jnp.concatenate([h / s for h, s in zip(halves, sums)], axis=0)
    o_ref[0] = mixed.T.astype(bf16)
    rows = [t + jnp.log(s) for t, s in zip(tops, sums)]
    pad = jnp.zeros((6, rows[0].shape[1]), f32)
    lse_ref[0, 0] = jnp.concatenate(rows + [pad], axis=0)


def cross_forward_kernel(rider, q_ref, c_ref, wk_ref, wv_ref, qid_ref, kid_ref, *refs):
    (o_ref, lse_ref, k_ref, v_ref) = rider.board(refs, 4)
    both = jnp.concatenate([wk_ref[0], wv_ref[0]], axis=0)
    projected = dot_nt(c_ref[0], both).astype(bf16)
    key, value = projected[:, :PAIR], projected[:, PAIR:]
    k_ref[0], v_ref[0] = key, value
    marked = jnp.concatenate([key, key_marks(kid_ref[0], False)], axis=1)
    bias = query_bias(qid_ref[0]).astype(bf16)
    query = q_ref[0] * jnp.asarray(score_scale, bf16)
    values = value.T
    halves, tops, sums = [], [], []
    for half in range(2):
        extended = jnp.concatenate([head_half(query, half), bias], axis=1)
        raised, top, total = softmax_columns(dot_nt(marked, extended))
        halves.append(dot_nn(values[half * HEAD : (half + 1) * HEAD], raised.astype(bf16)))
        tops.append(top)
        sums.append(total)
    finish_forward(halves, tops, sums, o_ref, lse_ref)


def causal_mask(qid_ref, kid_ref):
    length = kid_ref.shape[1]
    key = lax.broadcasted_iota(jnp.int32, (length, length), 0)
    query = lax.broadcasted_iota(jnp.int32, (length, length), 1)
    return (key <= query) & (kid_ref[0] == qid_ref[0])


def self_forward_kernel(q_ref, k_ref, v_ref, qid_ref, kid_ref, o_ref, lse_ref):
    allowed = causal_mask(qid_ref, kid_ref)
    query = q_ref[0] * jnp.asarray(score_scale, bf16)
    key = k_ref[0]
    values = v_ref[0].T
    halves, tops, sums = [], [], []
    for half in range(2):
        scores = jnp.where(allowed, dot_nt(key, head_half(query, half)), masked_value)
        raised, top, total = softmax_columns(scores)
        halves.append(dot_nn(values[half * HEAD : (half + 1) * HEAD], raised.astype(bf16)))
        tops.append(top)
        sums.append(total)
    finish_forward(halves, tops, sums, o_ref, lse_ref)


def backward_pair(q_ref, k_ref, v_ref, o_ref, do_ref, lse_ref, marked, bias, allowed,
                  dq_ref, dk_ref, dv_ref):
    query, grad = q_ref[0], do_ref[0]
    scaled = query * jnp.asarray(score_scale, bf16)
    key_turned = k_ref[0].T
    length = query.shape[0]
    lse_columns = lse_ref[0, 0].T
    product = o_ref[0].astype(f32) * grad.astype(f32)
    ones = key_marks(jnp.full((v_ref.shape[1], 1), -1, jnp.int32), True)
    valued = jnp.concatenate([v_ref[0], ones], axis=1)
    probs, grads, turned = [], [], []
    for half in range(2):
        stats = stat_lanes(bias, lse_columns[:, half : half + 1], SEGS).astype(bf16)
        scores = dot_nt(marked, jnp.concatenate([head_half(scaled, half), stats], axis=1))
        if allowed is not None:
            scores = jnp.where(allowed, scores, masked_value)
        weight = jnp.exp(scores)
        inner = jnp.sum(head_half(product, half), axis=1, keepdims=True)
        delta = stat_lanes(jnp.zeros((length, 128), f32), inner, SEGS).astype(bf16)
        shifted = dot_nt(valued, jnp.concatenate([head_half(grad, half), delta], axis=1))
        grad_scores = (weight * shifted).astype(bf16)
        probs.append(weight.astype(bf16))
        grads.append(grad_scores)
        turned.append(dot_nn(key_turned[half * HEAD : (half + 1) * HEAD], grad_scores))
    dq_ref[0] = (score_scale * jnp.concatenate(turned, axis=0)).T.astype(bf16)
    dv_ref[0] = dot_nn(
        jnp.concatenate(probs, axis=1),
        jnp.concatenate([head_half(grad, 0), head_half(grad, 1)], axis=0),
    ).astype(bf16)
    dk_ref[0] = dot_nn(
        jnp.concatenate(grads, axis=1),
        jnp.concatenate([head_half(scaled, 0), head_half(scaled, 1)], axis=0),
    ).astype(bf16)


def cross_backward_kernel(rider, q_ref, k_ref, v_ref, o_ref, do_ref, lse_ref, qid_ref, kid_ref,
                          *refs):
    dq_ref, dk_ref, dv_ref = rider.board(refs, 3)
    marked = jnp.concatenate([k_ref[0], key_marks(kid_ref[0], True)], axis=1)
    backward_pair(q_ref, k_ref, v_ref, o_ref, do_ref, lse_ref, marked, query_bias(qid_ref[0]),
                  None, dq_ref, dk_ref, dv_ref)


def self_backward_kernel(rider, q_ref, k_ref, v_ref, o_ref, do_ref, lse_ref, qid_ref, kid_ref,
                         *refs):
    dq_ref, dk_ref, dv_ref = rider.board(refs, 3)
    length = k_ref.shape[1]
    ones = key_marks(jnp.full((length, 1), -1, jnp.int32), True)
    marked = jnp.concatenate([k_ref[0], ones], axis=1)
    backward_pair(q_ref, k_ref, v_ref, o_ref, do_ref, lse_ref, marked,
                  jnp.zeros((length, 128), f32), causal_mask(qid_ref, kid_ref),
                  dq_ref, dk_ref, dv_ref)


def pair_spec(length, offset):
    return pl.BlockSpec((1, length, PAIR), lambda row, pair: (row, 0, offset + pair))


def row_spec(shape):
    return pl.BlockSpec((1,) + shape, lambda row, pair: (row, 0, 0))


def stat_spec(length):
    return pl.BlockSpec((1, 1, 8, length), lambda row, pair: (row, pair, 0, 0))


def cost(rows, queries, keys, products):
    elements = rows * HEADS * queries * keys
    return pl.CostEstimate(
        flops=2 * elements * 256 * products // 2,
        transcendentals=elements,
        bytes_accessed=rows * (queries + keys) * D * 2 * 3,
    )


class Rider:
    def __init__(self, sizes, names, kind, number, steps):
        self.sizes, self.names, self.kind, self.number = sizes, names, kind, number
        self.steps = steps

    def board(self, refs, outputs):
        count = len(self.names)
        theirs, mine, scratch = refs[:count], refs[count : count + outputs], refs[count + outputs :]
        if count:
            ends, scratch = scratch[:count], scratch[count:]
            build = gather_stages if self.kind == "gather" else scatter_stages
            stages = build(self.sizes, self.names, theirs, ends, scratch)
            step = pl.program_id(0) * pl.num_programs(1) + pl.program_id(1)
            run_stages(stages, step, self.steps)
        return mine

    def in_specs(self):
        return [VMEM if self.kind == "gather" else HBM] * len(self.names)

    def out_specs(self):
        return [HBM if self.kind == "gather" else VMEM] * len(self.names)

    def out_shape(self):
        if self.kind == "gather":
            return [jax.ShapeDtypeStruct(self.sizes.full(n), bf16) for n in self.names]
        return [jax.ShapeDtypeStruct(self.sizes.shard(n), f32) for n in self.names]

    def scratch(self):
        if not self.names:
            return []
        build = gather_scratch if self.kind == "gather" else scatter_scratch
        return build(self.sizes, self.names)

    def params(self):
        if not self.names:
            return pltpu.CompilerParams()
        return pltpu.CompilerParams(
            collective_id=self.number, has_side_effects=True, vmem_limit_bytes=60 * 1024 * 1024
        )


def self_forward(packed, query_ids, key_ids):
    rows, length = packed.shape[:2]
    return pl.pallas_call(
        self_forward_kernel,
        grid=(rows, PAIRS),
        in_specs=[
            pair_spec(length, 0),
            pair_spec(length, PAIRS),
            pair_spec(length, 2 * PAIRS),
            row_spec((1, length)),
            row_spec((length, 1)),
        ],
        out_specs=[pair_spec(length, 0), stat_spec(length)],
        out_shape=[
            jax.ShapeDtypeStruct((rows, length, D), bf16),
            jax.ShapeDtypeStruct((rows, PAIRS, 8, length), f32),
        ],
        cost_estimate=cost(rows, length, length, 2),
        name="self_forward",
    )(packed, packed, packed, query_ids, key_ids)


def cross_forward(rider, queries, patches, projections, query_ids, key_ids, shards):
    rows, length = queries.shape[:2]
    count = patches.shape[1]

    def slab(which):
        return pl.BlockSpec((1, PAIR, D), lambda row, pair: (which, pair, 0))

    return pl.pallas_call(
        functools.partial(cross_forward_kernel, rider),
        grid=(rows, PAIRS),
        in_specs=[
            pair_spec(length, 0),
            row_spec((count, D)),
            slab(1),
            slab(2),
            row_spec((length, 1)),
            row_spec((count, 1)),
        ]
        + rider.in_specs(),
        out_specs=[
            pair_spec(length, 0), stat_spec(length), pair_spec(count, 0), pair_spec(count, 0),
        ]
        + rider.out_specs(),
        out_shape=[
            jax.ShapeDtypeStruct((rows, length, D), bf16),
            jax.ShapeDtypeStruct((rows, PAIRS, 8, length), f32),
            jax.ShapeDtypeStruct((rows, count, D), bf16),
            jax.ShapeDtypeStruct((rows, count, D), bf16),
        ]
        + rider.out_shape(),
        scratch_shapes=rider.scratch(),
        compiler_params=rider.params(),
        cost_estimate=cost(rows, length, count, 4),
        name="cross_forward",
    )(queries, patches, projections, projections, query_ids, key_ids, *shards)


def attend_backward(kernel, rider, queries, keys, values, offsets, mixed, grad, lse, query_ids,
                    key_ids, query_shape, fulls, name):
    rows, length = grad.shape[:2]
    count = keys.shape[1]
    return pl.pallas_call(
        functools.partial(kernel, rider),
        grid=(rows, PAIRS),
        in_specs=[
            pair_spec(length, 0),
            pair_spec(count, offsets[0]),
            pair_spec(count, offsets[1]),
            pair_spec(length, 0),
            pair_spec(length, 0),
            stat_spec(length),
            row_spec(query_shape),
            row_spec((count, 1)),
        ]
        + rider.in_specs(),
        out_specs=[pair_spec(length, 0), pair_spec(count, 0), pair_spec(count, 0)]
        + rider.out_specs(),
        out_shape=[
            jax.ShapeDtypeStruct((rows, length, D), bf16),
            jax.ShapeDtypeStruct((rows, count, D), bf16),
            jax.ShapeDtypeStruct((rows, count, D), bf16),
        ]
        + rider.out_shape(),
        scratch_shapes=rider.scratch(),
        compiler_params=rider.params(),
        cost_estimate=cost(rows, length, count, 5),
        name=name,
    )(queries, keys, values, mixed, grad, lse, query_ids, key_ids, *fulls)


def gather_weights(attention, inner, outer):
    turned = lax.all_gather(jnp.swapaxes(attention, 1, 2), BOTH, axis=0, tiled=False)
    heads = lax.axis_size("dp"), lax.axis_size("fsdp")
    turned = turned.reshape(heads + turned.shape[1:])
    full_attention = jnp.transpose(turned, (2, 0, 3, 1, 4)).reshape(8, D, D)
    wide = lax.all_gather(inner, BOTH, axis=0, tiled=False)
    wide = wide.reshape(heads + wide.shape[1:])
    full_inner = jnp.transpose(wide, (2, 1, 3, 0, 4)).reshape(2, D, -1)
    tall = lax.all_gather(outer.T, BOTH, axis=0, tiled=False)
    tall = tall.reshape(heads + tall.shape[1:])
    full_outer = jnp.transpose(tall, (0, 2, 1, 3)).reshape(D, -1)
    return full_attention, full_inner, full_outer


def scatter_grads(attention, inner, outer):
    across, within = lax.axis_size("dp"), lax.axis_size("fsdp")
    blocks = attention.reshape(8, across, D // across, within, D // within)
    blocks = jnp.transpose(blocks, (1, 3, 0, 2, 4))
    blocks = blocks.reshape((across * within,) + blocks.shape[2:])
    own_attention = lax.psum_scatter(blocks, BOTH, scatter_dimension=0, tiled=False)
    blocks = inner.reshape(2, within, D // within, across, inner.shape[2] // across)
    blocks = jnp.transpose(blocks, (3, 1, 0, 2, 4))
    blocks = blocks.reshape((across * within,) + blocks.shape[2:])
    own_inner = lax.psum_scatter(blocks, BOTH, scatter_dimension=0, tiled=False)
    blocks = outer.reshape(across, D // across, within, outer.shape[1] // within)
    blocks = jnp.transpose(blocks, (0, 2, 1, 3))
    blocks = blocks.reshape((across * within,) + blocks.shape[2:])
    own_outer = lax.psum_scatter(blocks, BOTH, scatter_dimension=0, tiled=False)
    return (
        jnp.swapaxes(own_attention, 1, 2).astype(f32),
        own_inner.astype(f32),
        own_outer.T.astype(f32),
    )


MESH = pl.DeviceIdType.MESH
RIGHT, LEFT, TO_Y, TO_X, TO_CORE = range(5)


def where_am_i():
    across, within = lax.axis_index("dp"), lax.axis_index("fsdp")
    return across // 2, across % 2, within // 2, within % 2


def device_at(z, y, x, core):
    return (2 * z + y, 2 * x + core)


def aligned(value, unit):
    return pl.multiple_of(value * unit, unit)


class Sizes:
    def __init__(self, down, width, side, deep):
        self.down, self.width, self.side, self.deep = down, width, side, deep
        self.across, self.within = D // down, D // width
        self.depth = self.across // 2
        self.chips = self.across * self.within // 2

    def shard(self, name):
        return {
            "low": (4, self.down, self.width),
            "high": (4, self.down, self.width),
            "inner": (2, self.width, self.side),
            "outer": (self.down, self.deep),
        }[name]

    def full(self, name):
        return {
            "low": (4, D, D),
            "high": (4, D, D),
            "inner": (D, 2 * self.across * self.side),
            "outer": (D, self.within * self.deep),
        }[name]

    def piece(self, name):
        return {
            "low": (self.down, 2 * self.width),
            "high": (self.down, 2 * self.width),
            "inner": (self.width, self.side),
            "outer": (self.down // 2, self.deep),
        }[name]

    def part(self, name):
        return {
            "low": (2, self.down, self.width),
            "high": (2, self.down, self.width),
            "inner": (self.width, self.side),
            "outer": (self.down // 2, self.deep),
        }[name]

    def place(self, name, ref, cut, z, y, x, half):
        place = 2 * z + y
        if name == "inner":
            return ref.at[
                pl.ds(aligned(2 * x + cut, self.width), self.width),
                pl.ds(aligned(half * self.across + place, self.side), self.side),
            ]
        if name == "outer":
            return ref.at[
                pl.ds(aligned(2 * place + half, self.down // 2), self.down // 2),
                pl.ds(aligned(2 * x + cut, self.deep), self.deep),
            ]
        return ref.at[
            2 * half + cut,
            pl.ds(aligned(place, self.down), self.down),
            pl.ds(aligned(x, 2 * self.width), 2 * self.width),
        ]

    def share(self, name, ref, half):
        if name == "inner":
            return ref.at[half]
        if name == "outer":
            return ref.at[pl.ds(aligned(half, self.down // 2), self.down // 2)]
        return ref.at[pl.ds(2 * half, 2)]


def greet(depth):
    z, y, x, core = where_am_i()
    barrier = pltpu.get_barrier_semaphore()

    def signal(device):
        pl.semaphore_signal(barrier, inc=1, device_id=device, device_id_type=MESH)

    signal(device_at(z, y, x, 1 - core))
    signal(device_at(z, y, 1 - x, core))
    signal(device_at(z, 1 - y, x, core))
    pl.when(z > 0)(lambda: signal(device_at(z - 1, y, x, core)))
    pl.when(z < depth - 1)(lambda: signal(device_at(z + 1, y, x, core)))
    pl.semaphore_wait(barrier, 3 + jnp.where(z > 0, 1, 0) + jnp.where(z < depth - 1, 1, 0))


def chip_index(bz, by, bx):
    return (2 * bz + by) * 2 + bx


def remote(src, dst, send, recv, device):
    return pltpu.make_async_remote_copy(
        src_ref=src, dst_ref=dst, send_sem=send, recv_sem=recv, device_id=device,
        device_id_type=MESH)


def gather_scratch(sizes, names):
    wave = pltpu.SemaphoreType.DMA
    count, pieces = len(names), 2 * len(names)
    return (
        [pltpu.VMEM((2,) + sizes.piece(name), bf16) for name in names]
        + [pltpu.VMEM(sizes.part(name), bf16) for name in names]
        + [wave((count,)), wave((count,)), wave((pieces,)), wave((pieces, 5, sizes.chips)),
           wave((pieces, 2, sizes.chips))]
    )


def gather_stages(sizes, names, shards, fulls, scratch):
    count, depth = len(names), sizes.depth
    pairs, got = scratch[:count], scratch[count : 2 * count]
    swap_send, swap_recv, own_sem, send_sem, recv_sem = scratch[2 * count :]
    z, y, x, core = where_am_i()
    other = 1 - core
    pieces = [(n, cut) for cut in range(2) for n in range(count)]

    def place(piece, bz, by, bx, half):
        n, cut = pieces[piece]
        return sizes.place(names[n], fulls[n], cut, bz, by, bx, half)

    def swap(n):
        return remote(sizes.share(names[n], shards[n], other), got[n], swap_send.at[n],
                      swap_recv.at[n], device_at(z, y, x, other))

    def merge(n, me):
        if names[n] in ("low", "high"):
            width = sizes.width
            for part, source in ((me, shards[n][2 * me : 2 * me + 2]), (1 - me, got[n][...])):
                pairs[n][:, :, part * width : (part + 1) * width] = source
        else:
            half = sizes.down // 2
            mine = shards[n][me] if names[n] == "inner" else shards[n][me * half : (me + 1) * half]
            pairs[n][me] = mine
            pairs[n][1 - me] = got[n][...]

    def copy(piece, bz, by, bx, kind, own=False):
        target = {
            RIGHT: device_at(z + 1, y, x, core),
            LEFT: device_at(z - 1, y, x, core),
            TO_Y: device_at(z, 1 - y, x, core),
            TO_X: device_at(z, y, 1 - x, core),
            TO_CORE: device_at(z, y, x, other),
        }[kind]
        spot = place(piece, bz, by, bx, core)
        n, cut = pieces[piece]
        slot = chip_index(bz, by, bx)
        return remote(pairs[n].at[cut] if own else spot, spot, send_sem.at[piece, kind, slot],
                      recv_sem.at[piece, 1 if kind == TO_CORE else 0, slot], target)

    def arrive(piece, bz, by, bx, from_core=False):
        spot = place(piece, bz, by, bx, other if from_core else core)
        remote(spot, spot, send_sem.at[piece, 0, 0],
               recv_sem.at[piece, 1 if from_core else 0, chip_index(bz, by, bx)],
               device_at(z, y, x, other)).wait_recv()

    def keep(piece):
        n, cut = pieces[piece]
        return pltpu.make_async_copy(pairs[n].at[cut], place(piece, z, y, x, core),
                                     own_sem.at[piece])

    every = range(len(pieces))
    first, later = every[:count], every[count:]

    def launch(kind):
        for piece in every:
            copy(piece, z, y, x, kind, True).start()

    def begin():
        greet(depth)
        for n in range(count):
            swap(n).start()

    def send_own():
        for n in range(count):
            swap(n).wait_recv()
        for me in range(2):
            @pl.when(core == me)
            def _(me=me):
                for n in range(count):
                    merge(n, me)
        pl.when(z < depth - 1)(lambda: launch(RIGHT))
        pl.when(z > 0)(lambda: launch(LEFT))
        for piece in every:
            copy(piece, z, y, x, TO_Y, True).start()
            copy(piece, z, y, x, TO_X, True).start()
        for piece in every:
            copy(piece, z, y, x, TO_CORE, True).start()
            keep(piece).start()

    def from_z(bz, kind, further):
        for piece in every:
            arrive(piece, bz, y, x)
            pl.when(further)(lambda piece=piece: copy(piece, bz, y, x, kind).start())
            copy(piece, bz, y, x, TO_Y).start()
            copy(piece, bz, y, x, TO_X).start()
            copy(piece, bz, y, x, TO_CORE).start()

    def from_sides(bz):
        for early, late in zip(first, later):
            arrive(early, bz, 1 - y, x)
            copy(early, bz, 1 - y, x, TO_X).start()
            copy(early, bz, 1 - y, x, TO_CORE).start()
            arrive(late, bz, y, 1 - x)
            copy(late, bz, y, 1 - x, TO_Y).start()
            copy(late, bz, y, 1 - x, TO_CORE).start()
        for early, late in zip(first, later):
            arrive(early, bz, y, 1 - x)
            copy(early, bz, y, 1 - x, TO_CORE).start()
            arrive(late, bz, 1 - y, x)
            copy(late, bz, 1 - y, x, TO_CORE).start()

    def from_corner(bz):
        for piece in every:
            arrive(piece, bz, 1 - y, 1 - x)
            copy(piece, bz, 1 - y, 1 - x, TO_CORE).start()

    def both_ways(step, action):
        if step == 0:
            action(z)
            return
        pl.when(z - step >= 0)(lambda: action(z - step))
        pl.when(z + step < depth)(lambda: action(z + step))

    def line(step):
        pl.when(z - step >= 0)(lambda: from_z(z - step, RIGHT, z < depth - 1))
        pl.when(z + step < depth)(lambda: from_z(z + step, LEFT, z > 0))

    def end():
        for n in range(count):
            swap(n).wait_send()
        for piece in every:
            keep(piece).wait()

            @pl.loop(0, depth)
            def _(bz, piece=piece):
                for by in range(2):
                    for bx in range(2):
                        arrive(piece, bz, by, bx, True)
                        copy(piece, bz, by, bx, TO_CORE).wait_send()
                copy(piece, bz, y, x, TO_Y).wait_send()
                copy(piece, bz, y, x, TO_X).wait_send()
                if piece in first:
                    copy(piece, bz, 1 - y, x, TO_X).wait_send()
                else:
                    copy(piece, bz, y, 1 - x, TO_Y).wait_send()
                pl.when((bz <= z) & (z < depth - 1))(
                    lambda: copy(piece, bz, y, x, RIGHT).wait_send())
                pl.when((bz >= z) & (z > 0))(lambda: copy(piece, bz, y, x, LEFT).wait_send())

    stages = [begin, send_own]
    for step in range(1, depth):
        stages.append(functools.partial(line, step))
        stages.append(functools.partial(both_ways, step - 1, from_sides))
    stages.append(functools.partial(both_ways, depth - 1, from_sides))
    for step in range(depth):
        stages.append(functools.partial(both_ways, step, from_corner))
    stages.append(end)
    return stages


def add_rows(target, sources):
    slab = 48

    def total(k):
        at = pl.ds(aligned(k, slab), slab)
        value = sources[0][at].astype(f32)
        for source in sources[1:]:
            value = value + source[at].astype(f32)
        target[at] = value.astype(target.dtype)

    pl.loop(0, target.shape[0] // slab)(total)


def scatter_scratch(sizes, names):
    wave = pltpu.SemaphoreType.DMA
    count, pieces, depth, chips = len(names), 2 * len(names), sizes.depth, sizes.chips

    def buffers(lead, kind):
        return [pltpu.VMEM(lead + (2,) + sizes.piece(name), kind) for name in names]

    return (
        buffers((chips,), bf16) + buffers((chips,), bf16) + buffers((2 * depth,), bf16)
        + buffers((depth,), bf16) + buffers((2, depth), bf16) + buffers((), f32)
        + [pltpu.VMEM(sizes.part(name), f32) for name in names]
        + [pltpu.VMEM(sizes.part(name), f32) for name in names]
        + [wave((pieces, chips))] * 3 + [wave((pieces, 2 * depth))] * 2
        + [wave((pieces, depth))] * 2 + [wave((pieces, 2, depth))] * 2 + [wave((count,))] * 2
    )


def scatter_stages(sizes, names, fulls, owns, scratch):
    count, depth = len(names), sizes.depth
    acc, swapped, first, second, line, sums, outs, ins = (
        scratch[k * count : (k + 1) * count] for k in range(8)
    )
    (load_sem, swap_send, swap_recv, one_send, one_recv, two_send, two_recv, line_send,
     line_recv, end_send, end_recv) = scratch[8 * count :]
    z, y, x, core = where_am_i()
    other = 1 - core
    partner = device_at(z, y, x, other)
    over_x, over_y = device_at(z, y, 1 - x, core), device_at(z, 1 - y, x, core)
    pieces = [(n, cut) for cut in range(2) for n in range(count)]
    every = range(len(pieces))
    order = sorted(range(depth), key=lambda spot: (-abs(2 * spot - depth + 1), -spot))

    def at(buffers, piece, *index):
        n, cut = pieces[piece]
        return buffers[n].at[(*index, cut)]

    def block(piece, bz, by, bx, half):
        n, cut = pieces[piece]
        return sizes.place(names[n], fulls[n], cut, bz, by, bx, half)

    def load(piece, bz, by, bx):
        slot = chip_index(bz, by, bx)
        return pltpu.make_async_copy(block(piece, bz, by, bx, core), at(acc, piece, slot),
                                     load_sem.at[piece, slot])

    def swap(piece, bz, by, bx):
        slot = chip_index(bz, by, bx)
        return remote(block(piece, bz, by, bx, other), at(swapped, piece, slot),
                      swap_send.at[piece, slot], swap_recv.at[piece, slot], partner)

    def turned(piece):
        return pieces[piece][1] == 1

    def stage_one(piece, bz, spot):
        if turned(piece):
            far, device = chip_index(bz, 1 - y, spot), over_y
        else:
            far, device = chip_index(bz, spot, 1 - x), over_x
        slot = 2 * bz + spot
        return remote(at(acc, piece, far), at(first, piece, slot), one_send.at[piece, slot],
                      one_recv.at[piece, slot], device)

    def stage_two(piece, bz):
        if turned(piece):
            far, device = chip_index(bz, y, 1 - x), over_x
        else:
            far, device = chip_index(bz, 1 - y, x), over_y
        return remote(at(acc, piece, far), at(second, piece, bz), two_send.at[piece, bz],
                      two_recv.at[piece, bz], device)

    def along(piece, bz, way):
        device = device_at(z + 1, y, x, core) if way == 0 else device_at(z - 1, y, x, core)
        return remote(at(acc, piece, chip_index(bz, y, x)), at(line, piece, way, bz),
                      line_send.at[piece, way, bz], line_recv.at[piece, way, bz], device)

    def begin():
        greet(depth)
        for bz in order:
            for flip_y, flip_x in ((1, 1), (0, 1), (1, 0), (0, 0)):
                for piece in every:
                    if turned(piece):
                        flip_y, flip_x = flip_x, flip_y
                    by = 1 - y if flip_y else y
                    bx = 1 - x if flip_x else x
                    swap(piece, bz, by, bx).start()
                    load(piece, bz, by, bx).start()
                    if turned(piece):
                        flip_y, flip_x = flip_x, flip_y

    def join(piece, bz, by, bx, extra=()):
        load(piece, bz, by, bx).wait()
        swap(piece, bz, by, bx).wait_recv()
        mine = at(acc, piece, chip_index(bz, by, bx))
        add_rows(mine, (mine, at(swapped, piece, chip_index(bz, by, bx))) + extra)

    def send_first(bz):
        for far in range(2):
            for piece in every:
                if turned(piece):
                    spot = x if far else 1 - x
                    join(piece, bz, 1 - y, spot)
                else:
                    spot = y if far else 1 - y
                    join(piece, bz, spot, 1 - x)
                stage_one(piece, bz, spot).start()

    def send_second(bz):
        for piece in every:
            spot = 1 - x if turned(piece) else 1 - y
            stage_one(piece, bz, spot).wait_recv()
            arrived = (at(first, piece, 2 * bz + spot),)
            if turned(piece):
                join(piece, bz, y, spot, arrived)
            else:
                join(piece, bz, spot, x, arrived)
            stage_two(piece, bz).start()

    def gathered(piece, bz):
        spot = x if turned(piece) else y
        stage_one(piece, bz, spot).wait_recv()
        stage_two(piece, bz).wait_recv()
        load(piece, bz, y, x).wait()
        swap(piece, bz, y, x).wait_recv()
        mine = at(acc, piece, chip_index(bz, y, x))
        return mine, (mine, at(swapped, piece, chip_index(bz, y, x)),
                      at(first, piece, 2 * bz + spot), at(second, piece, bz))

    def pass_on(bz, level, way):
        for piece in every:
            mine, base = gathered(piece, bz)
            if level > 0:
                along(piece, bz, way).wait_recv()
                base = base + (at(line, piece, way, bz),)
            add_rows(mine, base)
            along(piece, bz, way).start()

    def pass_level(bz, level):
        if level < bz:
            pl.when(z == level)(lambda: pass_on(bz, level, 0))
        if depth - 1 - level > bz:
            pl.when(z == depth - 1 - level)(lambda: pass_on(bz, level, 1))

    def finish(bz):
        @pl.when(z == bz)
        def _():
            ways = ((0,) if bz > 0 else ()) + ((1,) if bz < depth - 1 else ())
            for piece in every:
                n, cut = pieces[piece]
                _, base = gathered(piece, bz)
                for way in ways:
                    along(piece, bz, way).wait_recv()
                add_rows(sums[n].at[cut], base + tuple(at(line, piece, way, bz) for way in ways))

    def exchange(n):
        return remote(outs[n], ins[n], end_send.at[n], end_recv.at[n], partner)

    width, half = sizes.width, sizes.down // 2

    def hand_over():
        for me in range(2):
            @pl.when(core == me)
            def _(me=me):
                far = 1 - me
                for n, name in enumerate(names):
                    if name == "inner":
                        outs[n][...] = sums[n][far]
                        owns[n][me] = sums[n][me]
                    elif name == "outer":
                        outs[n][...] = sums[n][far]
                        owns[n][me * half : (me + 1) * half] = sums[n][me]
                    else:
                        outs[n][...] = sums[n][:, :, far * width : (far + 1) * width]
                        owns[n][2 * me : 2 * me + 2] = sums[n][:, :, me * width : (me + 1) * width]
        for n in range(count):
            exchange(n).start()

    def end():
        for n in range(count):
            exchange(n).wait_recv()
        for me in range(2):
            @pl.when(core == me)
            def _(me=me):
                far = 1 - me
                for n, name in enumerate(names):
                    if name == "inner":
                        owns[n][far] = ins[n][...]
                    elif name == "outer":
                        owns[n][far * half : (far + 1) * half] = ins[n][...]
                    else:
                        owns[n][2 * far : 2 * far + 2] = ins[n][...]
        for n in range(count):
            exchange(n).wait_send()
        for piece in every:
            @pl.loop(0, depth)
            def _(bz, piece=piece):
                for by in range(2):
                    for bx in range(2):
                        swap(piece, bz, by, bx).wait_send()
                for spot in range(2):
                    stage_one(piece, bz, spot).wait_send()
                stage_two(piece, bz).wait_send()
                pl.when(z < bz)(lambda: along(piece, bz, 0).wait_send())
                pl.when(z > bz)(lambda: along(piece, bz, 1).wait_send())

    stages = [begin]
    for turn in range(2 * depth + 1):
        if turn < depth:
            stages.append(functools.partial(send_first, order[turn]))
        if 0 <= turn - 1 < depth:
            stages.append(functools.partial(send_second, order[turn - 1]))
        passes = [
            functools.partial(pass_level, order[turn - 2 - level], level)
            for level in range(depth - 1)
            if 0 <= turn - 2 - level < depth
        ]
        if passes:
            stages.append(functools.partial(in_turn, passes))
    stages.append(functools.partial(in_turn, [functools.partial(finish, bz) for bz in order]))
    return stages + [hand_over, end]


def in_turn(actions):
    for action in actions:
        action()


def run_stages(stages, step, steps):
    for number in range(steps):
        mine = [s for k, s in enumerate(stages) if k * steps // len(stages) == number]
        if mine:
            @pl.when(step == number)
            def _(mine=mine):
                for stage in mine:
                    stage()


HBM = pl.BlockSpec(memory_space=pl.ANY)
VMEM = pl.BlockSpec(memory_space=pltpu.VMEM)


def gather_kernel(sizes, names, *refs):
    count = len(names)
    gain_ref, gain_out, send, recv = refs[count], refs[2 * count + 1], *refs[-2:]
    stages = gather_stages(sizes, names, refs[:count], refs[count + 1 : 2 * count + 1],
                           refs[2 * count + 2 : -2])
    z, y, x, core = where_am_i()
    mine, near = 2 * x + core, 2 * x + 1 - core
    far, corner = 2 * (1 - x) + core, 2 * (1 - x) + 1 - core

    def pass_gain(src, slot, kind, device):
        return remote(src, gain_out.at[slot], send.at[kind], recv.at[kind], device)

    partner, beside = device_at(z, y, x, 1 - core), device_at(z, y, 1 - x, core)
    hops = (
        (gain_ref, mine, 0, partner),
        (gain_ref, mine, 1, beside),
        (gain_out.at[near], near, 2, beside),
    )
    stages[0]()
    gain_out[mine] = gain_ref[...]
    pass_gain(*hops[0]).start()
    pass_gain(*hops[1]).start()
    stages[1]()
    pass_gain(gain_ref, near, 0, partner).wait_recv()
    pass_gain(*hops[2]).start()
    for stage in stages[2:]:
        stage()
    pass_gain(gain_ref, far, 1, beside).wait_recv()
    pass_gain(gain_ref, corner, 2, beside).wait_recv()
    for hop in hops:
        pass_gain(*hop).wait_send()


def gather_blocks(sizes, names, shards, gain):
    wave = pltpu.SemaphoreType.DMA
    return pl.pallas_call(
        functools.partial(gather_kernel, sizes, names),
        out_shape=[jax.ShapeDtypeStruct(sizes.full(name), bf16) for name in names]
        + [jax.ShapeDtypeStruct((sizes.within,) + gain.shape, f32)],
        in_specs=[VMEM] * (len(names) + 1),
        out_specs=[HBM] * len(names) + [VMEM],
        scratch_shapes=gather_scratch(sizes, names) + [wave((3,)), wave((3,))],
        compiler_params=pltpu.CompilerParams(collective_id=0, has_side_effects=True),
        name="gather_blocks",
    )(*shards, gain)


def gain_stages(depth, gain_ref, gain_out, buf, send, recv):
    z, y, x, core = where_am_i()
    hops = (device_at(z, y, x, 1 - core), device_at(z, y, 1 - x, core),
            device_at(z, 1 - y, x, core))

    def hop(step):
        return remote(buf.at[2 * step], buf.at[2 * step + 1], send.at[step], recv.at[step],
                      hops[step])

    def line(way):
        device = device_at(z + 1, y, x, core) if way == 0 else device_at(z - 1, y, x, core)
        return remote(buf.at[7 + way], buf.at[9 + way], send.at[3 + way], recv.at[3 + way],
                      device)

    def begin():
        buf[0] = gain_ref[...]
        hop(0).start()

    def turn(step):
        hop(step).wait_recv()
        buf[2 * step + 2] = buf[2 * step] + buf[2 * step + 1]
        if step < 2:
            hop(step + 1).start()

    def rightward():
        gain_out[...] = buf[6]

        @pl.when(z > 0)
        def _():
            line(0).wait_recv()
            gain_out[...] = gain_out[...] + buf[9]

        @pl.when(z < depth - 1)
        def _():
            buf[7] = gain_out[...]
            line(0).start()

    def leftward():
        buf[8] = buf[6]

        @pl.when(z < depth - 1)
        def _():
            line(1).wait_recv()
            gain_out[...] = gain_out[...] + buf[10]
            buf[8] = buf[6] + buf[10]

        pl.when(z > 0)(lambda: line(1).start())

    def end():
        for step in range(3):
            hop(step).wait_send()
        pl.when(z < depth - 1)(lambda: line(0).wait_send())
        pl.when(z > 0)(lambda: line(1).wait_send())

    return [begin] + [functools.partial(turn, step) for step in range(3)] + [
        rightward, leftward, end]


def scatter_kernel(sizes, names, k_ref, v_ref, wk_ref, wv_ref, *refs):
    count = len(names)
    fulls, gain_ref, grad_ref = refs[:count], refs[count], refs[count + 1]
    owns, gain_out = refs[count + 2 : 2 * count + 2], refs[2 * count + 2]
    gain_scratch, scratch = refs[2 * count + 3 : 2 * count + 6], refs[2 * count + 6 :]
    stages = scatter_stages(sizes, names, fulls, owns, scratch)
    gains = gain_stages(sizes.depth, gain_ref, gain_out, *gain_scratch)
    joined = [stages[0]]
    for number, stage in enumerate(stages[1:]):
        joined.append(functools.partial(in_turn, [stage] + gains[number : number + 1]))
    run_stages(joined, pl.program_id(0), pl.num_programs(0))
    grad_ref[...] = dot_nn(k_ref[...], wk_ref[0]) + dot_nn(v_ref[...], wv_ref[0])


def scatter_blocks(sizes, names, fulls, gains, grad_key, grad_value, projections):
    wave = pltpu.SemaphoreType.DMA
    slab = 256
    rows = pl.BlockSpec((slab, D), lambda step: (step, 0))

    def matrix(which):
        return pl.BlockSpec((1, D, D), lambda step: (which, 0, 0))

    return pl.pallas_call(
        functools.partial(scatter_kernel, sizes, names),
        grid=(grad_key.shape[0] // slab,),
        out_shape=[jax.ShapeDtypeStruct(grad_key.shape, f32)]
        + [jax.ShapeDtypeStruct(sizes.shard(name), f32) for name in names]
        + [jax.ShapeDtypeStruct(gains.shape, f32)],
        in_specs=[rows, rows, matrix(1), matrix(2)] + [HBM] * len(names) + [VMEM],
        out_specs=[rows] + [VMEM] * (len(names) + 1),
        scratch_shapes=[pltpu.VMEM((11,) + gains.shape, f32), wave((5,)), wave((5,))]
        + scatter_scratch(sizes, names),
        compiler_params=pltpu.CompilerParams(
            collective_id=1, has_side_effects=True, vmem_limit_bytes=60 * 1024 * 1024
        ),
        name="scatter_blocks",
    )(grad_key, grad_value, projections, projections, *fulls, gains)


def tile_aligned(down, width, side, deep):
    return (
        lax.axis_size("fsdp") == 4
        and lax.axis_size("dp") % 2 == 0
        and down % 96 == 0
        and width % 48 == 0
        and (2 * width) % 128 == 0
        and side % 128 == 0
        and deep % 128 == 0
    )


def adam_update(weight, mean_old, square_old, gradient, step_rate, decay_rate):
    mean_new = beta_one * mean_old + (1.0 - beta_one) * gradient
    square_new = beta_two * square_old + (1.0 - beta_two) * gradient * gradient
    corrected = (
        mean_new
        / (1.0 - beta_one**STEP)
        / (jnp.sqrt(square_new / (1.0 - beta_two**STEP)) + adam_epsilon)
    )
    master = weight - step_rate * (corrected + decay_rate * weight)
    return (mean_new, square_new, master, master.astype(bf16))


def on_device(
    hidden_in,
    patches,
    token_segments,
    patch_segments,
    cotangent,
    attention_weights,
    attention_means,
    attention_squares,
    inner_weights,
    inner_means,
    inner_squares,
    outer_weights,
    outer_means,
    outer_squares,
    norm_gains,
    gain_means,
    gain_squares,
):
    rows, _, length, _ = hidden_in.shape
    count = patches.shape[2]
    tokens = rows * length
    width, down = attention_weights.shape[1:]
    side, deep = inner_weights.shape[2], outer_weights.shape[0]
    direct = tile_aligned(down, width, side, deep)
    low_inner, low_outer = inner_weights.astype(bf16), outer_weights.astype(bf16)
    if direct:
        sizes = Sizes(down, width, side, deep)
        turned = jnp.swapaxes(attention_weights, 1, 2).astype(bf16)
        parts = norm_gains.shape[1]
        gain_block = jnp.pad(
            norm_gains.astype(bf16).astype(f32), ((0, 8 - norm_gains.shape[0]), (0, -parts % 128))
        )
        low, high, gains = gather_blocks(
            sizes, ("low", "high"), (turned[:4], turned[4:]), gain_block
        )
        gains = jnp.swapaxes(gains[:, : norm_gains.shape[0], :parts], 0, 1).reshape(-1, D)
        rest, rest_shards = ("inner", "outer"), (low_inner, low_outer.T)
    else:
        sizes = None
        gains = lax.all_gather(norm_gains.astype(bf16), "fsdp", axis=1, tiled=True)
        weights, inner, outer = gather_weights(
            attention_weights.astype(bf16), low_inner, low_outer
        )
        low, high = weights[:4], weights[4:]
        inner = jnp.concatenate([inner[0], inner[1]], axis=1)
        rest, rest_shards = (), ()

    initial = hidden_in.reshape(tokens, D).astype(f32)
    patch_rows = patches.reshape(rows * count, D)
    token_rows = token_segments.reshape(rows, 1, length)
    token_columns = token_segments.reshape(rows, length, 1)
    patch_columns = patch_segments.reshape(rows, count, 1)

    normed_one, unit_one, rms_one = norm_forward(initial, gains[0])
    packed = dot_nt(normed_one, low[0:3].reshape(3 * D, D)).astype(bf16)
    packed = packed.reshape(rows, length, 3 * D)
    mixture_one, lse_one = self_forward(packed, token_rows, token_columns)
    mixed_one = mixture_one.reshape(tokens, D)
    after_one = initial + dot_nt(mixed_one, low[3])
    normed_two, unit_two, rms_two = norm_forward(after_one, gains[1])
    cross_query = dot_nt(normed_two, high[0]).astype(bf16).reshape(rows, length, D)
    mixture_two, lse_two, cross_key, cross_value, *arrived = cross_forward(
        Rider(sizes, rest, "gather", 2, rows * PAIRS), cross_query, patches.reshape(rows, count, D), high,
        token_columns, patch_columns, rest_shards,
    )
    if direct:
        inner, outer = arrived
    mixed_two = mixture_two.reshape(tokens, D)
    after_two = after_one + dot_nt(mixed_two, high[3])
    normed_three, unit_three, rms_three = norm_forward(after_two, gains[2])
    gated = dot_nn(normed_three, inner)
    hidden_units = outer.shape[1]
    gate, up = gated[:, :hidden_units], gated[:, hidden_units:]
    units = (gelu_tanh(gate) * up).astype(bf16)
    hidden_out = (after_two + dot_nt(units, outer)).astype(bf16)

    grad_low = cotangent.reshape(tokens, D)
    grad_final = grad_low.astype(f32)
    grad_outer = dot_tn(grad_low, units).astype(bf16)
    grad_units = dot_nn(grad_low, outer)
    activation, gelu_back = jax.vjp(gelu_tanh, gate)
    grad_gated = jnp.concatenate(
        [gelu_back(grad_units * up)[0], grad_units * activation], axis=1
    ).astype(bf16)
    grad_inner = dot_tn(normed_three, grad_gated).astype(bf16)
    grad_normed = dot_nt(grad_gated, inner)
    grad_from_three, gain_three = norm_backward(grad_normed, gains[2], unit_three, rms_three)
    grad_two = grad_final + grad_from_three
    branch_two = grad_two.astype(bf16)
    grad_mixture_two = dot_nn(branch_two, high[3]).astype(bf16).reshape(rows, length, D)
    grad_cq, grad_ck, grad_cv, *summed_rest = attend_backward(
        cross_backward_kernel, Rider(sizes, rest, "scatter", 3, rows * PAIRS), cross_query, cross_key,
        cross_value, (0, 0), mixture_two, grad_mixture_two, lse_two, token_columns,
        patch_columns, (length, 1), (grad_inner, grad_outer) if direct else (),
        "cross_backward",
    )
    grad_cq = grad_cq.reshape(tokens, D)
    grad_ck = grad_ck.reshape(rows * count, D)
    grad_cv = grad_cv.reshape(rows * count, D)
    grad_high = jnp.stack(
        [
            dot_tn(grad_cq, normed_two).astype(bf16),
            dot_tn(grad_ck, patch_rows).astype(bf16),
            dot_tn(grad_cv, patch_rows).astype(bf16),
            dot_tn(branch_two, mixed_two).astype(bf16),
        ]
    )
    grad_from_two, gain_two = norm_backward(
        dot_nn(grad_cq, high[0]), gains[1], unit_two, rms_two
    )
    grad_one = grad_two + grad_from_two
    branch_one = grad_one.astype(bf16)
    grad_mixture_one = dot_nn(branch_one, low[3]).astype(bf16).reshape(rows, length, D)
    grad_q, grad_k, grad_v = attend_backward(
        self_backward_kernel, Rider(sizes, (), "scatter", 4, rows * PAIRS), packed, packed,
        packed, (PAIRS, 2 * PAIRS), mixture_one, grad_mixture_one, lse_one, token_rows,
        token_columns, (1, length), (), "self_backward",
    )
    grad_q = grad_q.reshape(tokens, D)
    grad_k = grad_k.reshape(tokens, D)
    grad_v = grad_v.reshape(tokens, D)
    grad_normed_one = dot_nn(grad_q, low[0]) + dot_nn(grad_k, low[1]) + dot_nn(grad_v, low[2])
    grad_from_one, gain_one = norm_backward(grad_normed_one, gains[0], unit_one, rms_one)
    hidden_grad = grad_one + grad_from_one
    grad_first = jnp.stack(
        [
            dot_tn(grad_q, normed_one).astype(bf16),
            dot_tn(grad_k, normed_one).astype(bf16),
            dot_tn(grad_v, normed_one).astype(bf16),
            dot_tn(branch_one, mixed_one).astype(bf16),
        ]
    )
    gain_grads = jnp.stack([gain_one, gain_two, gain_three])
    if direct:
        own_inner, own_outer = summed_rest
        patch_grad, own_low, own_high, gain_totals = scatter_blocks(
            sizes, ("low", "high"), (grad_first, grad_high),
            jnp.pad(gain_grads, ((0, 5), (0, 0))), grad_ck, grad_cv, high,
        )
        own_attention = jnp.swapaxes(jnp.concatenate([own_low, own_high]), 1, 2)
        own_outer = own_outer.T
        gain_totals = gain_totals[:3]
    else:
        patch_grad = dot_nn(grad_ck, high[1]) + dot_nn(grad_cv, high[2])
        own_attention, own_inner, own_outer = scatter_grads(
            jnp.concatenate([grad_first, grad_high]),
            jnp.stack([grad_inner[:, :hidden_units], grad_inner[:, hidden_units:]]),
            grad_outer,
        )
        gain_totals = lax.psum(gain_grads, BOTH)
    width = norm_gains.shape[1]
    own_gains = lax.dynamic_slice_in_dim(
        gain_totals, lax.axis_index("fsdp") * width, width, axis=1
    )

    attention_new = adam_update(
        attention_weights, attention_means, attention_squares, own_attention,
        rate_matrix, decay_matrix,
    )
    inner_new = adam_update(
        inner_weights, inner_means, inner_squares, own_inner, rate_matrix, decay_matrix
    )
    outer_new = adam_update(
        outer_weights, outer_means, outer_squares, own_outer, rate_matrix, decay_matrix
    )
    gain_new = adam_update(norm_gains, gain_means, gain_squares, own_gains, rate_gain, 0.0)
    return (
        hidden_out.reshape(hidden_in.shape),
        hidden_grad.reshape(hidden_in.shape),
        patch_grad.reshape(patches.shape),
        *attention_new,
        *inner_new,
        *outer_new,
        *gain_new,
    )


def solution(mesh):
    rows = P(None, BOTH, None, None)
    ids = P(None, BOTH, None)
    matrix = P(None, "fsdp", "dp")
    down = P("fsdp", "dp")
    gain = P(None, "fsdp")
    return jax.shard_map(
        on_device,
        mesh=mesh,
        in_specs=(rows, rows, ids, ids, rows) + (matrix,) * 6 + (down,) * 3 + (gain,) * 3,
        out_specs=(rows, rows, rows) + (matrix,) * 8 + (down,) * 4 + (gain,) * 4,
        check_vma=False,
    )
```

```python
import functools

import jax
import jax.numpy as jnp
from jax import lax
from jax.experimental import pallas as pl
from jax.experimental.pallas import tpu as pltpu
from jax.sharding import PartitionSpec as P

D = 768
HEADS = 12
HEAD = 64
PAIR = 2 * HEAD
PAIRS = HEADS // 2
GROUP = 3
STEP = 10
SEGS = 4

epsilon = 1e-06
score_scale = 0.125
masked_value = -1000000000.0
beta_one = 0.9
beta_two = 0.95
adam_epsilon = 1e-08
decay_matrix = 0.1
rate_matrix = 0.1
rate_gain = 0.3
f32 = jnp.float32
bf16 = jnp.bfloat16
BOTH = ("dp", "fsdp")


def gelu_tanh(values):
    return (
        0.5
        * values
        * (1.0 + jnp.tanh(0.7978845608028654 * (values + 0.044715 * values * values * values)))
    )


def dot_nn(a, b):
    return lax.dot_general(a, b, (((1,), (0,)), ((), ())), preferred_element_type=f32)


def dot_nt(a, b):
    return lax.dot_general(a, b, (((1,), (1,)), ((), ())), preferred_element_type=f32)


def dot_tn(a, b):
    return lax.dot_general(a, b, (((0,), (0,)), ((), ())), preferred_element_type=f32)


def norm_forward(values, gain):
    inverse_rms = lax.rsqrt(jnp.mean(values * values, axis=-1, keepdims=True) + epsilon)
    unit_rows = values * inverse_rms
    return ((unit_rows * gain.astype(f32)).astype(bf16), unit_rows, inverse_rms)


def norm_backward(grad_rows, gain, unit_rows, inverse_rms):
    grad_unit = grad_rows * gain.astype(f32)
    grad_values = inverse_rms * (
        grad_unit - unit_rows * jnp.mean(grad_unit * unit_rows, axis=-1, keepdims=True)
    )
    return (grad_values, jnp.sum(grad_rows * unit_rows, axis=0))


def head_half(block, half):
    lane = lax.broadcasted_iota(jnp.int32, block.shape, 1)
    keep = (lane < HEAD) if half == 0 else (lane >= HEAD)
    return jnp.where(keep, block, jnp.zeros_like(block))


def three_parts(column):
    high = column.astype(bf16).astype(f32)
    rest = column - high
    middle = rest.astype(bf16).astype(f32)
    low = rest - middle
    return high, middle, low


def stat_lanes(base, column, first):
    lane = lax.broadcasted_iota(jnp.int32, base.shape, 1)
    for place, part in enumerate(three_parts(column)):
        base = jnp.where(lane == first + place, -part, base)
    return base


def key_marks(key_ids, stats):
    lane = lax.broadcasted_iota(jnp.int32, (key_ids.shape[0], 128), 1)
    marks = lane == key_ids
    if stats:
        marks = marks | ((lane >= SEGS) & (lane < SEGS + 3))
    return jnp.where(marks, 1.0, 0.0).astype(bf16)


def query_bias(query_ids):
    lane = lax.broadcasted_iota(jnp.int32, (query_ids.shape[0], 128), 1)
    return jnp.where((lane == query_ids) | (lane >= SEGS), 0.0, masked_value)


def softmax_columns(scores):
    top = jnp.max(scores, axis=0, keepdims=True)
    raised = jnp.exp(scores - top)
    return raised, top, jnp.sum(raised, axis=0, keepdims=True)


def finish_forward(halves, tops, sums):
    mixed = jnp.concatenate([h / s for h, s in zip(halves, sums)], axis=0)
    rows = [t + jnp.log(s) for t, s in zip(tops, sums)]
    pad = jnp.zeros((6, rows[0].shape[1]), f32)
    return mixed.T.astype(bf16), jnp.concatenate(rows + [pad], axis=0)


def cross_forward_kernel(rider, q_ref, c_ref, wk_ref, wv_ref, qid_ref, kid_ref, *refs):
    (o_ref, lse_ref, k_ref, v_ref) = rider.board(refs, 4)
    both = jnp.concatenate([wk_ref[0], wv_ref[0]], axis=0)
    projected = dot_nt(c_ref[0], both).astype(bf16)
    key, value = projected[:, :PAIR], projected[:, PAIR:]
    k_ref[0], v_ref[0] = key, value
    marked = jnp.concatenate([key, key_marks(kid_ref[0], False)], axis=1)
    bias = query_bias(qid_ref[0]).astype(bf16)
    query = q_ref[0] * jnp.asarray(score_scale, bf16)
    values = value.T
    halves, tops, sums = [], [], []
    for half in range(2):
        extended = jnp.concatenate([head_half(query, half), bias], axis=1)
        raised, top, total = softmax_columns(dot_nt(marked, extended))
        halves.append(dot_nn(values[half * HEAD : (half + 1) * HEAD], raised.astype(bf16)))
        tops.append(top)
        sums.append(total)
    o_ref[0], lse_ref[0, 0] = finish_forward(halves, tops, sums)
    rider.leave()


def causal_mask(qid_ref, kid_ref):
    length = kid_ref.shape[1]
    key = lax.broadcasted_iota(jnp.int32, (length, length), 0)
    query = lax.broadcasted_iota(jnp.int32, (length, length), 1)
    return (key <= query) & (kid_ref[0] == qid_ref[0])


def pair_lanes(pair):
    return slice(pair * PAIR, (pair + 1) * PAIR)


def self_forward_kernel(q_ref, k_ref, v_ref, qid_ref, kid_ref, o_ref, lse_ref):
    allowed = causal_mask(qid_ref, kid_ref)
    for pair in range(GROUP):
        lanes = pair_lanes(pair)
        query = q_ref[0, :, lanes] * jnp.asarray(score_scale, bf16)
        key = k_ref[0, :, lanes]
        values = v_ref[0, :, lanes].T
        halves, tops, sums = [], [], []
        for half in range(2):
            scores = jnp.where(allowed, dot_nt(key, head_half(query, half)), masked_value)
            raised, top, total = softmax_columns(scores)
            halves.append(dot_nn(values[half * HEAD : (half + 1) * HEAD], raised.astype(bf16)))
            tops.append(top)
            sums.append(total)
        o_ref[0, :, lanes], lse_ref[0, pair] = finish_forward(halves, tops, sums)


def backward_pair(query, key, value, mixed, grad, lse, marked, bias, allowed):
    scaled = query * jnp.asarray(score_scale, bf16)
    key_turned = key.T
    length = query.shape[0]
    lse_columns = lse.T
    product = mixed.astype(f32) * grad.astype(f32)
    ones = key_marks(jnp.full((value.shape[0], 1), -1, jnp.int32), True)
    valued = jnp.concatenate([value, ones], axis=1)
    probs, grads, turned = [], [], []
    for half in range(2):
        stats = stat_lanes(bias, lse_columns[:, half : half + 1], SEGS).astype(bf16)
        scores = dot_nt(marked, jnp.concatenate([head_half(scaled, half), stats], axis=1))
        if allowed is not None:
            scores = jnp.where(allowed, scores, masked_value)
        weight = jnp.exp(scores)
        inner = jnp.sum(head_half(product, half), axis=1, keepdims=True)
        delta = stat_lanes(jnp.zeros((length, 128), f32), inner, SEGS).astype(bf16)
        shifted = dot_nt(valued, jnp.concatenate([head_half(grad, half), delta], axis=1))
        grad_scores = (weight * shifted).astype(bf16)
        probs.append(weight.astype(bf16))
        grads.append(grad_scores)
        turned.append(dot_nn(key_turned[half * HEAD : (half + 1) * HEAD], grad_scores))
    grad_query = (score_scale * jnp.concatenate(turned, axis=0)).T.astype(bf16)
    grad_turned, scaled_turned = grad.T, scaled.T
    halves = [slice(0, HEAD), slice(HEAD, PAIR)]
    value_turned = jnp.concatenate(
        [dot_nt(grad_turned[h], p) for h, p in zip(halves, probs)], axis=0).astype(bf16)
    keyed_turned = jnp.concatenate(
        [dot_nt(scaled_turned[h], p) for h, p in zip(halves, grads)], axis=0).astype(bf16)
    grad_value, grad_key = value_turned.T, keyed_turned.T
    return grad_query, grad_key, grad_value, keyed_turned, value_turned


def cross_backward_kernel(rider, q_ref, k_ref, v_ref, o_ref, do_ref, lse_ref, qid_ref, kid_ref,
                          c_ref, *refs):
    total_ref = refs[-1]
    dq_ref, dk_ref, dv_ref, sum_ref = rider.board(refs[:-1], 4)
    marked = jnp.concatenate([k_ref[0], key_marks(kid_ref[0], True)], axis=1)
    dq_ref[0], grad_key, grad_value, key_t, value_t = backward_pair(
        q_ref[0], k_ref[0], v_ref[0], o_ref[0], do_ref[0], lse_ref[0, 0], marked,
        query_bias(qid_ref[0]), None)
    dk_ref[0], dv_ref[0] = grad_key, grad_value
    row, pair = pl.program_id(0), pl.program_id(1)
    part = dot_nn(jnp.concatenate([key_t, value_t], axis=0), c_ref[0])

    @pl.when(row == 0)
    def _():
        total_ref[pair] = part

    @pl.when(row > 0)
    def _():
        total_ref[pair] = total_ref[pair] + part

    @pl.when(row == pl.num_programs(0) - 1)
    def _():
        at = pl.ds(pl.multiple_of(pair * PAIR, PAIR), PAIR)
        sum_ref[0, at] = total_ref[pair, :PAIR].astype(bf16)
        sum_ref[1, at] = total_ref[pair, PAIR:].astype(bf16)

    rider.leave()


def self_backward_kernel(q_ref, k_ref, v_ref, o_ref, do_ref, lse_ref, qid_ref, kid_ref,
                         dq_ref, dk_ref, dv_ref):
    length = k_ref.shape[1]
    ones = key_marks(jnp.full((length, 1), -1, jnp.int32), True)
    allowed = causal_mask(qid_ref, kid_ref)
    for pair in range(GROUP):
        lanes = pair_lanes(pair)
        key = k_ref[0, :, lanes]
        dq_ref[0, :, lanes], dk_ref[0, :, lanes], dv_ref[0, :, lanes] = backward_pair(
            q_ref[0, :, lanes], key, v_ref[0, :, lanes], o_ref[0, :, lanes],
            do_ref[0, :, lanes], lse_ref[0, pair], jnp.concatenate([key, ones], axis=1),
            jnp.zeros((length, 128), f32), allowed)[:3]


def pair_spec(length, offset, pairs=1):
    return pl.BlockSpec((1, length, pairs * PAIR), lambda row, step: (row, 0, offset + step))


def row_spec(shape):
    return pl.BlockSpec((1,) + shape, lambda row, step: (row, 0, 0))


def stat_spec(length, pairs=1):
    return pl.BlockSpec((1, pairs, 8, length), lambda row, step: (row, step, 0, 0))


def cost(rows, queries, keys, products):
    elements = rows * HEADS * queries * keys
    return pl.CostEstimate(
        flops=2 * elements * 256 * products // 2,
        transcendentals=elements,
        bytes_accessed=rows * (queries + keys) * D * 2 * 3,
    )


class Rider:
    def __init__(self, sizes, names, kind, number, steps):
        self.sizes, self.names, self.kind, self.number = sizes, names, kind, number
        self.steps = steps

    def board(self, refs, outputs):
        count = len(self.names)
        theirs, mine, scratch = refs[:count], refs[count : count + outputs], refs[count + outputs :]
        if count:
            ends, scratch = scratch[:count], scratch[count:]
            build = gather_stages if self.kind == "gather" else scatter_stages
            stages = build(self.sizes, self.names, theirs, ends, scratch)
            step = pl.program_id(0) * pl.num_programs(1) + pl.program_id(1)
            for number in range(self.steps):
                run_stages(stages, step, number, self.steps)
            self.rest = ([s for time, s in stages if time >= 12], step == self.steps - 1)
        return mine

    def leave(self):
        if self.names and self.rest[0]:
            pl.when(self.rest[1])(functools.partial(in_turn, self.rest[0]))

    def in_specs(self):
        return [VMEM if self.kind == "gather" else HBM] * len(self.names)

    def out_specs(self):
        return [HBM if self.kind == "gather" else VMEM] * len(self.names)

    def out_shape(self):
        if self.kind == "gather":
            return [jax.ShapeDtypeStruct(self.sizes.full(n), bf16) for n in self.names]
        return [jax.ShapeDtypeStruct(self.sizes.shard(n), f32) for n in self.names]

    def scratch(self):
        if not self.names:
            return []
        build = gather_scratch if self.kind == "gather" else scatter_scratch
        return build(self.sizes, self.names)

    def params(self):
        if not self.names:
            return pltpu.CompilerParams()
        return pltpu.CompilerParams(
            collective_id=self.number, has_side_effects=True, vmem_limit_bytes=60 * 1024 * 1024
        )


def self_forward(packed, query_ids, key_ids):
    rows, length = packed.shape[:2]
    steps = PAIRS // GROUP
    return pl.pallas_call(
        self_forward_kernel,
        grid=(rows, steps),
        in_specs=[pair_spec(length, part * steps, GROUP) for part in range(3)]
        + [row_spec((1, length)), row_spec((length, 1))],
        out_specs=[pair_spec(length, 0, GROUP), stat_spec(length, GROUP)],
        out_shape=[
            jax.ShapeDtypeStruct((rows, length, D), bf16),
            jax.ShapeDtypeStruct((rows, PAIRS, 8, length), f32),
        ],
        cost_estimate=cost(rows, length, length, 2),
        name="self_forward",
    )(packed, packed, packed, query_ids, key_ids)


def self_backward(packed, mixed, grad, lse, query_ids, key_ids):
    rows, length = packed.shape[:2]
    steps = PAIRS // GROUP
    plain = pair_spec(length, 0, GROUP)
    return pl.pallas_call(
        self_backward_kernel,
        grid=(rows, steps),
        in_specs=[pair_spec(length, part * steps, GROUP) for part in range(3)]
        + [plain, plain, stat_spec(length, GROUP), row_spec((1, length)), row_spec((length, 1))],
        out_specs=[plain] * 3,
        out_shape=[jax.ShapeDtypeStruct((rows, length, D), bf16)] * 3,
        cost_estimate=cost(rows, length, length, 5),
        name="self_backward",
    )(packed, packed, packed, mixed, grad, lse, query_ids, key_ids)


def cross_forward(rider, queries, patches, projections, query_ids, key_ids, shards):
    rows, length = queries.shape[:2]
    count = patches.shape[1]

    def slab(which):
        return pl.BlockSpec((1, PAIR, D), lambda row, pair: (which, pair, 0))

    return pl.pallas_call(
        functools.partial(cross_forward_kernel, rider),
        grid=(rows, PAIRS),
        in_specs=[
            pair_spec(length, 0),
            row_spec((count, D)),
            slab(1),
            slab(2),
            row_spec((length, 1)),
            row_spec((count, 1)),
        ]
        + rider.in_specs(),
        out_specs=[
            pair_spec(length, 0), stat_spec(length), pair_spec(count, 0), pair_spec(count, 0),
        ]
        + rider.out_specs(),
        out_shape=[
            jax.ShapeDtypeStruct((rows, length, D), bf16),
            jax.ShapeDtypeStruct((rows, PAIRS, 8, length), f32),
            jax.ShapeDtypeStruct((rows, count, D), bf16),
            jax.ShapeDtypeStruct((rows, count, D), bf16),
        ]
        + rider.out_shape(),
        scratch_shapes=rider.scratch(),
        compiler_params=rider.params(),
        cost_estimate=cost(rows, length, count, 4),
        name="cross_forward",
    )(queries, patches, projections, projections, query_ids, key_ids, *shards)


def cross_backward(rider, queries, keys, values, mixed, grad, lse, query_ids, key_ids, patches,
                   fulls):
    rows, length = grad.shape[:2]
    count = keys.shape[1]
    short, tall = pair_spec(length, 0), pair_spec(count, 0)
    return pl.pallas_call(
        functools.partial(cross_backward_kernel, rider),
        grid=(rows, PAIRS),
        in_specs=[
            short, tall, tall, short, short, stat_spec(length), row_spec((length, 1)),
            row_spec((count, 1)), row_spec((count, D)),
        ]
        + rider.in_specs(),
        out_specs=[short, tall, tall, VMEM] + rider.out_specs(),
        out_shape=[
            jax.ShapeDtypeStruct((rows, length, D), bf16),
            jax.ShapeDtypeStruct((rows, count, D), bf16),
            jax.ShapeDtypeStruct((rows, count, D), bf16),
            jax.ShapeDtypeStruct((2, D, D), bf16),
        ]
        + rider.out_shape(),
        scratch_shapes=rider.scratch() + [pltpu.VMEM((PAIRS, 2 * PAIR, D), f32)],
        compiler_params=rider.params(),
        cost_estimate=cost(rows, length, count, 7),
        name="cross_backward",
    )(queries, keys, values, mixed, grad, lse, query_ids, key_ids, patches, *fulls)


def gather_weights(attention, inner, outer):
    turned = lax.all_gather(jnp.swapaxes(attention, 1, 2), BOTH, axis=0, tiled=False)
    heads = lax.axis_size("dp"), lax.axis_size("fsdp")
    turned = turned.reshape(heads + turned.shape[1:])
    full_attention = jnp.transpose(turned, (2, 0, 3, 1, 4)).reshape(8, D, D)
    wide = lax.all_gather(inner, BOTH, axis=0, tiled=False)
    wide = wide.reshape(heads + wide.shape[1:])
    full_inner = jnp.transpose(wide, (2, 1, 3, 0, 4)).reshape(2, D, -1)
    tall = lax.all_gather(outer.T, BOTH, axis=0, tiled=False)
    tall = tall.reshape(heads + tall.shape[1:])
    full_outer = jnp.transpose(tall, (0, 2, 1, 3)).reshape(D, -1)
    return full_attention, full_inner, full_outer


def scatter_grads(attention, inner, outer):
    across, within = lax.axis_size("dp"), lax.axis_size("fsdp")
    blocks = attention.reshape(8, across, D // across, within, D // within)
    blocks = jnp.transpose(blocks, (1, 3, 0, 2, 4))
    blocks = blocks.reshape((across * within,) + blocks.shape[2:])
    own_attention = lax.psum_scatter(blocks, BOTH, scatter_dimension=0, tiled=False)
    blocks = inner.reshape(2, within, D // within, across, inner.shape[2] // across)
    blocks = jnp.transpose(blocks, (3, 1, 0, 2, 4))
    blocks = blocks.reshape((across * within,) + blocks.shape[2:])
    own_inner = lax.psum_scatter(blocks, BOTH, scatter_dimension=0, tiled=False)
    blocks = outer.reshape(across, D // across, within, outer.shape[1] // within)
    blocks = jnp.transpose(blocks, (0, 2, 1, 3))
    blocks = blocks.reshape((across * within,) + blocks.shape[2:])
    own_outer = lax.psum_scatter(blocks, BOTH, scatter_dimension=0, tiled=False)
    return (
        jnp.swapaxes(own_attention, 1, 2).astype(f32),
        own_inner.astype(f32),
        own_outer.T.astype(f32),
    )


MESH = pl.DeviceIdType.MESH
RIGHT, LEFT, TO_Y, TO_X, TO_CORE = range(5)


def where_am_i():
    across, within = lax.axis_index("dp"), lax.axis_index("fsdp")
    return across // 2, across % 2, within // 2, within % 2


def device_at(z, y, x, core):
    return (2 * z + y, 2 * x + core)


def aligned(value, unit):
    return pl.multiple_of(value * unit, unit)


class Sizes:
    def __init__(self, down, width, side, deep):
        self.down, self.width, self.side, self.deep = down, width, side, deep
        self.across, self.within = D // down, D // width
        self.depth = self.across // 2
        self.chips = self.across * self.within // 2

    def shard(self, name):
        return {
            "low": (4, self.down, self.width),
            "high": (4, self.down, self.width),
            "inner": (2, self.width, self.side),
            "outer": (self.down, self.deep),
        }[name]

    def full(self, name):
        return {
            "low": (4, D, D),
            "high": (4, D, D),
            "inner": (D, 2 * self.across * self.side),
            "outer": (D, self.within * self.deep),
        }[name]

    def piece(self, name):
        return {
            "low": (self.down, 2 * self.width),
            "high": (self.down, 2 * self.width),
            "inner": (self.width, self.side),
            "outer": (self.down // 2, self.deep),
        }[name]

    def part(self, name):
        return {
            "low": (2, self.down, self.width),
            "high": (2, self.down, self.width),
            "inner": (self.width, self.side),
            "outer": (self.down // 2, self.deep),
        }[name]

    def place(self, name, ref, cut, z, y, x, half):
        place = 2 * z + y
        if name == "inner":
            return ref.at[
                pl.ds(aligned(2 * x + cut, self.width), self.width),
                pl.ds(aligned(half * self.across + place, self.side), self.side),
            ]
        if name == "outer":
            return ref.at[
                pl.ds(aligned(2 * place + half, self.down // 2), self.down // 2),
                pl.ds(aligned(2 * x + cut, self.deep), self.deep),
            ]
        return ref.at[
            2 * half + cut,
            pl.ds(aligned(place, self.down), self.down),
            pl.ds(aligned(x, 2 * self.width), 2 * self.width),
        ]

    def share(self, name, ref, half):
        if name == "inner":
            return ref.at[half]
        if name == "outer":
            return ref.at[pl.ds(aligned(half, self.down // 2), self.down // 2)]
        return ref.at[pl.ds(2 * half, 2)]


def greet(depth):
    z, y, x, core = where_am_i()
    barrier = pltpu.get_barrier_semaphore()

    def signal(device):
        pl.semaphore_signal(barrier, inc=1, device_id=device, device_id_type=MESH)

    signal(device_at(z, y, x, 1 - core))
    signal(device_at(z, y, 1 - x, core))
    signal(device_at(z, 1 - y, x, core))
    pl.when(z > 0)(lambda: signal(device_at(z - 1, y, x, core)))
    pl.when(z < depth - 1)(lambda: signal(device_at(z + 1, y, x, core)))
    pl.semaphore_wait(barrier, 3 + jnp.where(z > 0, 1, 0) + jnp.where(z < depth - 1, 1, 0))


def chip_index(bz, by, bx):
    return (2 * bz + by) * 2 + bx


def remote(src, dst, send, recv, device):
    return pltpu.make_async_remote_copy(
        src_ref=src, dst_ref=dst, send_sem=send, recv_sem=recv, device_id=device,
        device_id_type=MESH)


def gather_scratch(sizes, names):
    wave = pltpu.SemaphoreType.DMA
    count, pieces = len(names), 2 * len(names)
    return (
        [pltpu.VMEM((2,) + sizes.piece(name), bf16) for name in names]
        + [pltpu.VMEM(sizes.part(name), bf16) for name in names]
        + [wave((count,)), wave((count,)), wave((pieces,)), wave((pieces, 5, sizes.chips)),
           wave((pieces, 2, sizes.chips))]
    )


def gather_stages(sizes, names, shards, fulls, scratch):
    count, depth = len(names), sizes.depth
    pairs, got = scratch[:count], scratch[count : 2 * count]
    swap_send, swap_recv, own_sem, send_sem, recv_sem = scratch[2 * count :]
    z, y, x, core = where_am_i()
    other = 1 - core
    pieces = [(n, cut) for cut in range(2) for n in range(count)]

    def place(piece, bz, by, bx, half):
        n, cut = pieces[piece]
        return sizes.place(names[n], fulls[n], cut, bz, by, bx, half)

    def swap(n):
        return remote(sizes.share(names[n], shards[n], other), got[n], swap_send.at[n],
                      swap_recv.at[n], device_at(z, y, x, other))

    def merge(n, me):
        if names[n] in ("low", "high"):
            width = sizes.width
            for part, source in ((me, shards[n][2 * me : 2 * me + 2]), (1 - me, got[n][...])):
                pairs[n][:, :, part * width : (part + 1) * width] = source
        else:
            half = sizes.down // 2
            mine = shards[n][me] if names[n] == "inner" else shards[n][me * half : (me + 1) * half]
            pairs[n][me] = mine
            pairs[n][1 - me] = got[n][...]

    def copy(piece, bz, by, bx, kind, own=False):
        target = {
            RIGHT: device_at(z + 1, y, x, core),
            LEFT: device_at(z - 1, y, x, core),
            TO_Y: device_at(z, 1 - y, x, core),
            TO_X: device_at(z, y, 1 - x, core),
            TO_CORE: device_at(z, y, x, other),
        }[kind]
        spot = place(piece, bz, by, bx, core)
        n, cut = pieces[piece]
        slot = chip_index(bz, by, bx)
        return remote(pairs[n].at[cut] if own else spot, spot, send_sem.at[piece, kind, slot],
                      recv_sem.at[piece, 1 if kind == TO_CORE else 0, slot], target)

    def arrive(piece, bz, by, bx, from_core=False):
        spot = place(piece, bz, by, bx, other if from_core else core)
        remote(spot, spot, send_sem.at[piece, 0, 0],
               recv_sem.at[piece, 1 if from_core else 0, chip_index(bz, by, bx)],
               device_at(z, y, x, other)).wait_recv()

    def keep(piece):
        n, cut = pieces[piece]
        return pltpu.make_async_copy(pairs[n].at[cut], place(piece, z, y, x, core),
                                     own_sem.at[piece])

    every = range(len(pieces))
    first, later = every[:count], every[count:]

    def launch(kind):
        for piece in every:
            copy(piece, z, y, x, kind, True).start()

    def begin():
        greet(depth)
        for n in range(count):
            swap(n).start()

    def send_own():
        for n in range(count):
            swap(n).wait_recv()
        for me in range(2):
            @pl.when(core == me)
            def _(me=me):
                for n in range(count):
                    merge(n, me)
        pl.when(z < depth - 1)(lambda: launch(RIGHT))
        pl.when(z > 0)(lambda: launch(LEFT))
        for piece in every:
            copy(piece, z, y, x, TO_Y, True).start()
            copy(piece, z, y, x, TO_X, True).start()
        for piece in every:
            copy(piece, z, y, x, TO_CORE, True).start()
            keep(piece).start()

    def from_z(bz, kind, further):
        for piece in every:
            arrive(piece, bz, y, x)
            pl.when(further)(lambda piece=piece: copy(piece, bz, y, x, kind).start())
            copy(piece, bz, y, x, TO_Y).start()
            copy(piece, bz, y, x, TO_X).start()
            copy(piece, bz, y, x, TO_CORE).start()

    def from_sides(bz):
        for early, late in zip(first, later):
            arrive(early, bz, 1 - y, x)
            copy(early, bz, 1 - y, x, TO_X).start()
            copy(early, bz, 1 - y, x, TO_CORE).start()
            arrive(late, bz, y, 1 - x)
            copy(late, bz, y, 1 - x, TO_Y).start()
            copy(late, bz, y, 1 - x, TO_CORE).start()
        for early, late in zip(first, later):
            arrive(early, bz, y, 1 - x)
            copy(early, bz, y, 1 - x, TO_CORE).start()
            arrive(late, bz, 1 - y, x)
            copy(late, bz, 1 - y, x, TO_CORE).start()

    def from_corner(bz):
        for piece in every:
            arrive(piece, bz, 1 - y, 1 - x)
            copy(piece, bz, 1 - y, 1 - x, TO_CORE).start()

    def both_ways(step, action):
        if step == 0:
            action(z)
            return
        pl.when(z - step >= 0)(lambda: action(z - step))
        pl.when(z + step < depth)(lambda: action(z + step))

    def line(step):
        pl.when(z - step >= 0)(lambda: from_z(z - step, RIGHT, z < depth - 1))
        pl.when(z + step < depth)(lambda: from_z(z + step, LEFT, z > 0))

    def end():
        for n in range(count):
            swap(n).wait_send()
        for piece in every:
            keep(piece).wait()

            @pl.loop(0, depth)
            def _(bz, piece=piece):
                for by in range(2):
                    for bx in range(2):
                        arrive(piece, bz, by, bx, True)
                        copy(piece, bz, by, bx, TO_CORE).wait_send()
                copy(piece, bz, y, x, TO_Y).wait_send()
                copy(piece, bz, y, x, TO_X).wait_send()
                if piece in first:
                    copy(piece, bz, 1 - y, x, TO_X).wait_send()
                else:
                    copy(piece, bz, y, 1 - x, TO_Y).wait_send()
                pl.when((bz <= z) & (z < depth - 1))(
                    lambda: copy(piece, bz, y, x, RIGHT).wait_send())
                pl.when((bz >= z) & (z > 0))(lambda: copy(piece, bz, y, x, LEFT).wait_send())

    timed = [(0, begin), (0, send_own), (12, end)]
    for step in range(1, depth):
        timed.append((2 * step, functools.partial(line, step)))
    for step in range(depth):
        timed.append(((3, 6, 8, 9)[step], functools.partial(both_ways, step, from_sides)))
        timed.append(((10, 10, 11, 11)[step], functools.partial(both_ways, step, from_corner)))
    return sorted(timed, key=lambda item: item[0])


def add_rows(target, sources):
    slab = 48

    def total(k):
        at = pl.ds(aligned(k, slab), slab)
        value = sources[0][at].astype(f32)
        for source in sources[1:]:
            value = value + source[at].astype(f32)
        target[at] = value.astype(target.dtype)

    pl.loop(0, target.shape[0] // slab)(total)


def scatter_scratch(sizes, names):
    wave = pltpu.SemaphoreType.DMA
    count, pieces, depth, chips = len(names), 2 * len(names), sizes.depth, sizes.chips

    def buffers(lead, kind):
        return [pltpu.VMEM(lead + (2,) + sizes.piece(name), kind) for name in names]

    return (
        buffers((chips,), bf16) + buffers((chips,), bf16) + buffers((2 * depth,), bf16)
        + buffers((depth,), bf16) + buffers((2, depth), bf16) + buffers((), f32)
        + [pltpu.VMEM(sizes.part(name), f32) for name in names]
        + [pltpu.VMEM(sizes.part(name), f32) for name in names]
        + [wave((pieces, chips))] * 3 + [wave((pieces, 2 * depth))] * 2
        + [wave((pieces, depth))] * 2 + [wave((pieces, 2, depth))] * 2 + [wave((count,))] * 2
    )


def scatter_stages(sizes, names, fulls, owns, scratch):
    count, depth = len(names), sizes.depth
    acc, swapped, first, second, line, sums, outs, ins = (
        scratch[k * count : (k + 1) * count] for k in range(8)
    )
    (load_sem, swap_send, swap_recv, one_send, one_recv, two_send, two_recv, line_send,
     line_recv, end_send, end_recv) = scratch[8 * count :]
    z, y, x, core = where_am_i()
    other = 1 - core
    partner = device_at(z, y, x, other)
    over_x, over_y = device_at(z, y, 1 - x, core), device_at(z, 1 - y, x, core)
    pieces = [(n, cut) for cut in range(2) for n in range(count)]
    every = range(len(pieces))
    order = sorted(range(depth), key=lambda spot: (-abs(2 * spot - depth + 1), -spot))

    def at(buffers, piece, *index):
        n, cut = pieces[piece]
        return buffers[n].at[(*index, cut)]

    def block(piece, bz, by, bx, half):
        n, cut = pieces[piece]
        return sizes.place(names[n], fulls[n], cut, bz, by, bx, half)

    def load(piece, bz, by, bx):
        slot = chip_index(bz, by, bx)
        return pltpu.make_async_copy(block(piece, bz, by, bx, core), at(acc, piece, slot),
                                     load_sem.at[piece, slot])

    def swap(piece, bz, by, bx):
        slot = chip_index(bz, by, bx)
        return remote(block(piece, bz, by, bx, other), at(swapped, piece, slot),
                      swap_send.at[piece, slot], swap_recv.at[piece, slot], partner)

    def turned(piece):
        return pieces[piece][1] == 1

    def stage_one(piece, bz, spot):
        if turned(piece):
            far, device = chip_index(bz, 1 - y, spot), over_y
        else:
            far, device = chip_index(bz, spot, 1 - x), over_x
        slot = 2 * bz + spot
        return remote(at(acc, piece, far), at(first, piece, slot), one_send.at[piece, slot],
                      one_recv.at[piece, slot], device)

    def stage_two(piece, bz):
        if turned(piece):
            far, device = chip_index(bz, y, 1 - x), over_x
        else:
            far, device = chip_index(bz, 1 - y, x), over_y
        return remote(at(acc, piece, far), at(second, piece, bz), two_send.at[piece, bz],
                      two_recv.at[piece, bz], device)

    def along(piece, bz, way):
        device = device_at(z + 1, y, x, core) if way == 0 else device_at(z - 1, y, x, core)
        return remote(at(acc, piece, chip_index(bz, y, x)), at(line, piece, way, bz),
                      line_send.at[piece, way, bz], line_recv.at[piece, way, bz], device)

    def begin():
        greet(depth)
        for bz in order:
            for flip_y, flip_x in ((1, 1), (0, 1), (1, 0), (0, 0)):
                for piece in every:
                    if turned(piece):
                        flip_y, flip_x = flip_x, flip_y
                    by = 1 - y if flip_y else y
                    bx = 1 - x if flip_x else x
                    swap(piece, bz, by, bx).start()
                    load(piece, bz, by, bx).start()
                    if turned(piece):
                        flip_y, flip_x = flip_x, flip_y

    def join(piece, bz, by, bx, extra=()):
        load(piece, bz, by, bx).wait()
        swap(piece, bz, by, bx).wait_recv()
        mine = at(acc, piece, chip_index(bz, by, bx))
        add_rows(mine, (mine, at(swapped, piece, chip_index(bz, by, bx))) + extra)

    def send_first(bz):
        for far in range(2):
            for piece in every:
                if turned(piece):
                    spot = x if far else 1 - x
                    join(piece, bz, 1 - y, spot)
                else:
                    spot = y if far else 1 - y
                    join(piece, bz, spot, 1 - x)
                stage_one(piece, bz, spot).start()

    def send_second(bz):
        for piece in every:
            spot = 1 - x if turned(piece) else 1 - y
            stage_one(piece, bz, spot).wait_recv()
            arrived = (at(first, piece, 2 * bz + spot),)
            if turned(piece):
                join(piece, bz, y, spot, arrived)
            else:
                join(piece, bz, spot, x, arrived)
            stage_two(piece, bz).start()

    def gathered(piece, bz):
        spot = x if turned(piece) else y
        stage_one(piece, bz, spot).wait_recv()
        stage_two(piece, bz).wait_recv()
        load(piece, bz, y, x).wait()
        swap(piece, bz, y, x).wait_recv()
        mine = at(acc, piece, chip_index(bz, y, x))
        return mine, (mine, at(swapped, piece, chip_index(bz, y, x)),
                      at(first, piece, 2 * bz + spot), at(second, piece, bz))

    def pass_on(bz, level, way):
        for piece in every:
            mine, base = gathered(piece, bz)
            if level > 0:
                along(piece, bz, way).wait_recv()
                base = base + (at(line, piece, way, bz),)
            add_rows(mine, base)
            along(piece, bz, way).start()

    def pass_level(bz, level):
        if level < bz:
            pl.when(z == level)(lambda: pass_on(bz, level, 0))
        if depth - 1 - level > bz:
            pl.when(z == depth - 1 - level)(lambda: pass_on(bz, level, 1))

    def finish(bz):
        @pl.when(z == bz)
        def _():
            ways = ((0,) if bz > 0 else ()) + ((1,) if bz < depth - 1 else ())
            for piece in every:
                n, cut = pieces[piece]
                _, base = gathered(piece, bz)
                for way in ways:
                    along(piece, bz, way).wait_recv()
                add_rows(sums[n].at[cut], base + tuple(at(line, piece, way, bz) for way in ways))

    def exchange(n):
        return remote(outs[n], ins[n], end_send.at[n], end_recv.at[n], partner)

    width, half = sizes.width, sizes.down // 2

    def hand_over():
        for me in range(2):
            @pl.when(core == me)
            def _(me=me):
                far = 1 - me
                for n, name in enumerate(names):
                    if name == "inner":
                        outs[n][...] = sums[n][far]
                        owns[n][me] = sums[n][me]
                    elif name == "outer":
                        outs[n][...] = sums[n][far]
                        owns[n][me * half : (me + 1) * half] = sums[n][me]
                    else:
                        outs[n][...] = sums[n][:, :, far * width : (far + 1) * width]
                        owns[n][2 * me : 2 * me + 2] = sums[n][:, :, me * width : (me + 1) * width]
        for n in range(count):
            exchange(n).start()

    def end():
        for n in range(count):
            exchange(n).wait_recv()
        for me in range(2):
            @pl.when(core == me)
            def _(me=me):
                far = 1 - me
                for n, name in enumerate(names):
                    if name == "inner":
                        owns[n][far] = ins[n][...]
                    elif name == "outer":
                        owns[n][far * half : (far + 1) * half] = ins[n][...]
                    else:
                        owns[n][2 * far : 2 * far + 2] = ins[n][...]
        for n in range(count):
            exchange(n).wait_send()
        for piece in every:
            @pl.loop(0, depth)
            def _(bz, piece=piece):
                for by in range(2):
                    for bx in range(2):
                        swap(piece, bz, by, bx).wait_send()
                for spot in range(2):
                    stage_one(piece, bz, spot).wait_send()
                stage_two(piece, bz).wait_send()
                pl.when(z < bz)(lambda: along(piece, bz, 0).wait_send())
                pl.when(z > bz)(lambda: along(piece, bz, 1).wait_send())

    timed = [(0, begin)]
    for turn, bz in enumerate(order):
        timed.append((turn, functools.partial(send_first, bz)))
        timed.append(((2, 4, 5, 7)[turn], functools.partial(send_second, bz)))
        for level in range(depth - 1):
            when = ((4, 6, 8), (8, 10, 12), (9, 11, 12), (9, 12, 12))[turn][level]
            timed.append((when, functools.partial(pass_level, bz, level)))
    ending = [functools.partial(finish, bz) for bz in order] + [hand_over, end]
    timed.append((13, functools.partial(in_turn, ending)))
    return sorted(timed, key=lambda item: item[0])


def in_turn(actions):
    for action in actions:
        action()


def run_stages(timed, step, number, steps):
    mine = [stage for time, stage in timed if time < 12 and time * steps // 12 == number]
    if mine:
        pl.when(step == number)(functools.partial(in_turn, mine))


HBM = pl.BlockSpec(memory_space=pl.ANY)
VMEM = pl.BlockSpec(memory_space=pltpu.VMEM)


def gather_kernel(sizes, names, *refs):
    count = len(names)
    gain_ref, gain_out, send, recv = refs[count], refs[2 * count + 1], *refs[-2:]
    stages = gather_stages(sizes, names, refs[:count], refs[count + 1 : 2 * count + 1],
                           refs[2 * count + 2 : -2])
    z, y, x, core = where_am_i()
    mine, near = 2 * x + core, 2 * x + 1 - core
    far, corner = 2 * (1 - x) + core, 2 * (1 - x) + 1 - core

    def pass_gain(src, slot, kind, device):
        return remote(src, gain_out.at[slot], send.at[kind], recv.at[kind], device)

    partner, beside = device_at(z, y, x, 1 - core), device_at(z, y, 1 - x, core)
    hops = (
        (gain_ref, mine, 0, partner),
        (gain_ref, mine, 1, beside),
        (gain_out.at[near], near, 2, beside),
    )
    stages = [stage for _, stage in stages]
    stages[0]()
    gain_out[mine] = gain_ref[...]
    pass_gain(*hops[0]).start()
    pass_gain(*hops[1]).start()
    stages[1]()
    pass_gain(gain_ref, near, 0, partner).wait_recv()
    pass_gain(*hops[2]).start()
    for stage in stages[2:]:
        stage()
    pass_gain(gain_ref, far, 1, beside).wait_recv()
    pass_gain(gain_ref, corner, 2, beside).wait_recv()
    for hop in hops:
        pass_gain(*hop).wait_send()


def gather_blocks(sizes, names, shards, gain):
    wave = pltpu.SemaphoreType.DMA
    return pl.pallas_call(
        functools.partial(gather_kernel, sizes, names),
        out_shape=[jax.ShapeDtypeStruct(sizes.full(name), bf16) for name in names]
        + [jax.ShapeDtypeStruct((sizes.within,) + gain.shape, f32)],
        in_specs=[VMEM] * (len(names) + 1),
        out_specs=[HBM] * len(names) + [VMEM],
        scratch_shapes=gather_scratch(sizes, names) + [wave((3,)), wave((3,))],
        compiler_params=pltpu.CompilerParams(collective_id=0, has_side_effects=True),
        name="gather_blocks",
    )(*shards, gain)


def gain_stages(depth, gain_ref, gain_out, buf, send, recv):
    z, y, x, core = where_am_i()
    hops = (device_at(z, y, x, 1 - core), device_at(z, y, 1 - x, core),
            device_at(z, 1 - y, x, core))

    def hop(step):
        return remote(buf.at[2 * step], buf.at[2 * step + 1], send.at[step], recv.at[step],
                      hops[step])

    def line(way):
        device = device_at(z + 1, y, x, core) if way == 0 else device_at(z - 1, y, x, core)
        return remote(buf.at[7 + way], buf.at[9 + way], send.at[3 + way], recv.at[3 + way],
                      device)

    def begin():
        buf[0] = gain_ref[...]
        hop(0).start()

    def turn(step):
        hop(step).wait_recv()
        buf[2 * step + 2] = buf[2 * step] + buf[2 * step + 1]
        if step < 2:
            hop(step + 1).start()

    def rightward():
        gain_out[...] = buf[6]

        @pl.when(z > 0)
        def _():
            line(0).wait_recv()
            gain_out[...] = gain_out[...] + buf[9]

        @pl.when(z < depth - 1)
        def _():
            buf[7] = gain_out[...]
            line(0).start()

    def leftward():
        buf[8] = buf[6]

        @pl.when(z < depth - 1)
        def _():
            line(1).wait_recv()
            gain_out[...] = gain_out[...] + buf[10]
            buf[8] = buf[6] + buf[10]

        pl.when(z > 0)(lambda: line(1).start())

    def end():
        for step in range(3):
            hop(step).wait_send()
        pl.when(z < depth - 1)(lambda: line(0).wait_send())
        pl.when(z > 0)(lambda: line(1).wait_send())

    return [begin] + [functools.partial(turn, step) for step in range(3)] + [
        rightward, leftward, end]


def scatter_kernel(sizes, names, k_ref, v_ref, wk_ref, wv_ref, *refs):
    count = len(names)
    fulls, gain_ref, grad_ref = refs[:count], refs[count], refs[count + 1]
    owns, gain_out = refs[count + 2 : 2 * count + 2], refs[2 * count + 2]
    gain_scratch, scratch = refs[2 * count + 3 : 2 * count + 6], refs[2 * count + 6 :]
    stages = scatter_stages(sizes, names, fulls, owns, scratch)
    gains = gain_stages(sizes.depth, gain_ref, gain_out, *gain_scratch)
    joined = [(0, stages[0][1])]
    for number, (_, stage) in enumerate(stages[1:]):
        both = functools.partial(in_turn, [stage] + gains[number : number + 1])
        joined.append((12 * (number + 1) / len(stages), both))
    steps = pl.num_programs(0)
    for number in range(steps):
        run_stages(joined, pl.program_id(0), number, steps)
    grad_ref[...] = dot_nn(k_ref[...], wk_ref[0]) + dot_nn(v_ref[...], wv_ref[0])


def scatter_blocks(sizes, names, fulls, gains, grad_key, grad_value, projections):
    wave = pltpu.SemaphoreType.DMA
    slab = 256
    rows = pl.BlockSpec((slab, D), lambda step: (step, 0))

    def matrix(which):
        return pl.BlockSpec((1, D, D), lambda step: (which, 0, 0))

    return pl.pallas_call(
        functools.partial(scatter_kernel, sizes, names),
        grid=(grad_key.shape[0] // slab,),
        out_shape=[jax.ShapeDtypeStruct(grad_key.shape, f32)]
        + [jax.ShapeDtypeStruct(sizes.shard(name), f32) for name in names]
        + [jax.ShapeDtypeStruct(gains.shape, f32)],
        in_specs=[rows, rows, matrix(1), matrix(2)] + [HBM] * len(names) + [VMEM],
        out_specs=[rows] + [VMEM] * (len(names) + 1),
        scratch_shapes=[pltpu.VMEM((11,) + gains.shape, f32), wave((5,)), wave((5,))]
        + scatter_scratch(sizes, names),
        compiler_params=pltpu.CompilerParams(
            collective_id=1, has_side_effects=True, vmem_limit_bytes=60 * 1024 * 1024
        ),
        name="scatter_blocks",
    )(grad_key, grad_value, projections, projections, *fulls, gains)


def tile_aligned(down, width, side, deep):
    return (
        lax.axis_size("fsdp") == 4
        and lax.axis_size("dp") in (2, 4, 8)
        and down % 96 == 0
        and width % 48 == 0
        and (2 * width) % 128 == 0
        and side % 128 == 0
        and deep % 128 == 0
    )


def adam_update(weight, mean_old, square_old, gradient, step_rate, decay_rate):
    mean_new = beta_one * mean_old + (1.0 - beta_one) * gradient
    square_new = beta_two * square_old + (1.0 - beta_two) * gradient * gradient
    corrected = (
        mean_new
        / (1.0 - beta_one**STEP)
        / (jnp.sqrt(square_new / (1.0 - beta_two**STEP)) + adam_epsilon)
    )
    master = weight - step_rate * (corrected + decay_rate * weight)
    return (mean_new, square_new, master, master.astype(bf16))


def on_device(
    hidden_in,
    patches,
    token_segments,
    patch_segments,
    cotangent,
    attention_weights,
    attention_means,
    attention_squares,
    inner_weights,
    inner_means,
    inner_squares,
    outer_weights,
    outer_means,
    outer_squares,
    norm_gains,
    gain_means,
    gain_squares,
):
    rows, _, length, _ = hidden_in.shape
    count = patches.shape[2]
    tokens = rows * length
    width, down = attention_weights.shape[1:]
    side, deep = inner_weights.shape[2], outer_weights.shape[0]
    direct = tile_aligned(down, width, side, deep)
    low_inner, low_outer = inner_weights.astype(bf16), outer_weights.astype(bf16)
    if direct:
        sizes = Sizes(down, width, side, deep)
        turned = jnp.swapaxes(attention_weights, 1, 2).astype(bf16)
        parts = norm_gains.shape[1]
        gain_block = jnp.pad(
            norm_gains.astype(bf16).astype(f32), ((0, 8 - norm_gains.shape[0]), (0, -parts % 128))
        )
        low, high, gains = gather_blocks(
            sizes, ("low", "high"), (turned[:4], turned[4:]), gain_block
        )
        gains = jnp.swapaxes(gains[:, : norm_gains.shape[0], :parts], 0, 1).reshape(-1, D)
        rest, rest_shards = ("inner", "outer"), (low_inner, low_outer.T)
    else:
        sizes = None
        gains = lax.all_gather(norm_gains.astype(bf16), "fsdp", axis=1, tiled=True)
        weights, inner, outer = gather_weights(
            attention_weights.astype(bf16), low_inner, low_outer
        )
        low, high = weights[:4], weights[4:]
        inner = jnp.concatenate([inner[0], inner[1]], axis=1)
        rest, rest_shards = (), ()

    initial = hidden_in.reshape(tokens, D).astype(f32)
    token_rows = token_segments.reshape(rows, 1, length)
    token_columns = token_segments.reshape(rows, length, 1)
    patch_columns = patch_segments.reshape(rows, count, 1)

    normed_one, unit_one, rms_one = norm_forward(initial, gains[0])
    packed = dot_nt(normed_one, low[0:3].reshape(3 * D, D)).astype(bf16)
    packed = packed.reshape(rows, length, 3 * D)
    mixture_one, lse_one = self_forward(packed, token_rows, token_columns)
    mixed_one = mixture_one.reshape(tokens, D)
    after_one = initial + dot_nt(mixed_one, low[3])
    normed_two, unit_two, rms_two = norm_forward(after_one, gains[1])
    cross_query = dot_nt(normed_two, high[0]).astype(bf16).reshape(rows, length, D)
    mixture_two, lse_two, cross_key, cross_value, *arrived = cross_forward(
        Rider(sizes, rest, "gather", 2, rows * PAIRS), cross_query, patches.reshape(rows, count, D), high,
        token_columns, patch_columns, rest_shards,
    )
    if direct:
        inner, outer = arrived
    mixed_two = mixture_two.reshape(tokens, D)
    after_two = after_one + dot_nt(mixed_two, high[3])
    normed_three, unit_three, rms_three = norm_forward(after_two, gains[2])
    gated = dot_nn(normed_three, inner)
    hidden_units = outer.shape[1]
    gate, up = gated[:, :hidden_units], gated[:, hidden_units:]
    units = (gelu_tanh(gate) * up).astype(bf16)
    hidden_out = (after_two + dot_nt(units, outer)).astype(bf16)

    grad_low = cotangent.reshape(tokens, D)
    grad_final = grad_low.astype(f32)
    grad_outer = dot_tn(grad_low, units).astype(bf16)
    grad_units = dot_nn(grad_low, outer)
    activation, gelu_back = jax.vjp(gelu_tanh, gate)
    grad_gated = jnp.concatenate(
        [gelu_back(grad_units * up)[0], grad_units * activation], axis=1
    ).astype(bf16)
    grad_inner = dot_tn(normed_three, grad_gated).astype(bf16)
    grad_normed = dot_nt(grad_gated, inner)
    grad_from_three, gain_three = norm_backward(grad_normed, gains[2], unit_three, rms_three)
    grad_two = grad_final + grad_from_three
    branch_two = grad_two.astype(bf16)
    grad_mixture_two = dot_nn(branch_two, high[3]).astype(bf16).reshape(rows, length, D)
    grad_cq, grad_ck, grad_cv, grad_pair, *summed_rest = cross_backward(
        Rider(sizes, rest, "scatter", 3, rows * PAIRS), cross_query, cross_key, cross_value,
        mixture_two, grad_mixture_two, lse_two, token_columns, patch_columns,
        patches.reshape(rows, count, D), (grad_inner, grad_outer) if direct else (),
    )
    grad_cq = grad_cq.reshape(tokens, D)
    grad_ck = grad_ck.reshape(rows * count, D)
    grad_cv = grad_cv.reshape(rows * count, D)
    grad_high = jnp.concatenate(
        [
            dot_tn(grad_cq, normed_two).astype(bf16)[None],
            grad_pair,
            dot_tn(branch_two, mixed_two).astype(bf16)[None],
        ]
    )
    grad_from_two, gain_two = norm_backward(
        dot_nn(grad_cq, high[0]), gains[1], unit_two, rms_two
    )
    grad_one = grad_two + grad_from_two
    branch_one = grad_one.astype(bf16)
    grad_mixture_one = dot_nn(branch_one, low[3]).astype(bf16).reshape(rows, length, D)
    grad_q, grad_k, grad_v = self_backward(
        packed, mixture_one, grad_mixture_one, lse_one, token_rows, token_columns
    )
    grad_q = grad_q.reshape(tokens, D)
    grad_k = grad_k.reshape(tokens, D)
    grad_v = grad_v.reshape(tokens, D)
    grad_normed_one = dot_nn(grad_q, low[0]) + dot_nn(grad_k, low[1]) + dot_nn(grad_v, low[2])
    grad_from_one, gain_one = norm_backward(grad_normed_one, gains[0], unit_one, rms_one)
    hidden_grad = grad_one + grad_from_one
    grad_first = jnp.stack(
        [
            dot_tn(grad_q, normed_one).astype(bf16),
            dot_tn(grad_k, normed_one).astype(bf16),
            dot_tn(grad_v, normed_one).astype(bf16),
            dot_tn(branch_one, mixed_one).astype(bf16),
        ]
    )
    gain_grads = jnp.stack([gain_one, gain_two, gain_three])
    if direct:
        own_inner, own_outer = summed_rest
        patch_grad, own_low, own_high, gain_totals = scatter_blocks(
            sizes, ("low", "high"), (grad_first, grad_high),
            jnp.pad(gain_grads, ((0, 5), (0, 0))), grad_ck, grad_cv, high,
        )
        own_attention = jnp.swapaxes(jnp.concatenate([own_low, own_high]), 1, 2)
        own_outer = own_outer.T
        gain_totals = gain_totals[:3]
    else:
        patch_grad = dot_nn(grad_ck, high[1]) + dot_nn(grad_cv, high[2])
        own_attention, own_inner, own_outer = scatter_grads(
            jnp.concatenate([grad_first, grad_high]),
            jnp.stack([grad_inner[:, :hidden_units], grad_inner[:, hidden_units:]]),
            grad_outer,
        )
        gain_totals = lax.psum(gain_grads, BOTH)
    width = norm_gains.shape[1]
    own_gains = lax.dynamic_slice_in_dim(
        gain_totals, lax.axis_index("fsdp") * width, width, axis=1
    )

    attention_new = adam_update(
        attention_weights, attention_means, attention_squares, own_attention,
        rate_matrix, decay_matrix,
    )
    inner_new = adam_update(
        inner_weights, inner_means, inner_squares, own_inner, rate_matrix, decay_matrix
    )
    outer_new = adam_update(
        outer_weights, outer_means, outer_squares, own_outer, rate_matrix, decay_matrix
    )
    gain_new = adam_update(norm_gains, gain_means, gain_squares, own_gains, rate_gain, 0.0)
    return (
        hidden_out.reshape(hidden_in.shape),
        hidden_grad.reshape(hidden_in.shape),
        patch_grad.reshape(patches.shape),
        *attention_new,
        *inner_new,
        *outer_new,
        *gain_new,
    )


def solution(mesh):
    rows = P(None, BOTH, None, None)
    ids = P(None, BOTH, None)
    matrix = P(None, "fsdp", "dp")
    down = P("fsdp", "dp")
    gain = P(None, "fsdp")
    return jax.shard_map(
        on_device,
        mesh=mesh,
        in_specs=(rows, rows, ids, ids, rows) + (matrix,) * 6 + (down,) * 3 + (gain,) * 3,
        out_specs=(rows, rows, rows) + (matrix,) * 8 + (down,) * 4 + (gain,) * 4,
        check_vma=False,
    )
```

```python
import functools

import jax
import jax.numpy as jnp
from jax import lax
from jax.experimental import pallas as pl
from jax.experimental.pallas import tpu as pltpu
from jax.sharding import PartitionSpec as P

D = 768
HEADS = 12
HEAD = 64
PAIR = 2 * HEAD
PAIRS = HEADS // 2
GROUP = 3
STEP = 10
SEGS = 4

epsilon = 1e-06
score_scale = 0.125
masked_value = -1000000000.0
beta_one = 0.9
beta_two = 0.95
adam_epsilon = 1e-08
decay_matrix = 0.1
rate_matrix = 0.1
rate_gain = 0.3
f32 = jnp.float32
bf16 = jnp.bfloat16
BOTH = ("dp", "fsdp")


def gelu_tanh(values):
    return (
        0.5
        * values
        * (1.0 + jnp.tanh(0.7978845608028654 * (values + 0.044715 * values * values * values)))
    )


def dot_nn(a, b):
    return lax.dot_general(a, b, (((1,), (0,)), ((), ())), preferred_element_type=f32)


def dot_nt(a, b):
    return lax.dot_general(a, b, (((1,), (1,)), ((), ())), preferred_element_type=f32)


def dot_tn(a, b):
    return lax.dot_general(a, b, (((0,), (0,)), ((), ())), preferred_element_type=f32)


def norm_forward(values, gain):
    inverse_rms = lax.rsqrt(jnp.mean(values * values, axis=-1, keepdims=True) + epsilon)
    unit_rows = values * inverse_rms
    return ((unit_rows * gain.astype(f32)).astype(bf16), unit_rows, inverse_rms)


def norm_backward(grad_rows, gain, unit_rows, inverse_rms):
    grad_unit = grad_rows * gain.astype(f32)
    grad_values = inverse_rms * (
        grad_unit - unit_rows * jnp.mean(grad_unit * unit_rows, axis=-1, keepdims=True)
    )
    return (grad_values, jnp.sum(grad_rows * unit_rows, axis=0))


def head_half(block, half):
    lane = lax.broadcasted_iota(jnp.int32, block.shape, 1)
    keep = (lane < HEAD) if half == 0 else (lane >= HEAD)
    return jnp.where(keep, block, jnp.zeros_like(block))


def three_parts(column):
    high = column.astype(bf16).astype(f32)
    rest = column - high
    middle = rest.astype(bf16).astype(f32)
    low = rest - middle
    return high, middle, low


def stat_lanes(base, column, first):
    lane = lax.broadcasted_iota(jnp.int32, base.shape, 1)
    for place, part in enumerate(three_parts(column)):
        base = jnp.where(lane == first + place, -part, base)
    return base


def key_marks(key_ids, stats):
    lane = lax.broadcasted_iota(jnp.int32, (key_ids.shape[0], 128), 1)
    marks = lane == key_ids
    if stats:
        marks = marks | ((lane >= SEGS) & (lane < SEGS + 3))
    return jnp.where(marks, 1.0, 0.0).astype(bf16)


def query_bias(query_ids):
    lane = lax.broadcasted_iota(jnp.int32, (query_ids.shape[0], 128), 1)
    return jnp.where((lane == query_ids) | (lane >= SEGS), 0.0, masked_value)


def softmax_columns(scores):
    top = jnp.max(scores, axis=0, keepdims=True)
    raised = jnp.exp(scores - top)
    return raised, top, jnp.sum(raised, axis=0, keepdims=True)


def finish_forward(halves, tops, sums):
    mixed = jnp.concatenate([h / s for h, s in zip(halves, sums)], axis=0)
    rows = [t + jnp.log(s) for t, s in zip(tops, sums)]
    pad = jnp.zeros((6, rows[0].shape[1]), f32)
    return mixed.T.astype(bf16), jnp.concatenate(rows + [pad], axis=0)


def cross_forward_kernel(rider, q_ref, c_ref, wk_ref, wv_ref, qid_ref, kid_ref, *refs):
    (o_ref, lse_ref, k_ref, v_ref) = rider.board(refs, 4)
    both = jnp.concatenate([wk_ref[0], wv_ref[0]], axis=0)
    projected = dot_nt(c_ref[0], both).astype(bf16)
    key, value = projected[:, :PAIR], projected[:, PAIR:]
    k_ref[0], v_ref[0] = key, value
    marked = jnp.concatenate([key, key_marks(kid_ref[0], False)], axis=1)
    bias = query_bias(qid_ref[0]).astype(bf16)
    query = q_ref[0] * jnp.asarray(score_scale, bf16)
    values = value.T
    halves, tops, sums = [], [], []
    scored = [
        dot_nt(marked, jnp.concatenate([head_half(query, half), bias], axis=1))
        for half in range(2)
    ]
    for half in range(2):
        raised, top, total = softmax_columns(scored[half])
        halves.append(dot_nn(values[half * HEAD : (half + 1) * HEAD], raised.astype(bf16)))
        tops.append(top)
        sums.append(total)
    o_ref[0], lse_ref[0, 0] = finish_forward(halves, tops, sums)
    rider.leave()


def causal_mask(qid_ref, kid_ref):
    length = kid_ref.shape[1]
    key = lax.broadcasted_iota(jnp.int32, (length, length), 0)
    query = lax.broadcasted_iota(jnp.int32, (length, length), 1)
    return (key <= query) & (kid_ref[0] == qid_ref[0])


def pair_lanes(pair):
    return slice(pair * PAIR, (pair + 1) * PAIR)


def self_forward_kernel(q_ref, k_ref, v_ref, qid_ref, kid_ref, o_ref, lse_ref):
    allowed = causal_mask(qid_ref, kid_ref)
    for pair in range(GROUP):
        lanes = pair_lanes(pair)
        query = q_ref[0, :, lanes] * jnp.asarray(score_scale, bf16)
        key = k_ref[0, :, lanes]
        values = v_ref[0, :, lanes].T
        halves, tops, sums = [], [], []
        for half in range(2):
            scores = jnp.where(allowed, dot_nt(key, head_half(query, half)), masked_value)
            raised, top, total = softmax_columns(scores)
            halves.append(dot_nn(values[half * HEAD : (half + 1) * HEAD], raised.astype(bf16)))
            tops.append(top)
            sums.append(total)
        o_ref[0, :, lanes], lse_ref[0, pair] = finish_forward(halves, tops, sums)


def backward_pair(query, key, value, mixed, grad, lse, marked, bias, allowed):
    scaled = query * jnp.asarray(score_scale, bf16)
    key_turned = key.T
    length = query.shape[0]
    lse_columns = lse.T
    product = mixed.astype(f32) * grad.astype(f32)
    ones = key_marks(jnp.full((value.shape[0], 1), -1, jnp.int32), True)
    valued = jnp.concatenate([value, ones], axis=1)
    scored, shifted = [], []
    for half in range(2):
        stats = stat_lanes(bias, lse_columns[:, half : half + 1], SEGS).astype(bf16)
        scored.append(
            dot_nt(marked, jnp.concatenate([head_half(scaled, half), stats], axis=1)))
        inner = jnp.sum(head_half(product, half), axis=1, keepdims=True)
        delta = stat_lanes(jnp.zeros((length, 128), f32), inner, SEGS).astype(bf16)
        shifted.append(dot_nt(valued, jnp.concatenate([head_half(grad, half), delta], axis=1)))
    probs, grads, turned = [], [], []
    for half in range(2):
        scores = scored[half]
        if allowed is not None:
            scores = jnp.where(allowed, scores, masked_value)
        weight = jnp.exp(scores)
        grad_scores = (weight * shifted[half]).astype(bf16)
        probs.append(weight.astype(bf16))
        grads.append(grad_scores)
        turned.append(dot_nn(key_turned[half * HEAD : (half + 1) * HEAD], grad_scores))
    grad_query = (score_scale * jnp.concatenate(turned, axis=0)).T.astype(bf16)
    grad_turned, scaled_turned = grad.T, scaled.T
    halves = [slice(0, HEAD), slice(HEAD, PAIR)]
    value_turned = jnp.concatenate(
        [dot_nt(grad_turned[h], p) for h, p in zip(halves, probs)], axis=0).astype(bf16)
    keyed_turned = jnp.concatenate(
        [dot_nt(scaled_turned[h], p) for h, p in zip(halves, grads)], axis=0).astype(bf16)
    grad_value, grad_key = value_turned.T, keyed_turned.T
    return grad_query, grad_key, grad_value, keyed_turned, value_turned


def cross_backward_kernel(rider, q_ref, k_ref, v_ref, o_ref, do_ref, lse_ref, qid_ref, kid_ref,
                          c_ref, *refs):
    total_ref = refs[-1]
    dq_ref, dk_ref, dv_ref, sum_ref = rider.board(refs[:-1], 4)
    marked = jnp.concatenate([k_ref[0], key_marks(kid_ref[0], True)], axis=1)
    dq_ref[0], grad_key, grad_value, key_t, value_t = backward_pair(
        q_ref[0], k_ref[0], v_ref[0], o_ref[0], do_ref[0], lse_ref[0, 0], marked,
        query_bias(qid_ref[0]), None)
    dk_ref[0], dv_ref[0] = grad_key, grad_value
    row, pair = pl.program_id(0), pl.program_id(1)
    part = dot_nn(jnp.concatenate([key_t, value_t], axis=0), c_ref[0])

    @pl.when(row == 0)
    def _():
        total_ref[pair] = part

    @pl.when(row > 0)
    def _():
        total_ref[pair] = total_ref[pair] + part

    @pl.when(row == pl.num_programs(0) - 1)
    def _():
        at = pl.ds(pl.multiple_of(pair * PAIR, PAIR), PAIR)
        sum_ref[0, at] = total_ref[pair, :PAIR].astype(bf16)
        sum_ref[1, at] = total_ref[pair, PAIR:].astype(bf16)

    rider.leave()


def self_backward_kernel(q_ref, k_ref, v_ref, o_ref, do_ref, lse_ref, qid_ref, kid_ref,
                         dq_ref, dk_ref, dv_ref):
    length = k_ref.shape[1]
    ones = key_marks(jnp.full((length, 1), -1, jnp.int32), True)
    allowed = causal_mask(qid_ref, kid_ref)
    for pair in range(GROUP):
        lanes = pair_lanes(pair)
        key = k_ref[0, :, lanes]
        dq_ref[0, :, lanes], dk_ref[0, :, lanes], dv_ref[0, :, lanes] = backward_pair(
            q_ref[0, :, lanes], key, v_ref[0, :, lanes], o_ref[0, :, lanes],
            do_ref[0, :, lanes], lse_ref[0, pair], jnp.concatenate([key, ones], axis=1),
            jnp.zeros((length, 128), f32), allowed)[:3]


def pair_spec(length, offset, pairs=1):
    return pl.BlockSpec((1, length, pairs * PAIR), lambda row, step: (row, 0, offset + step))


def row_spec(shape):
    return pl.BlockSpec((1,) + shape, lambda row, step: (row, 0, 0))


def stat_spec(length, pairs=1):
    return pl.BlockSpec((1, pairs, 8, length), lambda row, step: (row, step, 0, 0))


def cost(rows, queries, keys, products):
    elements = rows * HEADS * queries * keys
    return pl.CostEstimate(
        flops=2 * elements * 256 * products // 2,
        transcendentals=elements,
        bytes_accessed=rows * (queries + keys) * D * 2 * 3,
    )


class Rider:
    def __init__(self, sizes, names, kind, number, steps):
        self.sizes, self.names, self.kind, self.number = sizes, names, kind, number
        self.steps = steps

    def board(self, refs, outputs):
        count = len(self.names)
        theirs, mine, scratch = refs[:count], refs[count : count + outputs], refs[count + outputs :]
        if count:
            ends, scratch = scratch[:count], scratch[count:]
            build = gather_stages if self.kind == "gather" else scatter_stages
            stages = build(self.sizes, self.names, theirs, ends, scratch)
            step = pl.program_id(0) * pl.num_programs(1) + pl.program_id(1)
            for number in range(self.steps):
                run_stages(stages, step, number, self.steps)
            self.rest = ([s for time, s in stages if time >= 12], step == self.steps - 1)
        return mine

    def leave(self):
        if self.names and self.rest[0]:
            pl.when(self.rest[1])(functools.partial(in_turn, self.rest[0]))

    def in_specs(self):
        return [VMEM if self.kind == "gather" else HBM] * len(self.names)

    def out_specs(self):
        return [HBM if self.kind == "gather" else VMEM] * len(self.names)

    def out_shape(self):
        if self.kind == "gather":
            return [jax.ShapeDtypeStruct(self.sizes.full(n), bf16) for n in self.names]
        return [jax.ShapeDtypeStruct(self.sizes.shard(n), f32) for n in self.names]

    def scratch(self):
        if not self.names:
            return []
        build = gather_scratch if self.kind == "gather" else scatter_scratch
        return build(self.sizes, self.names)

    def params(self):
        if not self.names:
            return pltpu.CompilerParams()
        return pltpu.CompilerParams(
            collective_id=self.number, has_side_effects=True, vmem_limit_bytes=60 * 1024 * 1024
        )


def self_forward(packed, query_ids, key_ids):
    rows, length = packed.shape[:2]
    steps = PAIRS // GROUP
    return pl.pallas_call(
        self_forward_kernel,
        grid=(rows, steps),
        in_specs=[pair_spec(length, part * steps, GROUP) for part in range(3)]
        + [row_spec((1, length)), row_spec((length, 1))],
        out_specs=[pair_spec(length, 0, GROUP), stat_spec(length, GROUP)],
        out_shape=[
            jax.ShapeDtypeStruct((rows, length, D), bf16),
            jax.ShapeDtypeStruct((rows, PAIRS, 8, length), f32),
        ],
        cost_estimate=cost(rows, length, length, 2),
        name="self_forward",
    )(packed, packed, packed, query_ids, key_ids)


def self_backward(packed, mixed, grad, lse, query_ids, key_ids):
    rows, length = packed.shape[:2]
    steps = PAIRS // GROUP
    plain = pair_spec(length, 0, GROUP)
    return pl.pallas_call(
        self_backward_kernel,
        grid=(rows, steps),
        in_specs=[pair_spec(length, part * steps, GROUP) for part in range(3)]
        + [plain, plain, stat_spec(length, GROUP), row_spec((1, length)), row_spec((length, 1))],
        out_specs=[plain] * 3,
        out_shape=[jax.ShapeDtypeStruct((rows, length, D), bf16)] * 3,
        cost_estimate=cost(rows, length, length, 5),
        name="self_backward",
    )(packed, packed, packed, mixed, grad, lse, query_ids, key_ids)


def cross_forward(rider, queries, patches, projections, query_ids, key_ids, shards):
    rows, length = queries.shape[:2]
    count = patches.shape[1]

    def slab(which):
        return pl.BlockSpec((1, PAIR, D), lambda row, pair: (which, pair, 0))

    return pl.pallas_call(
        functools.partial(cross_forward_kernel, rider),
        grid=(rows, PAIRS),
        in_specs=[
            pair_spec(length, 0),
            row_spec((count, D)),
            slab(1),
            slab(2),
            row_spec((length, 1)),
            row_spec((count, 1)),
        ]
        + rider.in_specs(),
        out_specs=[
            pair_spec(length, 0), stat_spec(length), pair_spec(count, 0), pair_spec(count, 0),
        ]
        + rider.out_specs(),
        out_shape=[
            jax.ShapeDtypeStruct((rows, length, D), bf16),
            jax.ShapeDtypeStruct((rows, PAIRS, 8, length), f32),
            jax.ShapeDtypeStruct((rows, count, D), bf16),
            jax.ShapeDtypeStruct((rows, count, D), bf16),
        ]
        + rider.out_shape(),
        scratch_shapes=rider.scratch(),
        compiler_params=rider.params(),
        cost_estimate=cost(rows, length, count, 4),
        name="cross_forward",
    )(queries, patches, projections, projections, query_ids, key_ids, *shards)


def cross_backward(rider, queries, keys, values, mixed, grad, lse, query_ids, key_ids, patches,
                   fulls):
    rows, length = grad.shape[:2]
    count = keys.shape[1]
    short, tall = pair_spec(length, 0), pair_spec(count, 0)
    return pl.pallas_call(
        functools.partial(cross_backward_kernel, rider),
        grid=(rows, PAIRS),
        in_specs=[
            short, tall, tall, short, short, stat_spec(length), row_spec((length, 1)),
            row_spec((count, 1)), row_spec((count, D)),
        ]
        + rider.in_specs(),
        out_specs=[short, tall, tall, VMEM] + rider.out_specs(),
        out_shape=[
            jax.ShapeDtypeStruct((rows, length, D), bf16),
            jax.ShapeDtypeStruct((rows, count, D), bf16),
            jax.ShapeDtypeStruct((rows, count, D), bf16),
            jax.ShapeDtypeStruct((2, D, D), bf16),
        ]
        + rider.out_shape(),
        scratch_shapes=rider.scratch() + [pltpu.VMEM((PAIRS, 2 * PAIR, D), f32)],
        compiler_params=rider.params(),
        cost_estimate=cost(rows, length, count, 7),
        name="cross_backward",
    )(queries, keys, values, mixed, grad, lse, query_ids, key_ids, patches, *fulls)


def gather_weights(attention, inner, outer):
    turned = lax.all_gather(jnp.swapaxes(attention, 1, 2), BOTH, axis=0, tiled=False)
    heads = lax.axis_size("dp"), lax.axis_size("fsdp")
    turned = turned.reshape(heads + turned.shape[1:])
    full_attention = jnp.transpose(turned, (2, 0, 3, 1, 4)).reshape(8, D, D)
    wide = lax.all_gather(inner, BOTH, axis=0, tiled=False)
    wide = wide.reshape(heads + wide.shape[1:])
    full_inner = jnp.transpose(wide, (2, 1, 3, 0, 4)).reshape(2, D, -1)
    tall = lax.all_gather(outer.T, BOTH, axis=0, tiled=False)
    tall = tall.reshape(heads + tall.shape[1:])
    full_outer = jnp.transpose(tall, (0, 2, 1, 3)).reshape(D, -1)
    return full_attention, full_inner, full_outer


def scatter_grads(attention, inner, outer):
    across, within = lax.axis_size("dp"), lax.axis_size("fsdp")
    blocks = attention.reshape(8, across, D // across, within, D // within)
    blocks = jnp.transpose(blocks, (1, 3, 0, 2, 4))
    blocks = blocks.reshape((across * within,) + blocks.shape[2:])
    own_attention = lax.psum_scatter(blocks, BOTH, scatter_dimension=0, tiled=False)
    blocks = inner.reshape(2, within, D // within, across, inner.shape[2] // across)
    blocks = jnp.transpose(blocks, (3, 1, 0, 2, 4))
    blocks = blocks.reshape((across * within,) + blocks.shape[2:])
    own_inner = lax.psum_scatter(blocks, BOTH, scatter_dimension=0, tiled=False)
    blocks = outer.reshape(across, D // across, within, outer.shape[1] // within)
    blocks = jnp.transpose(blocks, (0, 2, 1, 3))
    blocks = blocks.reshape((across * within,) + blocks.shape[2:])
    own_outer = lax.psum_scatter(blocks, BOTH, scatter_dimension=0, tiled=False)
    return (
        jnp.swapaxes(own_attention, 1, 2).astype(f32),
        own_inner.astype(f32),
        own_outer.T.astype(f32),
    )


MESH = pl.DeviceIdType.MESH
RIGHT, LEFT, TO_Y, TO_X, TO_CORE = range(5)


def where_am_i():
    across, within = lax.axis_index("dp"), lax.axis_index("fsdp")
    return across // 2, across % 2, within // 2, within % 2


def device_at(z, y, x, core):
    return (2 * z + y, 2 * x + core)


def aligned(value, unit):
    return pl.multiple_of(value * unit, unit)


class Sizes:
    def __init__(self, down, width, side, deep):
        self.down, self.width, self.side, self.deep = down, width, side, deep
        self.across, self.within = D // down, D // width
        self.depth = self.across // 2
        self.chips = self.across * self.within // 2

    def shard(self, name):
        return {
            "low": (4, self.down, self.width),
            "high": (4, self.down, self.width),
            "inner": (2, self.width, self.side),
            "outer": (self.down, self.deep),
        }[name]

    def full(self, name):
        return {
            "low": (4, D, D),
            "high": (4, D, D),
            "inner": (D, 2 * self.across * self.side),
            "outer": (D, self.within * self.deep),
        }[name]

    def piece(self, name):
        return {
            "low": (self.down, 2 * self.width),
            "high": (self.down, 2 * self.width),
            "inner": (self.width, self.side),
            "outer": (self.down // 2, self.deep),
        }[name]

    def part(self, name):
        return {
            "low": (2, self.down, self.width),
            "high": (2, self.down, self.width),
            "inner": (self.width, self.side),
            "outer": (self.down // 2, self.deep),
        }[name]

    def place(self, name, ref, cut, z, y, x, half):
        place = 2 * z + y
        if name == "inner":
            return ref.at[
                pl.ds(aligned(2 * x + cut, self.width), self.width),
                pl.ds(aligned(half * self.across + place, self.side), self.side),
            ]
        if name == "outer":
            return ref.at[
                pl.ds(aligned(2 * place + half, self.down // 2), self.down // 2),
                pl.ds(aligned(2 * x + cut, self.deep), self.deep),
            ]
        return ref.at[
            2 * half + cut,
            pl.ds(aligned(place, self.down), self.down),
            pl.ds(aligned(x, 2 * self.width), 2 * self.width),
        ]

    def share(self, name, ref, half):
        if name == "inner":
            return ref.at[half]
        if name == "outer":
            return ref.at[pl.ds(aligned(half, self.down // 2), self.down // 2)]
        return ref.at[pl.ds(2 * half, 2)]


def greet(depth):
    z, y, x, core = where_am_i()
    barrier = pltpu.get_barrier_semaphore()

    def signal(device):
        pl.semaphore_signal(barrier, inc=1, device_id=device, device_id_type=MESH)

    signal(device_at(z, y, x, 1 - core))
    signal(device_at(z, y, 1 - x, core))
    signal(device_at(z, 1 - y, x, core))
    pl.when(z > 0)(lambda: signal(device_at(z - 1, y, x, core)))
    pl.when(z < depth - 1)(lambda: signal(device_at(z + 1, y, x, core)))
    pl.semaphore_wait(barrier, 3 + jnp.where(z > 0, 1, 0) + jnp.where(z < depth - 1, 1, 0))


def chip_index(bz, by, bx):
    return (2 * bz + by) * 2 + bx


def remote(src, dst, send, recv, device):
    return pltpu.make_async_remote_copy(
        src_ref=src, dst_ref=dst, send_sem=send, recv_sem=recv, device_id=device,
        device_id_type=MESH)


def gather_scratch(sizes, names):
    wave = pltpu.SemaphoreType.DMA
    count, pieces = len(names), 2 * len(names)
    return (
        [pltpu.VMEM((2,) + sizes.piece(name), bf16) for name in names]
        + [pltpu.VMEM(sizes.part(name), bf16) for name in names]
        + [wave((count,)), wave((count,)), wave((pieces,)), wave((pieces, 5, sizes.chips)),
           wave((pieces, 2, sizes.chips))]
    )


def gather_stages(sizes, names, shards, fulls, scratch):
    count, depth = len(names), sizes.depth
    pairs, got = scratch[:count], scratch[count : 2 * count]
    swap_send, swap_recv, own_sem, send_sem, recv_sem = scratch[2 * count :]
    z, y, x, core = where_am_i()
    other = 1 - core
    pieces = [(n, cut) for cut in range(2) for n in range(count)]

    def place(piece, bz, by, bx, half):
        n, cut = pieces[piece]
        return sizes.place(names[n], fulls[n], cut, bz, by, bx, half)

    def swap(n):
        return remote(sizes.share(names[n], shards[n], other), got[n], swap_send.at[n],
                      swap_recv.at[n], device_at(z, y, x, other))

    def merge(n, me):
        if names[n] in ("low", "high"):
            width = sizes.width
            for part, source in ((me, shards[n][2 * me : 2 * me + 2]), (1 - me, got[n][...])):
                pairs[n][:, :, part * width : (part + 1) * width] = source
        else:
            half = sizes.down // 2
            mine = shards[n][me] if names[n] == "inner" else shards[n][me * half : (me + 1) * half]
            pairs[n][me] = mine
            pairs[n][1 - me] = got[n][...]

    def copy(piece, bz, by, bx, kind, own=False):
        target = {
            RIGHT: device_at(z + 1, y, x, core),
            LEFT: device_at(z - 1, y, x, core),
            TO_Y: device_at(z, 1 - y, x, core),
            TO_X: device_at(z, y, 1 - x, core),
            TO_CORE: device_at(z, y, x, other),
        }[kind]
        spot = place(piece, bz, by, bx, core)
        n, cut = pieces[piece]
        slot = chip_index(bz, by, bx)
        return remote(pairs[n].at[cut] if own else spot, spot, send_sem.at[piece, kind, slot],
                      recv_sem.at[piece, 1 if kind == TO_CORE else 0, slot], target)

    def arrive(piece, bz, by, bx, from_core=False):
        spot = place(piece, bz, by, bx, other if from_core else core)
        remote(spot, spot, send_sem.at[piece, 0, 0],
               recv_sem.at[piece, 1 if from_core else 0, chip_index(bz, by, bx)],
               device_at(z, y, x, other)).wait_recv()

    def keep(piece):
        n, cut = pieces[piece]
        return pltpu.make_async_copy(pairs[n].at[cut], place(piece, z, y, x, core),
                                     own_sem.at[piece])

    every = range(len(pieces))
    first, later = every[:count], every[count:]

    def launch(kind):
        for piece in every:
            copy(piece, z, y, x, kind, True).start()

    def begin():
        greet(depth)
        for n in range(count):
            swap(n).start()

    def send_own():
        for n in range(count):
            swap(n).wait_recv()
        for me in range(2):
            @pl.when(core == me)
            def _(me=me):
                for n in range(count):
                    merge(n, me)
        pl.when(z < depth - 1)(lambda: launch(RIGHT))
        pl.when(z > 0)(lambda: launch(LEFT))
        for piece in every:
            copy(piece, z, y, x, TO_Y, True).start()
            copy(piece, z, y, x, TO_X, True).start()
        for piece in every:
            copy(piece, z, y, x, TO_CORE, True).start()
            keep(piece).start()

    def from_z(bz, kind, further):
        for piece in every:
            arrive(piece, bz, y, x)
            pl.when(further)(lambda piece=piece: copy(piece, bz, y, x, kind).start())
            copy(piece, bz, y, x, TO_Y).start()
            copy(piece, bz, y, x, TO_X).start()
            copy(piece, bz, y, x, TO_CORE).start()

    def from_sides(bz):
        for early, late in zip(first, later):
            arrive(early, bz, 1 - y, x)
            copy(early, bz, 1 - y, x, TO_X).start()
            copy(early, bz, 1 - y, x, TO_CORE).start()
            arrive(late, bz, y, 1 - x)
            copy(late, bz, y, 1 - x, TO_Y).start()
            copy(late, bz, y, 1 - x, TO_CORE).start()
        for early, late in zip(first, later):
            arrive(early, bz, y, 1 - x)
            copy(early, bz, y, 1 - x, TO_CORE).start()
            arrive(late, bz, 1 - y, x)
            copy(late, bz, 1 - y, x, TO_CORE).start()

    def from_corner(bz):
        for piece in every:
            arrive(piece, bz, 1 - y, 1 - x)
            copy(piece, bz, 1 - y, 1 - x, TO_CORE).start()

    def both_ways(step, action):
        if step == 0:
            action(z)
            return
        pl.when(z - step >= 0)(lambda: action(z - step))
        pl.when(z + step < depth)(lambda: action(z + step))

    def line(step):
        pl.when(z - step >= 0)(lambda: from_z(z - step, RIGHT, z < depth - 1))
        pl.when(z + step < depth)(lambda: from_z(z + step, LEFT, z > 0))

    def end():
        for n in range(count):
            swap(n).wait_send()
        for piece in every:
            keep(piece).wait()

            @pl.loop(0, depth)
            def _(bz, piece=piece):
                for by in range(2):
                    for bx in range(2):
                        arrive(piece, bz, by, bx, True)
                        copy(piece, bz, by, bx, TO_CORE).wait_send()
                copy(piece, bz, y, x, TO_Y).wait_send()
                copy(piece, bz, y, x, TO_X).wait_send()
                if piece in first:
                    copy(piece, bz, 1 - y, x, TO_X).wait_send()
                else:
                    copy(piece, bz, y, 1 - x, TO_Y).wait_send()
                pl.when((bz <= z) & (z < depth - 1))(
                    lambda: copy(piece, bz, y, x, RIGHT).wait_send())
                pl.when((bz >= z) & (z > 0))(lambda: copy(piece, bz, y, x, LEFT).wait_send())

    timed = [(0, begin), (0, send_own), (12, end)]
    for step in range(1, depth):
        timed.append((2 * step, functools.partial(line, step)))
    for step in range(depth):
        timed.append(((3, 6, 8, 9)[step], functools.partial(both_ways, step, from_sides)))
        timed.append(((10, 10, 11, 11)[step], functools.partial(both_ways, step, from_corner)))
    return sorted(timed, key=lambda item: item[0])


def add_rows(target, sources):
    slab = 48

    def total(k):
        at = pl.ds(aligned(k, slab), slab)
        value = sources[0][at].astype(f32)
        for source in sources[1:]:
            value = value + source[at].astype(f32)
        target[at] = value.astype(target.dtype)

    pl.loop(0, target.shape[0] // slab)(total)


def scatter_scratch(sizes, names):
    wave = pltpu.SemaphoreType.DMA
    count, pieces, depth, chips = len(names), 2 * len(names), sizes.depth, sizes.chips

    def buffers(lead, kind):
        return [pltpu.VMEM(lead + (2,) + sizes.piece(name), kind) for name in names]

    return (
        buffers((chips,), bf16) + buffers((chips,), bf16) + buffers((2 * depth,), bf16)
        + buffers((depth,), bf16) + buffers((2, depth), bf16) + buffers((), f32)
        + [pltpu.VMEM(sizes.part(name), f32) for name in names]
        + [pltpu.VMEM(sizes.part(name), f32) for name in names]
        + [wave((pieces, chips))] * 3 + [wave((pieces, 2 * depth))] * 2
        + [wave((pieces, depth))] * 2 + [wave((pieces, 2, depth))] * 2 + [wave((count,))] * 2
    )


def scatter_stages(sizes, names, fulls, owns, scratch):
    count, depth = len(names), sizes.depth
    acc, swapped, first, second, line, sums, outs, ins = (
        scratch[k * count : (k + 1) * count] for k in range(8)
    )
    (load_sem, swap_send, swap_recv, one_send, one_recv, two_send, two_recv, line_send,
     line_recv, end_send, end_recv) = scratch[8 * count :]
    z, y, x, core = where_am_i()
    other = 1 - core
    partner = device_at(z, y, x, other)
    over_x, over_y = device_at(z, y, 1 - x, core), device_at(z, 1 - y, x, core)
    pieces = [(n, cut) for cut in range(2) for n in range(count)]
    every = range(len(pieces))
    order = sorted(range(depth), key=lambda spot: (-abs(2 * spot - depth + 1), -spot))

    def at(buffers, piece, *index):
        n, cut = pieces[piece]
        return buffers[n].at[(*index, cut)]

    def block(piece, bz, by, bx, half):
        n, cut = pieces[piece]
        return sizes.place(names[n], fulls[n], cut, bz, by, bx, half)

    def load(piece, bz, by, bx):
        slot = chip_index(bz, by, bx)
        return pltpu.make_async_copy(block(piece, bz, by, bx, core), at(acc, piece, slot),
                                     load_sem.at[piece, slot])

    def swap(piece, bz, by, bx):
        slot = chip_index(bz, by, bx)
        return remote(block(piece, bz, by, bx, other), at(swapped, piece, slot),
                      swap_send.at[piece, slot], swap_recv.at[piece, slot], partner)

    def turned(piece):
        return pieces[piece][1] == 1

    def stage_one(piece, bz, spot):
        if turned(piece):
            far, device = chip_index(bz, 1 - y, spot), over_y
        else:
            far, device = chip_index(bz, spot, 1 - x), over_x
        slot = 2 * bz + spot
        return remote(at(acc, piece, far), at(first, piece, slot), one_send.at[piece, slot],
                      one_recv.at[piece, slot], device)

    def stage_two(piece, bz):
        if turned(piece):
            far, device = chip_index(bz, y, 1 - x), over_x
        else:
            far, device = chip_index(bz, 1 - y, x), over_y
        return remote(at(acc, piece, far), at(second, piece, bz), two_send.at[piece, bz],
                      two_recv.at[piece, bz], device)

    def along(piece, bz, way):
        device = device_at(z + 1, y, x, core) if way == 0 else device_at(z - 1, y, x, core)
        return remote(at(acc, piece, chip_index(bz, y, x)), at(line, piece, way, bz),
                      line_send.at[piece, way, bz], line_recv.at[piece, way, bz], device)

    def begin():
        greet(depth)
        for bz in order:
            for flip_y, flip_x in ((1, 1), (0, 1), (1, 0), (0, 0)):
                for piece in every:
                    if turned(piece):
                        flip_y, flip_x = flip_x, flip_y
                    by = 1 - y if flip_y else y
                    bx = 1 - x if flip_x else x
                    swap(piece, bz, by, bx).start()
                    load(piece, bz, by, bx).start()
                    if turned(piece):
                        flip_y, flip_x = flip_x, flip_y

    def join(piece, bz, by, bx, extra=()):
        load(piece, bz, by, bx).wait()
        swap(piece, bz, by, bx).wait_recv()
        mine = at(acc, piece, chip_index(bz, by, bx))
        add_rows(mine, (mine, at(swapped, piece, chip_index(bz, by, bx))) + extra)

    def send_first(bz):
        for far in range(2):
            for piece in every:
                if turned(piece):
                    spot = x if far else 1 - x
                    join(piece, bz, 1 - y, spot)
                else:
                    spot = y if far else 1 - y
                    join(piece, bz, spot, 1 - x)
                stage_one(piece, bz, spot).start()

    def send_second(bz):
        for piece in every:
            spot = 1 - x if turned(piece) else 1 - y
            stage_one(piece, bz, spot).wait_recv()
            arrived = (at(first, piece, 2 * bz + spot),)
            if turned(piece):
                join(piece, bz, y, spot, arrived)
            else:
                join(piece, bz, spot, x, arrived)
            stage_two(piece, bz).start()

    def gathered(piece, bz):
        spot = x if turned(piece) else y
        stage_one(piece, bz, spot).wait_recv()
        stage_two(piece, bz).wait_recv()
        load(piece, bz, y, x).wait()
        swap(piece, bz, y, x).wait_recv()
        mine = at(acc, piece, chip_index(bz, y, x))
        return mine, (mine, at(swapped, piece, chip_index(bz, y, x)),
                      at(first, piece, 2 * bz + spot), at(second, piece, bz))

    def pass_on(bz, level, way):
        for piece in every:
            mine, base = gathered(piece, bz)
            if level > 0:
                along(piece, bz, way).wait_recv()
                base = base + (at(line, piece, way, bz),)
            add_rows(mine, base)
            along(piece, bz, way).start()

    def pass_level(bz, level):
        if level < bz:
            pl.when(z == level)(lambda: pass_on(bz, level, 0))
        if depth - 1 - level > bz:
            pl.when(z == depth - 1 - level)(lambda: pass_on(bz, level, 1))

    def finish(bz):
        @pl.when(z == bz)
        def _():
            ways = ((0,) if bz > 0 else ()) + ((1,) if bz < depth - 1 else ())
            for piece in every:
                n, cut = pieces[piece]
                _, base = gathered(piece, bz)
                for way in ways:
                    along(piece, bz, way).wait_recv()
                add_rows(sums[n].at[cut], base + tuple(at(line, piece, way, bz) for way in ways))

    def exchange(n):
        return remote(outs[n], ins[n], end_send.at[n], end_recv.at[n], partner)

    width, half = sizes.width, sizes.down // 2

    def hand_over():
        for me in range(2):
            @pl.when(core == me)
            def _(me=me):
                far = 1 - me
                for n, name in enumerate(names):
                    if name == "inner":
                        outs[n][...] = sums[n][far]
                        owns[n][me] = sums[n][me]
                    elif name == "outer":
                        outs[n][...] = sums[n][far]
                        owns[n][me * half : (me + 1) * half] = sums[n][me]
                    else:
                        outs[n][...] = sums[n][:, :, far * width : (far + 1) * width]
                        owns[n][2 * me : 2 * me + 2] = sums[n][:, :, me * width : (me + 1) * width]
        for n in range(count):
            exchange(n).start()

    def end():
        for n in range(count):
            exchange(n).wait_recv()
        for me in range(2):
            @pl.when(core == me)
            def _(me=me):
                far = 1 - me
                for n, name in enumerate(names):
                    if name == "inner":
                        owns[n][far] = ins[n][...]
                    elif name == "outer":
                        owns[n][far * half : (far + 1) * half] = ins[n][...]
                    else:
                        owns[n][2 * far : 2 * far + 2] = ins[n][...]
        for n in range(count):
            exchange(n).wait_send()
        for piece in every:
            @pl.loop(0, depth)
            def _(bz, piece=piece):
                for by in range(2):
                    for bx in range(2):
                        swap(piece, bz, by, bx).wait_send()
                for spot in range(2):
                    stage_one(piece, bz, spot).wait_send()
                stage_two(piece, bz).wait_send()
                pl.when(z < bz)(lambda: along(piece, bz, 0).wait_send())
                pl.when(z > bz)(lambda: along(piece, bz, 1).wait_send())

    timed = [(0, begin)]
    for turn, bz in enumerate(order):
        timed.append((turn, functools.partial(send_first, bz)))
        timed.append(((2, 4, 5, 7)[turn], functools.partial(send_second, bz)))
        for level in range(depth - 1):
            when = ((4, 6, 8), (8, 10, 12), (9, 11, 12), (9, 12, 12))[turn][level]
            timed.append((when, functools.partial(pass_level, bz, level)))
    ending = [functools.partial(finish, bz) for bz in order] + [hand_over, end]
    timed.append((13, functools.partial(in_turn, ending)))
    return sorted(timed, key=lambda item: item[0])


def in_turn(actions):
    for action in actions:
        action()


def run_stages(timed, step, number, steps):
    mine = [stage for time, stage in timed if time < 12 and time * steps // 12 == number]
    if mine:
        pl.when(step == number)(functools.partial(in_turn, mine))


HBM = pl.BlockSpec(memory_space=pl.ANY)
VMEM = pl.BlockSpec(memory_space=pltpu.VMEM)


def gather_kernel(sizes, names, *refs):
    count = len(names)
    gain_ref, gain_out, send, recv = refs[count], refs[2 * count + 1], *refs[-2:]
    stages = gather_stages(sizes, names, refs[:count], refs[count + 1 : 2 * count + 1],
                           refs[2 * count + 2 : -2])
    z, y, x, core = where_am_i()
    mine, near = 2 * x + core, 2 * x + 1 - core
    far, corner = 2 * (1 - x) + core, 2 * (1 - x) + 1 - core

    def pass_gain(src, slot, kind, device):
        return remote(src, gain_out.at[slot], send.at[kind], recv.at[kind], device)

    partner, beside = device_at(z, y, x, 1 - core), device_at(z, y, 1 - x, core)
    hops = (
        (gain_ref, mine, 0, partner),
        (gain_ref, mine, 1, beside),
        (gain_out.at[near], near, 2, beside),
    )
    stages = [stage for _, stage in stages]
    stages[0]()
    gain_out[mine] = gain_ref[...]
    pass_gain(*hops[0]).start()
    pass_gain(*hops[1]).start()
    stages[1]()
    pass_gain(gain_ref, near, 0, partner).wait_recv()
    pass_gain(*hops[2]).start()
    for stage in stages[2:]:
        stage()
    pass_gain(gain_ref, far, 1, beside).wait_recv()
    pass_gain(gain_ref, corner, 2, beside).wait_recv()
    for hop in hops:
        pass_gain(*hop).wait_send()


def gather_blocks(sizes, names, shards, gain):
    wave = pltpu.SemaphoreType.DMA
    return pl.pallas_call(
        functools.partial(gather_kernel, sizes, names),
        out_shape=[jax.ShapeDtypeStruct(sizes.full(name), bf16) for name in names]
        + [jax.ShapeDtypeStruct((sizes.within,) + gain.shape, f32)],
        in_specs=[VMEM] * (len(names) + 1),
        out_specs=[HBM] * len(names) + [VMEM],
        scratch_shapes=gather_scratch(sizes, names) + [wave((3,)), wave((3,))],
        compiler_params=pltpu.CompilerParams(collective_id=0, has_side_effects=True),
        name="gather_blocks",
    )(*shards, gain)


def gain_stages(depth, gain_ref, gain_out, buf, send, recv):
    z, y, x, core = where_am_i()
    hops = (device_at(z, y, x, 1 - core), device_at(z, y, 1 - x, core),
            device_at(z, 1 - y, x, core))

    def hop(step):
        return remote(buf.at[2 * step], buf.at[2 * step + 1], send.at[step], recv.at[step],
                      hops[step])

    def line(way):
        device = device_at(z + 1, y, x, core) if way == 0 else device_at(z - 1, y, x, core)
        return remote(buf.at[7 + way], buf.at[9 + way], send.at[3 + way], recv.at[3 + way],
                      device)

    def begin():
        buf[0] = gain_ref[...]
        hop(0).start()

    def turn(step):
        hop(step).wait_recv()
        buf[2 * step + 2] = buf[2 * step] + buf[2 * step + 1]
        if step < 2:
            hop(step + 1).start()

    def rightward():
        gain_out[...] = buf[6]

        @pl.when(z > 0)
        def _():
            line(0).wait_recv()
            gain_out[...] = gain_out[...] + buf[9]

        @pl.when(z < depth - 1)
        def _():
            buf[7] = gain_out[...]
            line(0).start()

    def leftward():
        buf[8] = buf[6]

        @pl.when(z < depth - 1)
        def _():
            line(1).wait_recv()
            gain_out[...] = gain_out[...] + buf[10]
            buf[8] = buf[6] + buf[10]

        pl.when(z > 0)(lambda: line(1).start())

    def end():
        for step in range(3):
            hop(step).wait_send()
        pl.when(z < depth - 1)(lambda: line(0).wait_send())
        pl.when(z > 0)(lambda: line(1).wait_send())

    return [begin] + [functools.partial(turn, step) for step in range(3)] + [
        rightward, leftward, end]


def scatter_kernel(sizes, names, k_ref, v_ref, wk_ref, wv_ref, *refs):
    count = len(names)
    fulls, gain_ref, grad_ref = refs[:count], refs[count], refs[count + 1]
    owns, gain_out = refs[count + 2 : 2 * count + 2], refs[2 * count + 2]
    gain_scratch, scratch = refs[2 * count + 3 : 2 * count + 6], refs[2 * count + 6 :]
    stages = scatter_stages(sizes, names, fulls, owns, scratch)
    gains = gain_stages(sizes.depth, gain_ref, gain_out, *gain_scratch)
    joined = [(0, stages[0][1])]
    for number, (_, stage) in enumerate(stages[1:]):
        both = functools.partial(in_turn, [stage] + gains[number : number + 1])
        joined.append((12 * (number + 1) / len(stages), both))
    steps = pl.num_programs(0)
    for number in range(steps):
        run_stages(joined, pl.program_id(0), number, steps)
    patch = dot_nn(k_ref[...], wk_ref[0]) + dot_nn(v_ref[...], wv_ref[0])
    grad_ref[...] = patch.astype(bf16)


def scatter_blocks(sizes, names, fulls, gains, grad_key, grad_value, projections):
    wave = pltpu.SemaphoreType.DMA
    slab = 256
    rows = pl.BlockSpec((slab, D), lambda step: (step, 0))

    def matrix(which):
        return pl.BlockSpec((1, D, D), lambda step: (which, 0, 0))

    return pl.pallas_call(
        functools.partial(scatter_kernel, sizes, names),
        grid=(grad_key.shape[0] // slab,),
        out_shape=[jax.ShapeDtypeStruct(grad_key.shape, bf16)]
        + [jax.ShapeDtypeStruct(sizes.shard(name), f32) for name in names]
        + [jax.ShapeDtypeStruct(gains.shape, f32)],
        in_specs=[rows, rows, matrix(1), matrix(2)] + [HBM] * len(names) + [VMEM],
        out_specs=[rows] + [VMEM] * (len(names) + 1),
        scratch_shapes=[pltpu.VMEM((11,) + gains.shape, f32), wave((5,)), wave((5,))]
        + scatter_scratch(sizes, names),
        compiler_params=pltpu.CompilerParams(
            collective_id=1, has_side_effects=True, vmem_limit_bytes=60 * 1024 * 1024
        ),
        name="scatter_blocks",
    )(grad_key, grad_value, projections, projections, *fulls, gains)


def tile_aligned(down, width, side, deep):
    return (
        lax.axis_size("fsdp") == 4
        and lax.axis_size("dp") in (2, 4, 8)
        and down % 96 == 0
        and width % 48 == 0
        and (2 * width) % 128 == 0
        and side % 128 == 0
        and deep % 128 == 0
    )


def adam_update(weight, mean_old, square_old, gradient, step_rate, decay_rate):
    mean_new = beta_one * mean_old + (1.0 - beta_one) * gradient
    square_new = beta_two * square_old + (1.0 - beta_two) * gradient * gradient
    corrected = (
        mean_new
        / (1.0 - beta_one**STEP)
        / (jnp.sqrt(square_new / (1.0 - beta_two**STEP)) + adam_epsilon)
    )
    master = weight - step_rate * (corrected + decay_rate * weight)
    return (mean_new, square_new, master, master.astype(bf16))


def adam_kernel(low_ref, high_ref, gi_ref, go_ref, *refs):
    attention, inner, outer = refs[0:3], refs[3:6], refs[6:9]
    new_attention, new_inner, new_outer = refs[9:13], refs[13:17], refs[17:21]
    step = pl.program_id(0)

    def update(old, new, gradient, *at):
        values = adam_update(*(ref[at] for ref in old), gradient, rate_matrix, decay_matrix)
        for ref, value in zip(new, values):
            ref[at] = value

    pl.when(step < 4)(lambda: update(attention, new_attention, low_ref[0].T, 0))
    pl.when(step >= 4)(lambda: update(attention, new_attention, high_ref[0].T, 0))

    @pl.when(step == 0)
    def _():
        for k in range(gi_ref.shape[0]):
            update(inner, new_inner, gi_ref[k], k)
        update(outer, new_outer, go_ref[...].T, Ellipsis)


def adam_matrices(own_low, own_high, own_inner, own_outer, attention, inner, outer):
    def whole(array):
        return pl.BlockSpec(array.shape, lambda step: (0,) * array.ndim)

    def matrix(array, pick):
        return pl.BlockSpec((1,) + array.shape[1:], lambda step: (pick(step), 0, 0))

    def results(group):
        return [jax.ShapeDtypeStruct(group[0].shape, kind) for kind in (f32, f32, f32, bf16)]

    one = matrix(attention[0], lambda step: step)
    return pl.pallas_call(
        adam_kernel,
        grid=(attention[0].shape[0],),
        in_specs=[
            matrix(own_low, lambda step: jnp.minimum(step, 3)),
            matrix(own_high, lambda step: jnp.maximum(step - 4, 0)),
            whole(own_inner), whole(own_outer),
        ]
        + [one] * 3 + [whole(inner[0])] * 3 + [whole(outer[0])] * 3,
        out_specs=[one] * 4 + [whole(inner[0])] * 4 + [whole(outer[0])] * 4,
        out_shape=results(attention) + results(inner) + results(outer),
        name="adam_matrices",
    )(own_low, own_high, own_inner, own_outer, *attention, *inner, *outer)


def on_device(
    hidden_in,
    patches,
    token_segments,
    patch_segments,
    cotangent,
    attention_weights,
    attention_means,
    attention_squares,
    inner_weights,
    inner_means,
    inner_squares,
    outer_weights,
    outer_means,
    outer_squares,
    norm_gains,
    gain_means,
    gain_squares,
):
    rows, _, length, _ = hidden_in.shape
    count = patches.shape[2]
    tokens = rows * length
    width, down = attention_weights.shape[1:]
    side, deep = inner_weights.shape[2], outer_weights.shape[0]
    direct = tile_aligned(down, width, side, deep)
    low_inner, low_outer = inner_weights.astype(bf16), outer_weights.astype(bf16)
    if direct:
        sizes = Sizes(down, width, side, deep)
        turned = jnp.swapaxes(attention_weights, 1, 2).astype(bf16)
        parts = norm_gains.shape[1]
        gain_block = jnp.pad(
            norm_gains.astype(bf16).astype(f32), ((0, 8 - norm_gains.shape[0]), (0, -parts % 128))
        )
        low, high, gains = gather_blocks(
            sizes, ("low", "high"), (turned[:4], turned[4:]), gain_block
        )
        gains = jnp.swapaxes(gains[:, : norm_gains.shape[0], :parts], 0, 1).reshape(-1, D)
        rest, rest_shards = ("inner", "outer"), (low_inner, low_outer.T)
    else:
        sizes = None
        gains = lax.all_gather(norm_gains.astype(bf16), "fsdp", axis=1, tiled=True)
        weights, inner, outer = gather_weights(
            attention_weights.astype(bf16), low_inner, low_outer
        )
        low, high = weights[:4], weights[4:]
        inner = jnp.concatenate([inner[0], inner[1]], axis=1)
        rest, rest_shards = (), ()

    initial = hidden_in.reshape(tokens, D).astype(f32)
    token_rows = token_segments.reshape(rows, 1, length)
    token_columns = token_segments.reshape(rows, length, 1)
    patch_columns = patch_segments.reshape(rows, count, 1)

    normed_one, unit_one, rms_one = norm_forward(initial, gains[0])
    packed = dot_nt(normed_one, low[0:3].reshape(3 * D, D)).astype(bf16)
    packed = packed.reshape(rows, length, 3 * D)
    mixture_one, lse_one = self_forward(packed, token_rows, token_columns)
    mixed_one = mixture_one.reshape(tokens, D)
    after_one = initial + dot_nt(mixed_one, low[3])
    normed_two, unit_two, rms_two = norm_forward(after_one, gains[1])
    cross_query = dot_nt(normed_two, high[0]).astype(bf16).reshape(rows, length, D)
    mixture_two, lse_two, cross_key, cross_value, *arrived = cross_forward(
        Rider(sizes, rest, "gather", 2, rows * PAIRS), cross_query, patches.reshape(rows, count, D), high,
        token_columns, patch_columns, rest_shards,
    )
    if direct:
        inner, outer = arrived
    mixed_two = mixture_two.reshape(tokens, D)
    after_two = after_one + dot_nt(mixed_two, high[3])
    normed_three, unit_three, rms_three = norm_forward(after_two, gains[2])
    gated = dot_nn(normed_three, inner)
    hidden_units = outer.shape[1]
    gate, up = gated[:, :hidden_units], gated[:, hidden_units:]
    units = (gelu_tanh(gate) * up).astype(bf16)
    hidden_out = (after_two + dot_nt(units, outer)).astype(bf16)

    grad_low = cotangent.reshape(tokens, D)
    grad_final = grad_low.astype(f32)
    grad_outer = dot_tn(grad_low, units).astype(bf16)
    grad_units = dot_nn(grad_low, outer)
    activation, gelu_back = jax.vjp(gelu_tanh, gate)
    grad_gated = jnp.concatenate(
        [gelu_back(grad_units * up)[0], grad_units * activation], axis=1
    ).astype(bf16)
    grad_inner = dot_tn(normed_three, grad_gated).astype(bf16)
    grad_normed = dot_nt(grad_gated, inner)
    grad_from_three, gain_three = norm_backward(grad_normed, gains[2], unit_three, rms_three)
    grad_two = grad_final + grad_from_three
    branch_two = grad_two.astype(bf16)
    grad_mixture_two = dot_nn(branch_two, high[3]).astype(bf16).reshape(rows, length, D)
    grad_cq, grad_ck, grad_cv, grad_pair, *summed_rest = cross_backward(
        Rider(sizes, rest, "scatter", 3, rows * PAIRS), cross_query, cross_key, cross_value,
        mixture_two, grad_mixture_two, lse_two, token_columns, patch_columns,
        patches.reshape(rows, count, D), (grad_inner, grad_outer) if direct else (),
    )
    grad_cq = grad_cq.reshape(tokens, D)
    grad_ck = grad_ck.reshape(rows * count, D)
    grad_cv = grad_cv.reshape(rows * count, D)
    grad_high = jnp.concatenate(
        [
            dot_tn(grad_cq, normed_two).astype(bf16)[None],
            grad_pair,
            dot_tn(branch_two, mixed_two).astype(bf16)[None],
        ]
    )
    grad_from_two, gain_two = norm_backward(
        dot_nn(grad_cq, high[0]), gains[1], unit_two, rms_two
    )
    grad_one = grad_two + grad_from_two
    branch_one = grad_one.astype(bf16)
    grad_mixture_one = dot_nn(branch_one, low[3]).astype(bf16).reshape(rows, length, D)
    grad_q, grad_k, grad_v = self_backward(
        packed, mixture_one, grad_mixture_one, lse_one, token_rows, token_columns
    )
    grad_q = grad_q.reshape(tokens, D)
    grad_k = grad_k.reshape(tokens, D)
    grad_v = grad_v.reshape(tokens, D)
    grad_normed_one = dot_nn(grad_q, low[0]) + dot_nn(grad_k, low[1]) + dot_nn(grad_v, low[2])
    grad_from_one, gain_one = norm_backward(grad_normed_one, gains[0], unit_one, rms_one)
    hidden_grad = grad_one + grad_from_one
    grad_first = jnp.stack(
        [
            dot_tn(grad_q, normed_one).astype(bf16),
            dot_tn(grad_k, normed_one).astype(bf16),
            dot_tn(grad_v, normed_one).astype(bf16),
            dot_tn(branch_one, mixed_one).astype(bf16),
        ]
    )
    gain_grads = jnp.stack([gain_one, gain_two, gain_three])
    if direct:
        own_inner, own_outer = summed_rest
        patch_grad, own_low, own_high, gain_totals = scatter_blocks(
            sizes, ("low", "high"), (grad_first, grad_high),
            jnp.pad(gain_grads, ((0, 5), (0, 0))), grad_ck, grad_cv, high,
        )
        gain_totals = gain_totals[:3]
    else:
        patch_grad = dot_nn(grad_ck, high[1]) + dot_nn(grad_cv, high[2])
        own_attention, own_inner, own_outer = scatter_grads(
            jnp.concatenate([grad_first, grad_high]),
            jnp.stack([grad_inner[:, :hidden_units], grad_inner[:, hidden_units:]]),
            grad_outer,
        )
        gain_totals = lax.psum(gain_grads, BOTH)
    width = norm_gains.shape[1]
    own_gains = lax.dynamic_slice_in_dim(
        gain_totals, lax.axis_index("fsdp") * width, width, axis=1
    )

    if direct:
        fresh = adam_matrices(
            own_low, own_high, own_inner, own_outer,
            (attention_weights, attention_means, attention_squares),
            (inner_weights, inner_means, inner_squares),
            (outer_weights, outer_means, outer_squares),
        )
        attention_new, inner_new, outer_new = fresh[0:4], fresh[4:8], fresh[8:12]
    else:
        attention_new = adam_update(
            attention_weights, attention_means, attention_squares, own_attention,
            rate_matrix, decay_matrix,
        )
        inner_new = adam_update(
            inner_weights, inner_means, inner_squares, own_inner, rate_matrix, decay_matrix
        )
        outer_new = adam_update(
            outer_weights, outer_means, outer_squares, own_outer, rate_matrix, decay_matrix
        )
    gain_new = adam_update(norm_gains, gain_means, gain_squares, own_gains, rate_gain, 0.0)
    return (
        hidden_out.reshape(hidden_in.shape),
        hidden_grad.reshape(hidden_in.shape),
        patch_grad.reshape(patches.shape).astype(f32),
        *attention_new,
        *inner_new,
        *outer_new,
        *gain_new,
    )


def solution(mesh):
    rows = P(None, BOTH, None, None)
    ids = P(None, BOTH, None)
    matrix = P(None, "fsdp", "dp")
    down = P("fsdp", "dp")
    gain = P(None, "fsdp")
    return jax.shard_map(
        on_device,
        mesh=mesh,
        in_specs=(rows, rows, ids, ids, rows) + (matrix,) * 6 + (down,) * 3 + (gain,) * 3,
        out_specs=(rows, rows, rows) + (matrix,) * 8 + (down,) * 4 + (gain,) * 4,
        check_vma=False,
    )
```

```python
import functools

import jax
import jax.numpy as jnp
from jax import lax
from jax.experimental import pallas as pl
from jax.experimental.pallas import tpu as pltpu
from jax.sharding import PartitionSpec as P

D = 768
HEADS = 12
HEAD = 64
PAIR = 2 * HEAD
PAIRS = HEADS // 2
GROUP = 3
STEP = 10
SEGS = 4

epsilon = 1e-06
score_scale = 0.125
masked_value = -1000000000.0
beta_one = 0.9
beta_two = 0.95
adam_epsilon = 1e-08
decay_matrix = 0.1
rate_matrix = 0.1
rate_gain = 0.3
f32 = jnp.float32
bf16 = jnp.bfloat16
BOTH = ("dp", "fsdp")


def gelu_tanh(values):
    return (
        0.5
        * values
        * (1.0 + jnp.tanh(0.7978845608028654 * (values + 0.044715 * values * values * values)))
    )


def dot_nn(a, b):
    return lax.dot_general(a, b, (((1,), (0,)), ((), ())), preferred_element_type=f32)


def dot_nt(a, b):
    return lax.dot_general(a, b, (((1,), (1,)), ((), ())), preferred_element_type=f32)


def dot_tn(a, b):
    return lax.dot_general(a, b, (((0,), (0,)), ((), ())), preferred_element_type=f32)


def norm_forward(values, gain):
    inverse_rms = lax.rsqrt(jnp.mean(values * values, axis=-1, keepdims=True) + epsilon)
    unit_rows = values * inverse_rms
    return ((unit_rows * gain.astype(f32)).astype(bf16), unit_rows, inverse_rms)


def norm_backward(grad_rows, gain, unit_rows, inverse_rms):
    grad_unit = grad_rows * gain.astype(f32)
    grad_values = inverse_rms * (
        grad_unit - unit_rows * jnp.mean(grad_unit * unit_rows, axis=-1, keepdims=True)
    )
    return (grad_values, jnp.sum(grad_rows * unit_rows, axis=0))


def head_half(block, half):
    lane = lax.broadcasted_iota(jnp.int32, block.shape, 1)
    keep = (lane < HEAD) if half == 0 else (lane >= HEAD)
    return jnp.where(keep, block, jnp.zeros_like(block))


def three_parts(column):
    high = column.astype(bf16).astype(f32)
    rest = column - high
    middle = rest.astype(bf16).astype(f32)
    low = rest - middle
    return high, middle, low


def stat_lanes(base, column, first):
    lane = lax.broadcasted_iota(jnp.int32, base.shape, 1)
    for place, part in enumerate(three_parts(column)):
        base = jnp.where(lane == first + place, -part, base)
    return base


def turned_marks(key_ids):
    spot = lax.broadcasted_iota(jnp.int32, (128, key_ids.shape[1]), 0)
    return jnp.where(spot == key_ids, 1.0, 0.0).astype(bf16).T


def key_marks(key_ids, stats):
    lane = lax.broadcasted_iota(jnp.int32, (key_ids.shape[0], 128), 1)
    marks = lane == key_ids
    if stats:
        marks = marks | ((lane >= SEGS) & (lane < SEGS + 3))
    return jnp.where(marks, 1.0, 0.0).astype(bf16)


def query_bias(query_ids):
    lane = lax.broadcasted_iota(jnp.int32, (query_ids.shape[0], 128), 1)
    return jnp.where((lane == query_ids) | (lane >= SEGS), 0.0, masked_value)


def softmax_columns(scores):
    top = jnp.max(scores, axis=0, keepdims=True)
    raised = jnp.exp(scores - top)
    return raised, top, jnp.sum(raised, axis=0, keepdims=True)


def finish_forward(halves, tops, sums):
    mixed = jnp.concatenate([h / s for h, s in zip(halves, sums)], axis=0)
    rows = [t + jnp.log(s) for t, s in zip(tops, sums)]
    pad = jnp.zeros((6, rows[0].shape[1]), f32)
    return mixed.T.astype(bf16), jnp.concatenate(rows + [pad], axis=0)


def cross_forward_kernel(rider, q_ref, c_ref, wk_ref, wv_ref, qid_ref, kid_ref, *refs):
    (o_ref, lse_ref, k_ref, v_ref) = rider.board(refs, 4)
    both = jnp.concatenate([wk_ref[0], wv_ref[0]], axis=0)
    projected = dot_nt(c_ref[0], both).astype(bf16)
    key, value = projected[:, :PAIR], projected[:, PAIR:]
    k_ref[0], v_ref[0] = key, value
    marked = jnp.concatenate([key, turned_marks(kid_ref[0])], axis=1)
    bias = query_bias(qid_ref[0]).astype(bf16)
    query = q_ref[0] * jnp.asarray(score_scale, bf16)
    values = value.T
    halves, tops, sums = [], [], []
    scored = [
        dot_nt(marked, jnp.concatenate([head_half(query, half), bias], axis=1))
        for half in range(2)
    ]
    for half in range(2):
        raised, top, total = softmax_columns(scored[half])
        halves.append(dot_nn(values[half * HEAD : (half + 1) * HEAD], raised.astype(bf16)))
        tops.append(top)
        sums.append(total)
    o_ref[0], lse_ref[0, 0] = finish_forward(halves, tops, sums)
    rider.leave()


def causal_mask(qid_ref, kid_ref):
    length = kid_ref.shape[1]
    key = lax.broadcasted_iota(jnp.int32, (length, length), 0)
    query = lax.broadcasted_iota(jnp.int32, (length, length), 1)
    return (key <= query) & (kid_ref[0] == qid_ref[0])


def pair_lanes(pair):
    return slice(pair * PAIR, (pair + 1) * PAIR)


def self_forward_kernel(q_ref, k_ref, v_ref, qid_ref, kid_ref, o_ref, lse_ref):
    allowed = causal_mask(qid_ref, kid_ref)
    for pair in range(GROUP):
        lanes = pair_lanes(pair)
        query = q_ref[0, :, lanes] * jnp.asarray(score_scale, bf16)
        key = k_ref[0, :, lanes]
        values = v_ref[0, :, lanes].T
        halves, tops, sums = [], [], []
        for half in range(2):
            scores = jnp.where(allowed, dot_nt(key, head_half(query, half)), masked_value)
            raised, top, total = softmax_columns(scores)
            halves.append(dot_nn(values[half * HEAD : (half + 1) * HEAD], raised.astype(bf16)))
            tops.append(top)
            sums.append(total)
        o_ref[0, :, lanes], lse_ref[0, pair] = finish_forward(halves, tops, sums)


def backward_pair(query, key, value, mixed, grad, lse, marked, bias, allowed):
    scaled = query * jnp.asarray(score_scale, bf16)
    key_turned = key.T
    length = query.shape[0]
    lse_columns = lse.T
    product = mixed.astype(f32) * grad.astype(f32)
    ones = key_marks(jnp.full((value.shape[0], 1), -1, jnp.int32), True)
    valued = jnp.concatenate([value, ones], axis=1)
    scored, shifted = [], []
    for half in range(2):
        stats = stat_lanes(bias, lse_columns[:, half : half + 1], SEGS).astype(bf16)
        scored.append(
            dot_nt(marked, jnp.concatenate([head_half(scaled, half), stats], axis=1)))
        inner = jnp.sum(head_half(product, half), axis=1, keepdims=True)
        delta = stat_lanes(jnp.zeros((length, 128), f32), inner, SEGS).astype(bf16)
        shifted.append(dot_nt(valued, jnp.concatenate([head_half(grad, half), delta], axis=1)))
    probs, grads, turned = [], [], []
    for half in range(2):
        scores = scored[half]
        if allowed is not None:
            scores = jnp.where(allowed, scores, masked_value)
        weight = jnp.exp(scores)
        grad_scores = (weight * shifted[half]).astype(bf16)
        probs.append(weight.astype(bf16))
        grads.append(grad_scores)
        turned.append(dot_nn(key_turned[half * HEAD : (half + 1) * HEAD], grad_scores))
    grad_query = (score_scale * jnp.concatenate(turned, axis=0)).T.astype(bf16)
    grad_turned, scaled_turned = grad.T, scaled.T
    halves = [slice(0, HEAD), slice(HEAD, PAIR)]
    value_turned = jnp.concatenate(
        [dot_nt(grad_turned[h], p) for h, p in zip(halves, probs)], axis=0).astype(bf16)
    keyed_turned = jnp.concatenate(
        [dot_nt(scaled_turned[h], p) for h, p in zip(halves, grads)], axis=0).astype(bf16)
    grad_value, grad_key = value_turned.T, keyed_turned.T
    return grad_query, grad_key, grad_value, keyed_turned, value_turned


def cross_backward_kernel(rider, q_ref, k_ref, v_ref, o_ref, do_ref, lse_ref, qid_ref, kid_ref,
                          c_ref, *refs):
    total_ref = refs[-1]
    dq_ref, dk_ref, dv_ref, sum_ref = rider.board(refs[:-1], 4)
    ones = key_marks(jnp.full((k_ref.shape[1], 1), -1, jnp.int32), True)
    marked = jnp.concatenate([k_ref[0], turned_marks(kid_ref[0]) + ones], axis=1)
    dq_ref[0], grad_key, grad_value, key_t, value_t = backward_pair(
        q_ref[0], k_ref[0], v_ref[0], o_ref[0], do_ref[0], lse_ref[0, 0], marked,
        query_bias(qid_ref[0]), None)
    dk_ref[0], dv_ref[0] = grad_key, grad_value
    row, pair = pl.program_id(0), pl.program_id(1)
    part = dot_nn(jnp.concatenate([key_t, value_t], axis=0), c_ref[0])

    @pl.when(row == 0)
    def _():
        total_ref[pair] = part

    @pl.when(row > 0)
    def _():
        total_ref[pair] = total_ref[pair] + part

    @pl.when(row == pl.num_programs(0) - 1)
    def _():
        at = pl.ds(pl.multiple_of(pair * PAIR, PAIR), PAIR)
        sum_ref[1, at] = total_ref[pair, :PAIR].astype(bf16)
        sum_ref[2, at] = total_ref[pair, PAIR:].astype(bf16)
        sum_ref[0, at] = jnp.zeros((PAIR, D), bf16)
        sum_ref[3, at] = jnp.zeros((PAIR, D), bf16)

    rider.leave()


def self_backward_kernel(q_ref, k_ref, v_ref, o_ref, do_ref, lse_ref, qid_ref, kid_ref,
                         grad_ref):
    length = k_ref.shape[1]
    ones = key_marks(jnp.full((length, 1), -1, jnp.int32), True)
    allowed = causal_mask(qid_ref, kid_ref)
    for pair in range(GROUP):
        lanes = pair_lanes(pair)
        key = k_ref[0, :, lanes]
        parts = backward_pair(
            q_ref[0, :, lanes], key, v_ref[0, :, lanes], o_ref[0, :, lanes],
            do_ref[0, :, lanes], lse_ref[0, pair], jnp.concatenate([key, ones], axis=1),
            jnp.zeros((length, 128), f32), allowed)[:3]
        for part, value in enumerate(parts):
            first = part * D + (pl.program_id(1) * GROUP + pair) * PAIR
            grad_ref[0, :, pl.ds(pl.multiple_of(first, PAIR), PAIR)] = value

    @pl.when(pl.program_id(1) == 0)
    def _():
        grad_ref[0, :, 3 * D :] = jnp.zeros((length, D), bf16)


def pair_spec(length, offset, pairs=1):
    return pl.BlockSpec((1, length, pairs * PAIR), lambda row, step: (row, 0, offset + step))


def row_spec(shape):
    return pl.BlockSpec((1,) + shape, lambda row, step: (row, 0, 0))


def stat_spec(length, pairs=1):
    return pl.BlockSpec((1, pairs, 8, length), lambda row, step: (row, step, 0, 0))


def cost(rows, queries, keys, products):
    elements = rows * HEADS * queries * keys
    return pl.CostEstimate(
        flops=2 * elements * 256 * products // 2,
        transcendentals=elements,
        bytes_accessed=rows * (queries + keys) * D * 2 * 3,
    )


class Rider:
    def __init__(self, sizes, names, kind, number, steps):
        self.sizes, self.names, self.kind, self.number = sizes, names, kind, number
        self.steps = steps

    def board(self, refs, outputs):
        count = len(self.names)
        theirs, mine, scratch = refs[:count], refs[count : count + outputs], refs[count + outputs :]
        if count:
            ends, scratch = scratch[:count], scratch[count:]
            build = gather_stages if self.kind == "gather" else scatter_stages
            stages = build(self.sizes, self.names, theirs, ends, scratch)
            step = pl.program_id(0) * pl.num_programs(1) + pl.program_id(1)
            for number in range(self.steps):
                run_stages(stages, step, number, self.steps)
            self.rest = ([s for time, s in stages if time >= 12], step == self.steps - 1)
        return mine

    def leave(self):
        if self.names and self.rest[0]:
            pl.when(self.rest[1])(functools.partial(in_turn, self.rest[0]))

    def in_specs(self):
        return [VMEM if self.kind == "gather" else HBM] * len(self.names)

    def out_specs(self):
        return [HBM if self.kind == "gather" else VMEM] * len(self.names)

    def out_shape(self):
        if self.kind == "gather":
            return [jax.ShapeDtypeStruct(self.sizes.full(n), bf16) for n in self.names]
        return [jax.ShapeDtypeStruct(self.sizes.owned(n), f32) for n in self.names]

    def scratch(self):
        if not self.names:
            return []
        build = gather_scratch if self.kind == "gather" else scatter_scratch
        return build(self.sizes, self.names)

    def params(self):
        if not self.names:
            return pltpu.CompilerParams()
        return pltpu.CompilerParams(
            collective_id=self.number, has_side_effects=True, vmem_limit_bytes=60 * 1024 * 1024
        )


def self_forward(packed, query_ids, key_ids):
    rows, length = packed.shape[:2]
    steps = PAIRS // GROUP
    return pl.pallas_call(
        self_forward_kernel,
        grid=(rows, steps),
        in_specs=[pair_spec(length, part * steps, GROUP) for part in range(3)]
        + [row_spec((1, length)), row_spec((length, 1))],
        out_specs=[pair_spec(length, 0, GROUP), stat_spec(length, GROUP)],
        out_shape=[
            jax.ShapeDtypeStruct((rows, length, D), bf16),
            jax.ShapeDtypeStruct((rows, PAIRS, 8, length), f32),
        ],
        cost_estimate=cost(rows, length, length, 2),
        name="self_forward",
    )(packed, packed, packed, query_ids, key_ids)


def self_backward(packed, mixed, grad, lse, query_ids, key_ids):
    rows, length = packed.shape[:2]
    steps = PAIRS // GROUP
    plain = pair_spec(length, 0, GROUP)
    return pl.pallas_call(
        self_backward_kernel,
        grid=(rows, steps),
        in_specs=[pair_spec(length, part * steps, GROUP) for part in range(3)]
        + [plain, plain, stat_spec(length, GROUP), row_spec((1, length)), row_spec((length, 1))],
        out_specs=row_spec((length, 4 * D)),
        out_shape=jax.ShapeDtypeStruct((rows, length, 4 * D), bf16),
        cost_estimate=cost(rows, length, length, 5),
        name="self_backward",
    )(packed, packed, packed, mixed, grad, lse, query_ids, key_ids)


def cross_forward(rider, queries, patches, projections, query_ids, key_ids, shards):
    rows, length = queries.shape[:2]
    count = patches.shape[1]

    def slab(which):
        return pl.BlockSpec((1, PAIR, D), lambda row, pair: (which, pair, 0))

    return pl.pallas_call(
        functools.partial(cross_forward_kernel, rider),
        grid=(rows, PAIRS),
        in_specs=[
            pair_spec(length, 0),
            row_spec((count, D)),
            slab(1),
            slab(2),
            row_spec((length, 1)),
            row_spec((1, count)),
        ]
        + rider.in_specs(),
        out_specs=[
            pair_spec(length, 0), stat_spec(length), pair_spec(count, 0), pair_spec(count, 0),
        ]
        + rider.out_specs(),
        out_shape=[
            jax.ShapeDtypeStruct((rows, length, D), bf16),
            jax.ShapeDtypeStruct((rows, PAIRS, 8, length), f32),
            jax.ShapeDtypeStruct((rows, count, D), bf16),
            jax.ShapeDtypeStruct((rows, count, D), bf16),
        ]
        + rider.out_shape(),
        scratch_shapes=rider.scratch(),
        compiler_params=rider.params(),
        cost_estimate=cost(rows, length, count, 4),
        name="cross_forward",
    )(queries, patches, projections, projections, query_ids, key_ids, *shards)


def cross_backward(rider, queries, keys, values, mixed, grad, lse, query_ids, key_ids, patches,
                   fulls):
    rows, length = grad.shape[:2]
    count = keys.shape[1]
    short, tall = pair_spec(length, 0), pair_spec(count, 0)
    return pl.pallas_call(
        functools.partial(cross_backward_kernel, rider),
        grid=(rows, PAIRS),
        in_specs=[
            short, tall, tall, short, short, stat_spec(length), row_spec((length, 1)),
            row_spec((1, count)), row_spec((count, D)),
        ]
        + rider.in_specs(),
        out_specs=[short, tall, tall, VMEM] + rider.out_specs(),
        out_shape=[
            jax.ShapeDtypeStruct((rows, length, D), bf16),
            jax.ShapeDtypeStruct((rows, count, D), bf16),
            jax.ShapeDtypeStruct((rows, count, D), bf16),
            jax.ShapeDtypeStruct((4, D, D), bf16),
        ]
        + rider.out_shape(),
        scratch_shapes=rider.scratch() + [pltpu.VMEM((PAIRS, 2 * PAIR, D), f32)],
        compiler_params=rider.params(),
        cost_estimate=cost(rows, length, count, 7),
        name="cross_backward",
    )(queries, keys, values, mixed, grad, lse, query_ids, key_ids, patches, *fulls)


def gather_weights(attention, inner, outer):
    turned = lax.all_gather(jnp.swapaxes(attention, 1, 2), BOTH, axis=0, tiled=False)
    heads = lax.axis_size("dp"), lax.axis_size("fsdp")
    turned = turned.reshape(heads + turned.shape[1:])
    full_attention = jnp.transpose(turned, (2, 0, 3, 1, 4)).reshape(8, D, D)
    wide = lax.all_gather(inner, BOTH, axis=0, tiled=False)
    wide = wide.reshape(heads + wide.shape[1:])
    full_inner = jnp.transpose(wide, (2, 1, 3, 0, 4)).reshape(2, D, -1)
    tall = lax.all_gather(outer.T, BOTH, axis=0, tiled=False)
    tall = tall.reshape(heads + tall.shape[1:])
    full_outer = jnp.transpose(tall, (0, 2, 1, 3)).reshape(D, -1)
    return full_attention, full_inner, full_outer


def scatter_grads(attention, inner, outer):
    across, within = lax.axis_size("dp"), lax.axis_size("fsdp")
    blocks = attention.reshape(8, across, D // across, within, D // within)
    blocks = jnp.transpose(blocks, (1, 3, 0, 2, 4))
    blocks = blocks.reshape((across * within,) + blocks.shape[2:])
    own_attention = lax.psum_scatter(blocks, BOTH, scatter_dimension=0, tiled=False)
    blocks = inner.reshape(2, within, D // within, across, inner.shape[2] // across)
    blocks = jnp.transpose(blocks, (3, 1, 0, 2, 4))
    blocks = blocks.reshape((across * within,) + blocks.shape[2:])
    own_inner = lax.psum_scatter(blocks, BOTH, scatter_dimension=0, tiled=False)
    blocks = outer.reshape(across, D // across, within, outer.shape[1] // within)
    blocks = jnp.transpose(blocks, (0, 2, 1, 3))
    blocks = blocks.reshape((across * within,) + blocks.shape[2:])
    own_outer = lax.psum_scatter(blocks, BOTH, scatter_dimension=0, tiled=False)
    return (
        jnp.swapaxes(own_attention, 1, 2).astype(f32),
        own_inner.astype(f32),
        own_outer.T.astype(f32),
    )


MESH = pl.DeviceIdType.MESH
RIGHT, LEFT, TO_Y, TO_X, TO_CORE = range(5)


def where_am_i():
    across, within = lax.axis_index("dp"), lax.axis_index("fsdp")
    return across // 2, across % 2, within // 2, within % 2


def device_at(z, y, x, core):
    return (2 * z + y, 2 * x + core)


def aligned(value, unit):
    return pl.multiple_of(value * unit, unit)


class Sizes:
    def __init__(self, down, width, side, deep):
        self.down, self.width, self.side, self.deep = down, width, side, deep
        self.across, self.within = D // down, D // width
        self.depth = self.across // 2
        self.chips = self.across * self.within // 2

    def shard(self, name):
        return {
            "low": (4, self.down, self.width),
            "high": (4, self.down, self.width),
            "inner": (2, self.width, self.side),
            "outer": (self.down, self.deep),
        }[name]

    def owned(self, name):
        if name in ("low", "high"):
            return (4, self.width, self.down)
        return self.shard(name)

    def full(self, name):
        return {
            "low": (4, D, D),
            "high": (4, D, D),
            "inner": (D, 2 * self.across * self.side),
            "outer": (D, self.within * self.deep),
        }[name]

    def piece(self, name):
        return {
            "low": (self.down, 2 * self.width),
            "high": (self.down, 2 * self.width),
            "inner": (self.width, self.side),
            "outer": (self.down // 2, self.deep),
        }[name]

    def part(self, name):
        return {
            "low": (2, self.down, self.width),
            "high": (2, self.down, self.width),
            "inner": (self.width, self.side),
            "outer": (self.down // 2, self.deep),
        }[name]

    def place(self, name, ref, cut, z, y, x, half):
        place = 2 * z + y
        if name == "inner":
            return ref.at[
                pl.ds(aligned(2 * x + cut, self.width), self.width),
                pl.ds(aligned(half * self.across + place, self.side), self.side),
            ]
        if name == "outer":
            return ref.at[
                pl.ds(aligned(2 * place + half, self.down // 2), self.down // 2),
                pl.ds(aligned(2 * x + cut, self.deep), self.deep),
            ]
        return ref.at[
            2 * half + cut,
            pl.ds(aligned(place, self.down), self.down),
            pl.ds(aligned(x, 2 * self.width), 2 * self.width),
        ]

    def share(self, name, ref, half):
        if name == "inner":
            return ref.at[half]
        if name == "outer":
            return ref.at[pl.ds(aligned(half, self.down // 2), self.down // 2)]
        return ref.at[pl.ds(2 * half, 2)]


def greet(depth):
    z, y, x, core = where_am_i()
    barrier = pltpu.get_barrier_semaphore()

    def signal(device):
        pl.semaphore_signal(barrier, inc=1, device_id=device, device_id_type=MESH)

    signal(device_at(z, y, x, 1 - core))
    signal(device_at(z, y, 1 - x, core))
    signal(device_at(z, 1 - y, x, core))
    pl.when(z > 0)(lambda: signal(device_at(z - 1, y, x, core)))
    pl.when(z < depth - 1)(lambda: signal(device_at(z + 1, y, x, core)))
    pl.semaphore_wait(barrier, 3 + jnp.where(z > 0, 1, 0) + jnp.where(z < depth - 1, 1, 0))


def chip_index(bz, by, bx):
    return (2 * bz + by) * 2 + bx


def remote(src, dst, send, recv, device):
    return pltpu.make_async_remote_copy(
        src_ref=src, dst_ref=dst, send_sem=send, recv_sem=recv, device_id=device,
        device_id_type=MESH)


def gather_scratch(sizes, names):
    wave = pltpu.SemaphoreType.DMA
    count, pieces = len(names), 2 * len(names)
    return (
        [pltpu.VMEM((2,) + sizes.piece(name), bf16) for name in names]
        + [pltpu.VMEM(sizes.part(name), bf16) for name in names]
        + [wave((count,)), wave((count,)), wave((pieces,)), wave((pieces, 5, sizes.chips)),
           wave((pieces, 2, sizes.chips))]
    )


def gather_stages(sizes, names, shards, fulls, scratch):
    count, depth = len(names), sizes.depth
    pairs, got = scratch[:count], scratch[count : 2 * count]
    swap_send, swap_recv, own_sem, send_sem, recv_sem = scratch[2 * count :]
    z, y, x, core = where_am_i()
    other = 1 - core
    pieces = [(n, cut) for cut in range(2) for n in range(count)]

    def place(piece, bz, by, bx, half):
        n, cut = pieces[piece]
        return sizes.place(names[n], fulls[n], cut, bz, by, bx, half)

    def swap(n):
        return remote(sizes.share(names[n], shards[n], other), got[n], swap_send.at[n],
                      swap_recv.at[n], device_at(z, y, x, other))

    def merge(n, me):
        if names[n] in ("low", "high"):
            width = sizes.width
            for part, source in ((me, shards[n][2 * me : 2 * me + 2]), (1 - me, got[n][...])):
                pairs[n][:, :, part * width : (part + 1) * width] = source
        else:
            half = sizes.down // 2
            mine = shards[n][me] if names[n] == "inner" else shards[n][me * half : (me + 1) * half]
            pairs[n][me] = mine
            pairs[n][1 - me] = got[n][...]

    def copy(piece, bz, by, bx, kind, own=False):
        target = {
            RIGHT: device_at(z + 1, y, x, core),
            LEFT: device_at(z - 1, y, x, core),
            TO_Y: device_at(z, 1 - y, x, core),
            TO_X: device_at(z, y, 1 - x, core),
            TO_CORE: device_at(z, y, x, other),
        }[kind]
        spot = place(piece, bz, by, bx, core)
        n, cut = pieces[piece]
        slot = chip_index(bz, by, bx)
        return remote(pairs[n].at[cut] if own else spot, spot, send_sem.at[piece, kind, slot],
                      recv_sem.at[piece, 1 if kind == TO_CORE else 0, slot], target)

    def arrive(piece, bz, by, bx, from_core=False):
        spot = place(piece, bz, by, bx, other if from_core else core)
        remote(spot, spot, send_sem.at[piece, 0, 0],
               recv_sem.at[piece, 1 if from_core else 0, chip_index(bz, by, bx)],
               device_at(z, y, x, other)).wait_recv()

    def keep(piece):
        n, cut = pieces[piece]
        return pltpu.make_async_copy(pairs[n].at[cut], place(piece, z, y, x, core),
                                     own_sem.at[piece])

    every = range(len(pieces))
    first, later = every[:count], every[count:]

    def launch(kind):
        for piece in every:
            copy(piece, z, y, x, kind, True).start()

    def begin():
        greet(depth)
        for n in range(count):
            swap(n).start()

    def send_own():
        for n in range(count):
            swap(n).wait_recv()
        for me in range(2):
            @pl.when(core == me)
            def _(me=me):
                for n in range(count):
                    merge(n, me)
        pl.when(z < depth - 1)(lambda: launch(RIGHT))
        pl.when(z > 0)(lambda: launch(LEFT))
        for piece in every:
            copy(piece, z, y, x, TO_Y, True).start()
            copy(piece, z, y, x, TO_X, True).start()
        for piece in every:
            copy(piece, z, y, x, TO_CORE, True).start()
            keep(piece).start()

    def from_z(bz, kind, further):
        for piece in every:
            arrive(piece, bz, y, x)
            pl.when(further)(lambda piece=piece: copy(piece, bz, y, x, kind).start())
            copy(piece, bz, y, x, TO_Y).start()
            copy(piece, bz, y, x, TO_X).start()
            copy(piece, bz, y, x, TO_CORE).start()

    def from_sides(bz):
        for early, late in zip(first, later):
            arrive(early, bz, 1 - y, x)
            copy(early, bz, 1 - y, x, TO_X).start()
            copy(early, bz, 1 - y, x, TO_CORE).start()
            arrive(late, bz, y, 1 - x)
            copy(late, bz, y, 1 - x, TO_Y).start()
            copy(late, bz, y, 1 - x, TO_CORE).start()
        for early, late in zip(first, later):
            arrive(early, bz, y, 1 - x)
            copy(early, bz, y, 1 - x, TO_CORE).start()
            arrive(late, bz, 1 - y, x)
            copy(late, bz, 1 - y, x, TO_CORE).start()

    def from_corner(bz):
        for piece in every:
            arrive(piece, bz, 1 - y, 1 - x)
            copy(piece, bz, 1 - y, 1 - x, TO_CORE).start()

    def both_ways(step, action):
        if step == 0:
            action(z)
            return
        pl.when(z - step >= 0)(lambda: action(z - step))
        pl.when(z + step < depth)(lambda: action(z + step))

    def line(step):
        pl.when(z - step >= 0)(lambda: from_z(z - step, RIGHT, z < depth - 1))
        pl.when(z + step < depth)(lambda: from_z(z + step, LEFT, z > 0))

    def end():
        for n in range(count):
            swap(n).wait_send()
        for piece in every:
            keep(piece).wait()

            @pl.loop(0, depth)
            def _(bz, piece=piece):
                for by in range(2):
                    for bx in range(2):
                        arrive(piece, bz, by, bx, True)
                        copy(piece, bz, by, bx, TO_CORE).wait_send()
                copy(piece, bz, y, x, TO_Y).wait_send()
                copy(piece, bz, y, x, TO_X).wait_send()
                if piece in first:
                    copy(piece, bz, 1 - y, x, TO_X).wait_send()
                else:
                    copy(piece, bz, y, 1 - x, TO_Y).wait_send()
                pl.when((bz <= z) & (z < depth - 1))(
                    lambda: copy(piece, bz, y, x, RIGHT).wait_send())
                pl.when((bz >= z) & (z > 0))(lambda: copy(piece, bz, y, x, LEFT).wait_send())

    timed = [(0, begin), (0, send_own), (12, end)]
    for step in range(1, depth):
        timed.append((2 * step, functools.partial(line, step)))
    for step in range(depth):
        timed.append(((3, 6, 8, 9)[step], functools.partial(both_ways, step, from_sides)))
        timed.append(((10, 10, 11, 11)[step], functools.partial(both_ways, step, from_corner)))
    return sorted(timed, key=lambda item: item[0])


def add_rows(target, sources):
    slab = 48

    def total(k):
        at = pl.ds(aligned(k, slab), slab)
        value = sources[0][at].astype(f32)
        for source in sources[1:]:
            value = value + source[at].astype(f32)
        target[at] = value.astype(target.dtype)

    pl.loop(0, target.shape[0] // slab)(total)


def scatter_scratch(sizes, names):
    wave = pltpu.SemaphoreType.DMA
    count, pieces, depth, chips = len(names), 2 * len(names), sizes.depth, sizes.chips

    def buffers(lead, kind):
        return [pltpu.VMEM(lead + (2,) + sizes.piece(name), kind) for name in names]

    return (
        buffers((chips,), bf16) + buffers((chips,), bf16) + buffers((2 * depth,), bf16)
        + buffers((depth,), bf16) + buffers((2, depth), bf16) + buffers((), f32)
        + [pltpu.VMEM(sizes.part(name), f32) for name in names]
        + [pltpu.VMEM(sizes.part(name), f32) for name in names]
        + [wave((pieces, chips))] * 3 + [wave((pieces, 2 * depth))] * 2
        + [wave((pieces, depth))] * 2 + [wave((pieces, 2, depth))] * 2 + [wave((count,))] * 2
    )


def scatter_stages(sizes, names, fulls, owns, scratch):
    count, depth = len(names), sizes.depth
    acc, swapped, first, second, line, sums, outs, ins = (
        scratch[k * count : (k + 1) * count] for k in range(8)
    )
    (load_sem, swap_send, swap_recv, one_send, one_recv, two_send, two_recv, line_send,
     line_recv, end_send, end_recv) = scratch[8 * count :]
    z, y, x, core = where_am_i()
    other = 1 - core
    partner = device_at(z, y, x, other)
    over_x, over_y = device_at(z, y, 1 - x, core), device_at(z, 1 - y, x, core)
    pieces = [(n, cut) for cut in range(2) for n in range(count)]
    every = range(len(pieces))
    order = sorted(range(depth), key=lambda spot: (-abs(2 * spot - depth + 1), -spot))

    def at(buffers, piece, *index):
        n, cut = pieces[piece]
        return buffers[n].at[(*index, cut)]

    def block(piece, bz, by, bx, half):
        n, cut = pieces[piece]
        return sizes.place(names[n], fulls[n], cut, bz, by, bx, half)

    def load(piece, bz, by, bx):
        slot = chip_index(bz, by, bx)
        return pltpu.make_async_copy(block(piece, bz, by, bx, core), at(acc, piece, slot),
                                     load_sem.at[piece, slot])

    def swap(piece, bz, by, bx):
        slot = chip_index(bz, by, bx)
        return remote(block(piece, bz, by, bx, other), at(swapped, piece, slot),
                      swap_send.at[piece, slot], swap_recv.at[piece, slot], partner)

    def turned(piece):
        return pieces[piece][1] == 1

    def stage_one(piece, bz, spot):
        if turned(piece):
            far, device = chip_index(bz, 1 - y, spot), over_y
        else:
            far, device = chip_index(bz, spot, 1 - x), over_x
        slot = 2 * bz + spot
        return remote(at(acc, piece, far), at(first, piece, slot), one_send.at[piece, slot],
                      one_recv.at[piece, slot], device)

    def stage_two(piece, bz):
        if turned(piece):
            far, device = chip_index(bz, y, 1 - x), over_x
        else:
            far, device = chip_index(bz, 1 - y, x), over_y
        return remote(at(acc, piece, far), at(second, piece, bz), two_send.at[piece, bz],
                      two_recv.at[piece, bz], device)

    def along(piece, bz, way):
        device = device_at(z + 1, y, x, core) if way == 0 else device_at(z - 1, y, x, core)
        return remote(at(acc, piece, chip_index(bz, y, x)), at(line, piece, way, bz),
                      line_send.at[piece, way, bz], line_recv.at[piece, way, bz], device)

    def begin():
        greet(depth)
        for bz in order:
            for flip_y, flip_x in ((1, 1), (0, 1), (1, 0), (0, 0)):
                for piece in every:
                    if turned(piece):
                        flip_y, flip_x = flip_x, flip_y
                    by = 1 - y if flip_y else y
                    bx = 1 - x if flip_x else x
                    swap(piece, bz, by, bx).start()
                    load(piece, bz, by, bx).start()
                    if turned(piece):
                        flip_y, flip_x = flip_x, flip_y

    def join(piece, bz, by, bx, extra=()):
        load(piece, bz, by, bx).wait()
        swap(piece, bz, by, bx).wait_recv()
        mine = at(acc, piece, chip_index(bz, by, bx))
        add_rows(mine, (mine, at(swapped, piece, chip_index(bz, by, bx))) + extra)

    def send_first(bz):
        for far in range(2):
            for piece in every:
                if turned(piece):
                    spot = x if far else 1 - x
                    join(piece, bz, 1 - y, spot)
                else:
                    spot = y if far else 1 - y
                    join(piece, bz, spot, 1 - x)
                stage_one(piece, bz, spot).start()

    def send_second(bz):
        for piece in every:
            spot = 1 - x if turned(piece) else 1 - y
            stage_one(piece, bz, spot).wait_recv()
            arrived = (at(first, piece, 2 * bz + spot),)
            if turned(piece):
                join(piece, bz, y, spot, arrived)
            else:
                join(piece, bz, spot, x, arrived)
            stage_two(piece, bz).start()

    def gathered(piece, bz):
        spot = x if turned(piece) else y
        stage_one(piece, bz, spot).wait_recv()
        stage_two(piece, bz).wait_recv()
        load(piece, bz, y, x).wait()
        swap(piece, bz, y, x).wait_recv()
        mine = at(acc, piece, chip_index(bz, y, x))
        return mine, (mine, at(swapped, piece, chip_index(bz, y, x)),
                      at(first, piece, 2 * bz + spot), at(second, piece, bz))

    def pass_on(bz, level, way):
        for piece in every:
            mine, base = gathered(piece, bz)
            if level > 0:
                along(piece, bz, way).wait_recv()
                base = base + (at(line, piece, way, bz),)
            add_rows(mine, base)
            along(piece, bz, way).start()

    def pass_level(bz, level):
        if level < bz:
            pl.when(z == level)(lambda: pass_on(bz, level, 0))
        if depth - 1 - level > bz:
            pl.when(z == depth - 1 - level)(lambda: pass_on(bz, level, 1))

    def finish(bz):
        @pl.when(z == bz)
        def _():
            ways = ((0,) if bz > 0 else ()) + ((1,) if bz < depth - 1 else ())
            for piece in every:
                n, cut = pieces[piece]
                _, base = gathered(piece, bz)
                for way in ways:
                    along(piece, bz, way).wait_recv()
                add_rows(sums[n].at[cut], base + tuple(at(line, piece, way, bz) for way in ways))

    def exchange(n):
        return remote(outs[n], ins[n], end_send.at[n], end_recv.at[n], partner)

    width, half = sizes.width, sizes.down // 2

    def hand_over():
        for me in range(2):
            @pl.when(core == me)
            def _(me=me):
                far = 1 - me
                for n, name in enumerate(names):
                    if name == "inner":
                        outs[n][...] = sums[n][far]
                        owns[n][me] = sums[n][me]
                    elif name == "outer":
                        outs[n][...] = sums[n][far]
                        owns[n][me * half : (me + 1) * half] = sums[n][me]
                    else:
                        outs[n][...] = sums[n][:, :, far * width : (far + 1) * width]
                        for k in range(2):
                            mine = sums[n][k, :, me * width : (me + 1) * width]
                            owns[n][2 * me + k] = mine.T
        for n in range(count):
            exchange(n).start()

    def end():
        for n in range(count):
            exchange(n).wait_recv()
        for me in range(2):
            @pl.when(core == me)
            def _(me=me):
                far = 1 - me
                for n, name in enumerate(names):
                    if name == "inner":
                        owns[n][far] = ins[n][...]
                    elif name == "outer":
                        owns[n][far * half : (far + 1) * half] = ins[n][...]
                    else:
                        for k in range(2):
                            owns[n][2 * far + k] = ins[n][k].T
        for n in range(count):
            exchange(n).wait_send()
        for piece in every:
            @pl.loop(0, depth)
            def _(bz, piece=piece):
                for by in range(2):
                    for bx in range(2):
                        swap(piece, bz, by, bx).wait_send()
                for spot in range(2):
                    stage_one(piece, bz, spot).wait_send()
                stage_two(piece, bz).wait_send()
                pl.when(z < bz)(lambda: along(piece, bz, 0).wait_send())
                pl.when(z > bz)(lambda: along(piece, bz, 1).wait_send())

    timed = [(0, begin)]
    for turn, bz in enumerate(order):
        timed.append((turn, functools.partial(send_first, bz)))
        timed.append(((2, 4, 5, 7)[turn], functools.partial(send_second, bz)))
        for level in range(depth - 1):
            when = ((4, 6, 8), (8, 10, 12), (9, 11, 12), (9, 12, 12))[turn][level]
            timed.append((when, functools.partial(pass_level, bz, level)))
    ending = [functools.partial(finish, bz) for bz in order] + [hand_over, end]
    timed.append((13, functools.partial(in_turn, ending)))
    return sorted(timed, key=lambda item: item[0])


def in_turn(actions):
    for action in actions:
        action()


def run_stages(timed, step, number, steps):
    mine = [stage for time, stage in timed if time < 12 and time * steps // 12 == number]
    if mine:
        pl.when(step == number)(functools.partial(in_turn, mine))


HBM = pl.BlockSpec(memory_space=pl.ANY)
VMEM = pl.BlockSpec(memory_space=pltpu.VMEM)


def gather_kernel(sizes, names, *refs):
    count = len(names)
    gain_ref, gain_out, send, recv = refs[count], refs[2 * count + 1], *refs[-2:]
    stages = gather_stages(sizes, names, refs[:count], refs[count + 1 : 2 * count + 1],
                           refs[2 * count + 2 : -2])
    z, y, x, core = where_am_i()
    mine, near = 2 * x + core, 2 * x + 1 - core
    far, corner = 2 * (1 - x) + core, 2 * (1 - x) + 1 - core

    def pass_gain(src, slot, kind, device):
        return remote(src, gain_out.at[slot], send.at[kind], recv.at[kind], device)

    partner, beside = device_at(z, y, x, 1 - core), device_at(z, y, 1 - x, core)
    hops = (
        (gain_ref, mine, 0, partner),
        (gain_ref, mine, 1, beside),
        (gain_out.at[near], near, 2, beside),
    )
    stages = [stage for _, stage in stages]
    stages[0]()
    gain_out[mine] = gain_ref[...]
    pass_gain(*hops[0]).start()
    pass_gain(*hops[1]).start()
    stages[1]()
    pass_gain(gain_ref, near, 0, partner).wait_recv()
    pass_gain(*hops[2]).start()
    for stage in stages[2:]:
        stage()
    pass_gain(gain_ref, far, 1, beside).wait_recv()
    pass_gain(gain_ref, corner, 2, beside).wait_recv()
    for hop in hops:
        pass_gain(*hop).wait_send()


def gather_blocks(sizes, names, shards, gain):
    wave = pltpu.SemaphoreType.DMA
    return pl.pallas_call(
        functools.partial(gather_kernel, sizes, names),
        out_shape=[jax.ShapeDtypeStruct(sizes.full(name), bf16) for name in names]
        + [jax.ShapeDtypeStruct((sizes.within,) + gain.shape, f32)],
        in_specs=[VMEM] * (len(names) + 1),
        out_specs=[HBM] * len(names) + [VMEM],
        scratch_shapes=gather_scratch(sizes, names) + [wave((3,)), wave((3,))],
        compiler_params=pltpu.CompilerParams(collective_id=0, has_side_effects=True),
        name="gather_blocks",
    )(*shards, gain)


def gain_stages(depth, gain_ref, gain_out, buf, send, recv):
    z, y, x, core = where_am_i()
    hops = (device_at(z, y, x, 1 - core), device_at(z, y, 1 - x, core),
            device_at(z, 1 - y, x, core))

    def hop(step):
        return remote(buf.at[2 * step], buf.at[2 * step + 1], send.at[step], recv.at[step],
                      hops[step])

    def line(way):
        device = device_at(z + 1, y, x, core) if way == 0 else device_at(z - 1, y, x, core)
        return remote(buf.at[7 + way], buf.at[9 + way], send.at[3 + way], recv.at[3 + way],
                      device)

    def begin():
        buf[0] = gain_ref[...]
        hop(0).start()

    def turn(step):
        hop(step).wait_recv()
        buf[2 * step + 2] = buf[2 * step] + buf[2 * step + 1]
        if step < 2:
            hop(step + 1).start()

    def rightward():
        gain_out[...] = buf[6]

        @pl.when(z > 0)
        def _():
            line(0).wait_recv()
            gain_out[...] = gain_out[...] + buf[9]

        @pl.when(z < depth - 1)
        def _():
            buf[7] = gain_out[...]
            line(0).start()

    def leftward():
        buf[8] = buf[6]

        @pl.when(z < depth - 1)
        def _():
            line(1).wait_recv()
            gain_out[...] = gain_out[...] + buf[10]
            buf[8] = buf[6] + buf[10]

        pl.when(z > 0)(lambda: line(1).start())

    def end():
        for step in range(3):
            hop(step).wait_send()
        pl.when(z < depth - 1)(lambda: line(0).wait_send())
        pl.when(z > 0)(lambda: line(1).wait_send())

    return [begin] + [functools.partial(turn, step) for step in range(3)] + [
        rightward, leftward, end]


def scatter_kernel(sizes, names, k_ref, v_ref, wk_ref, wv_ref, *refs):
    count = len(names)
    fulls, gain_ref, grad_ref = refs[:count], refs[count], refs[count + 1]
    owns, gain_out = refs[count + 2 : 2 * count + 2], refs[2 * count + 2]
    gain_scratch, scratch = refs[2 * count + 3 : 2 * count + 6], refs[2 * count + 6 :]
    stages = scatter_stages(sizes, names, fulls, owns, scratch)
    gains = gain_stages(sizes.depth, gain_ref, gain_out, *gain_scratch)
    joined = [(0, stages[0][1])]
    for number, (_, stage) in enumerate(stages[1:]):
        both = functools.partial(in_turn, [stage] + gains[number : number + 1])
        joined.append((12 * (number + 1) / len(stages), both))
    steps = pl.num_programs(0)
    for number in range(steps):
        run_stages(joined, pl.program_id(0), number, steps)
    grad_ref[...] = dot_nn(k_ref[...], wk_ref[0]) + dot_nn(v_ref[...], wv_ref[0])


def scatter_blocks(sizes, names, fulls, gains, grad_key, grad_value, projections):
    wave = pltpu.SemaphoreType.DMA
    slab = 256
    rows = pl.BlockSpec((slab, D), lambda step: (step, 0))

    def matrix(which):
        return pl.BlockSpec((1, D, D), lambda step: (which, 0, 0))

    return pl.pallas_call(
        functools.partial(scatter_kernel, sizes, names),
        grid=(grad_key.shape[0] // slab,),
        out_shape=[jax.ShapeDtypeStruct(grad_key.shape, f32)]
        + [jax.ShapeDtypeStruct(sizes.owned(name), f32) for name in names]
        + [jax.ShapeDtypeStruct(gains.shape, f32)],
        in_specs=[rows, rows, matrix(1), matrix(2)] + [HBM] * len(names) + [VMEM],
        out_specs=[rows] + [VMEM] * (len(names) + 1),
        scratch_shapes=[pltpu.VMEM((11,) + gains.shape, f32), wave((5,)), wave((5,))]
        + scatter_scratch(sizes, names),
        compiler_params=pltpu.CompilerParams(
            collective_id=1, has_side_effects=True, vmem_limit_bytes=60 * 1024 * 1024
        ),
        name="scatter_blocks",
    )(grad_key, grad_value, projections, projections, *fulls, gains)


def tile_aligned(down, width, side, deep):
    return (
        lax.axis_size("fsdp") == 4
        and lax.axis_size("dp") in (2, 4, 8)
        and down % 96 == 0
        and width % 48 == 0
        and (2 * width) % 128 == 0
        and side % 128 == 0
        and deep % 128 == 0
    )


def adam_update(weight, mean_old, square_old, gradient, step_rate, decay_rate):
    mean_new = beta_one * mean_old + (1.0 - beta_one) * gradient
    square_new = beta_two * square_old + (1.0 - beta_two) * gradient * gradient
    corrected = (
        mean_new
        / (1.0 - beta_one**STEP)
        / (jnp.sqrt(square_new / (1.0 - beta_two**STEP)) + adam_epsilon)
    )
    master = weight - step_rate * (corrected + decay_rate * weight)
    return (mean_new, square_new, master, master.astype(bf16))


def on_device(
    hidden_in,
    patches,
    token_segments,
    patch_segments,
    cotangent,
    attention_weights,
    attention_means,
    attention_squares,
    inner_weights,
    inner_means,
    inner_squares,
    outer_weights,
    outer_means,
    outer_squares,
    norm_gains,
    gain_means,
    gain_squares,
):
    rows, _, length, _ = hidden_in.shape
    count = patches.shape[2]
    tokens = rows * length
    width, down = attention_weights.shape[1:]
    side, deep = inner_weights.shape[2], outer_weights.shape[0]
    direct = tile_aligned(down, width, side, deep)
    low_inner, low_outer = inner_weights.astype(bf16), outer_weights.astype(bf16)
    if direct:
        sizes = Sizes(down, width, side, deep)
        turned = jnp.swapaxes(attention_weights, 1, 2).astype(bf16)
        parts = norm_gains.shape[1]
        gain_block = jnp.pad(
            norm_gains.astype(bf16).astype(f32), ((0, 8 - norm_gains.shape[0]), (0, -parts % 128))
        )
        low, high, gains = gather_blocks(
            sizes, ("low", "high"), (turned[:4], turned[4:]), gain_block
        )
        gains = jnp.swapaxes(gains[:, : norm_gains.shape[0], :parts], 0, 1).reshape(-1, D)
        rest, rest_shards = ("inner", "outer"), (low_inner, low_outer.T)
    else:
        sizes = None
        gains = lax.all_gather(norm_gains.astype(bf16), "fsdp", axis=1, tiled=True)
        weights, inner, outer = gather_weights(
            attention_weights.astype(bf16), low_inner, low_outer
        )
        low, high = weights[:4], weights[4:]
        inner = jnp.concatenate([inner[0], inner[1]], axis=1)
        rest, rest_shards = (), ()

    initial = hidden_in.reshape(tokens, D).astype(f32)
    token_rows = token_segments.reshape(rows, 1, length)
    token_columns = token_segments.reshape(rows, length, 1)
    patch_ids = patch_segments.reshape(rows, 1, count)

    normed_one, unit_one, rms_one = norm_forward(initial, gains[0])
    stacked = low.reshape(4 * D, D)
    packed = dot_nt(normed_one, stacked).astype(bf16).reshape(rows, length, 4 * D)
    mixture_one, lse_one = self_forward(packed, token_rows, token_columns)
    mixed_one = mixture_one.reshape(tokens, D)
    after_one = initial + dot_nt(mixed_one, low[3])
    normed_two, unit_two, rms_two = norm_forward(after_one, gains[1])
    cross_query = dot_nt(normed_two, high[0]).astype(bf16).reshape(rows, length, D)
    mixture_two, lse_two, cross_key, cross_value, *arrived = cross_forward(
        Rider(sizes, rest, "gather", 2, rows * PAIRS), cross_query, patches.reshape(rows, count, D), high,
        token_columns, patch_ids, rest_shards,
    )
    if direct:
        inner, outer = arrived
    mixed_two = mixture_two.reshape(tokens, D)
    after_two = after_one + dot_nt(mixed_two, high[3])
    normed_three, unit_three, rms_three = norm_forward(after_two, gains[2])
    gated = dot_nn(normed_three, inner)
    hidden_units = outer.shape[1]
    gate, up = gated[:, :hidden_units], gated[:, hidden_units:]
    units = (gelu_tanh(gate) * up).astype(bf16)
    hidden_out = (after_two + dot_nt(units, outer)).astype(bf16)

    grad_low = cotangent.reshape(tokens, D)
    grad_final = grad_low.astype(f32)
    grad_outer = dot_tn(grad_low, units).astype(bf16)
    grad_units = dot_nn(grad_low, outer)
    activation, gelu_back = jax.vjp(gelu_tanh, gate)
    grad_gated = jnp.concatenate(
        [gelu_back(grad_units * up)[0], grad_units * activation], axis=1
    ).astype(bf16)
    grad_inner = dot_tn(normed_three, grad_gated).astype(bf16)
    grad_normed = dot_nt(grad_gated, inner)
    grad_from_three, gain_three = norm_backward(grad_normed, gains[2], unit_three, rms_three)
    grad_two = grad_final + grad_from_three
    branch_two = grad_two.astype(bf16)
    grad_mixture_two = dot_nn(branch_two, high[3]).astype(bf16).reshape(rows, length, D)
    grad_cq, grad_ck, grad_cv, grad_pair, *summed_rest = cross_backward(
        Rider(sizes, rest, "scatter", 3, rows * PAIRS), cross_query, cross_key, cross_value,
        mixture_two, grad_mixture_two, lse_two, token_columns, patch_ids,
        patches.reshape(rows, count, D), (grad_inner, grad_outer) if direct else (),
    )
    grad_cq = grad_cq.reshape(tokens, D)
    grad_ck = grad_ck.reshape(rows * count, D)
    grad_cv = grad_cv.reshape(rows * count, D)
    grad_high = grad_pair.at[0].set(dot_tn(grad_cq, normed_two).astype(bf16))
    grad_high = grad_high.at[3].set(dot_tn(branch_two, mixed_two).astype(bf16))
    grad_from_two, gain_two = norm_backward(
        dot_nn(grad_cq, high[0]), gains[1], unit_two, rms_two
    )
    grad_one = grad_two + grad_from_two
    branch_one = grad_one.astype(bf16)
    grad_mixture_one = dot_nn(branch_one, low[3]).astype(bf16).reshape(rows, length, D)
    grad_packed = self_backward(
        packed, mixture_one, grad_mixture_one, lse_one, token_rows, token_columns
    ).reshape(tokens, 4 * D)
    grad_normed_one = dot_nn(grad_packed, stacked)
    grad_from_one, gain_one = norm_backward(grad_normed_one, gains[0], unit_one, rms_one)
    hidden_grad = grad_one + grad_from_one
    grad_first = dot_tn(grad_packed, normed_one).astype(bf16).reshape(4, D, D)
    grad_first = grad_first.at[3].set(dot_tn(branch_one, mixed_one).astype(bf16))
    gain_grads = jnp.stack([gain_one, gain_two, gain_three])
    if direct:
        own_inner, own_outer = summed_rest
        patch_grad, own_low, own_high, gain_totals = scatter_blocks(
            sizes, ("low", "high"), (grad_first, grad_high),
            jnp.pad(gain_grads, ((0, 5), (0, 0))), grad_ck, grad_cv, high,
        )
        own_attention = jnp.concatenate([own_low, own_high])
        own_outer = own_outer.T
        gain_totals = gain_totals[:3]
    else:
        patch_grad = dot_nn(grad_ck, high[1]) + dot_nn(grad_cv, high[2])
        own_attention, own_inner, own_outer = scatter_grads(
            jnp.concatenate([grad_first, grad_high]),
            jnp.stack([grad_inner[:, :hidden_units], grad_inner[:, hidden_units:]]),
            grad_outer,
        )
        gain_totals = lax.psum(gain_grads, BOTH)
    width = norm_gains.shape[1]
    own_gains = lax.dynamic_slice_in_dim(
        gain_totals, lax.axis_index("fsdp") * width, width, axis=1
    )

    attention_new = adam_update(
        attention_weights, attention_means, attention_squares, own_attention,
        rate_matrix, decay_matrix,
    )
    inner_new = adam_update(
        inner_weights, inner_means, inner_squares, own_inner, rate_matrix, decay_matrix
    )
    outer_new = adam_update(
        outer_weights, outer_means, outer_squares, own_outer, rate_matrix, decay_matrix
    )
    gain_new = adam_update(norm_gains, gain_means, gain_squares, own_gains, rate_gain, 0.0)
    return (
        hidden_out.reshape(hidden_in.shape),
        hidden_grad.reshape(hidden_in.shape),
        patch_grad.reshape(patches.shape),
        *attention_new,
        *inner_new,
        *outer_new,
        *gain_new,
    )


def solution(mesh):
    rows = P(None, BOTH, None, None)
    ids = P(None, BOTH, None)
    matrix = P(None, "fsdp", "dp")
    down = P("fsdp", "dp")
    gain = P(None, "fsdp")
    return jax.shard_map(
        on_device,
        mesh=mesh,
        in_specs=(rows, rows, ids, ids, rows) + (matrix,) * 6 + (down,) * 3 + (gain,) * 3,
        out_specs=(rows, rows, rows) + (matrix,) * 8 + (down,) * 4 + (gain,) * 4,
        check_vma=False,
    )
```

```python
import functools

import jax
import jax.numpy as jnp
from jax import lax
from jax.experimental import pallas as pl
from jax.experimental.pallas import tpu as pltpu
from jax.sharding import PartitionSpec as P

D = 768
HEADS = 12
HEAD = 64
PAIR = 2 * HEAD
PAIRS = HEADS // 2
GROUP = 3
STEP = 10
SEGS = 4

epsilon = 1e-06
score_scale = 0.125
masked_value = -1000000000.0
beta_one = 0.9
beta_two = 0.95
adam_epsilon = 1e-08
decay_matrix = 0.1
rate_matrix = 0.1
rate_gain = 0.3
f32 = jnp.float32
bf16 = jnp.bfloat16
BOTH = ("dp", "fsdp")


def gelu_tanh(values):
    return (
        0.5
        * values
        * (1.0 + jnp.tanh(0.7978845608028654 * (values + 0.044715 * values * values * values)))
    )


def dot_nn(a, b):
    return lax.dot_general(a, b, (((1,), (0,)), ((), ())), preferred_element_type=f32)


def dot_nt(a, b):
    return lax.dot_general(a, b, (((1,), (1,)), ((), ())), preferred_element_type=f32)


def dot_tn(a, b):
    return lax.dot_general(a, b, (((0,), (0,)), ((), ())), preferred_element_type=f32)


def norm_forward(values, gain):
    inverse_rms = lax.rsqrt(jnp.mean(values * values, axis=-1, keepdims=True) + epsilon)
    unit_rows = values * inverse_rms
    return ((unit_rows * gain.astype(f32)).astype(bf16), unit_rows, inverse_rms)


def norm_backward(grad_rows, gain, unit_rows, inverse_rms):
    grad_unit = grad_rows * gain.astype(f32)
    grad_values = inverse_rms * (
        grad_unit - unit_rows * jnp.mean(grad_unit * unit_rows, axis=-1, keepdims=True)
    )
    return (grad_values, jnp.sum(grad_rows * unit_rows, axis=0))


def head_half(block, half):
    lane = lax.broadcasted_iota(jnp.int32, block.shape, 1)
    keep = (lane < HEAD) if half == 0 else (lane >= HEAD)
    return jnp.where(keep, block, jnp.zeros_like(block))


def three_parts(column):
    high = column.astype(bf16).astype(f32)
    rest = column - high
    middle = rest.astype(bf16).astype(f32)
    low = rest - middle
    return high, middle, low


def stat_lanes(base, column, first):
    lane = lax.broadcasted_iota(jnp.int32, base.shape, 1)
    for place, part in enumerate(three_parts(column)):
        base = jnp.where(lane == first + place, -part, base)
    return base


def turned_marks(key_ids):
    spot = lax.broadcasted_iota(jnp.int32, (128, key_ids.shape[1]), 0)
    return jnp.where(spot == key_ids, 1.0, 0.0).astype(bf16).T


def key_marks(key_ids, stats):
    lane = lax.broadcasted_iota(jnp.int32, (key_ids.shape[0], 128), 1)
    marks = lane == key_ids
    if stats:
        marks = marks | ((lane >= SEGS) & (lane < SEGS + 3))
    return jnp.where(marks, 1.0, 0.0).astype(bf16)


def query_bias(query_ids):
    lane = lax.broadcasted_iota(jnp.int32, (query_ids.shape[0], 128), 1)
    return jnp.where((lane == query_ids) | (lane >= SEGS), 0.0, masked_value)


def softmax_columns(scores):
    top = jnp.max(scores, axis=0, keepdims=True)
    raised = jnp.exp(scores - top)
    return raised, top, jnp.sum(raised, axis=0, keepdims=True)


def finish_forward(halves, tops, sums):
    mixed = jnp.concatenate([h / s for h, s in zip(halves, sums)], axis=0)
    rows = [t + jnp.log(s) for t, s in zip(tops, sums)]
    pad = jnp.zeros((6, rows[0].shape[1]), f32)
    return mixed.T.astype(bf16), jnp.concatenate(rows + [pad], axis=0)


def cross_forward_kernel(rider, q_ref, c_ref, wk_ref, wv_ref, qid_ref, kid_ref, *refs):
    (o_ref, lse_ref, k_ref, v_ref) = rider.board(refs, 4)
    both = jnp.concatenate([wk_ref[0], wv_ref[0]], axis=0)
    projected = dot_nt(c_ref[0], both).astype(bf16)
    key, value = projected[:, :PAIR], projected[:, PAIR:]
    k_ref[0], v_ref[0] = key, value
    marked = jnp.concatenate([key, turned_marks(kid_ref[0])], axis=1)
    bias = query_bias(qid_ref[0]).astype(bf16)
    query = q_ref[0] * jnp.asarray(score_scale, bf16)
    values = value.T
    halves, tops, sums = [], [], []
    scored = [
        dot_nt(marked, jnp.concatenate([head_half(query, half), bias], axis=1))
        for half in range(2)
    ]
    for half in range(2):
        raised, top, total = softmax_columns(scored[half])
        halves.append(dot_nn(values[half * HEAD : (half + 1) * HEAD], raised.astype(bf16)))
        tops.append(top)
        sums.append(total)
    o_ref[0], lse_ref[0, 0] = finish_forward(halves, tops, sums)
    rider.leave()


def causal_mask(qid_ref, kid_ref):
    length = kid_ref.shape[1]
    key = lax.broadcasted_iota(jnp.int32, (length, length), 0)
    query = lax.broadcasted_iota(jnp.int32, (length, length), 1)
    return (key <= query) & (kid_ref[0] == qid_ref[0])


def pair_lanes(pair):
    return slice(pair * PAIR, (pair + 1) * PAIR)


def self_forward_kernel(q_ref, k_ref, v_ref, qid_ref, kid_ref, o_ref, lse_ref):
    allowed = causal_mask(qid_ref, kid_ref)
    for pair in range(GROUP):
        lanes = pair_lanes(pair)
        query = q_ref[0, :, lanes] * jnp.asarray(score_scale, bf16)
        key = k_ref[0, :, lanes]
        values = v_ref[0, :, lanes].T
        halves, tops, sums = [], [], []
        for half in range(2):
            scores = jnp.where(allowed, dot_nt(key, head_half(query, half)), masked_value)
            raised, top, total = softmax_columns(scores)
            halves.append(dot_nn(values[half * HEAD : (half + 1) * HEAD], raised.astype(bf16)))
            tops.append(top)
            sums.append(total)
        o_ref[0, :, lanes], lse_ref[0, pair] = finish_forward(halves, tops, sums)


def backward_pair(query, key, value, mixed, grad, lse, marked, bias, allowed):
    scaled = query * jnp.asarray(score_scale, bf16)
    key_turned = key.T
    length = query.shape[0]
    lse_columns = lse.T
    product = mixed.astype(f32) * grad.astype(f32)
    ones = key_marks(jnp.full((value.shape[0], 1), -1, jnp.int32), True)
    valued = jnp.concatenate([value, ones], axis=1)
    scored, shifted = [], []
    for half in range(2):
        stats = stat_lanes(bias, lse_columns[:, half : half + 1], SEGS).astype(bf16)
        scored.append(
            dot_nt(marked, jnp.concatenate([head_half(scaled, half), stats], axis=1)))
        inner = jnp.sum(head_half(product, half), axis=1, keepdims=True)
        delta = stat_lanes(jnp.zeros((length, 128), f32), inner, SEGS).astype(bf16)
        shifted.append(dot_nt(valued, jnp.concatenate([head_half(grad, half), delta], axis=1)))
    probs, grads, turned = [], [], []
    for half in range(2):
        scores = scored[half]
        if allowed is not None:
            scores = jnp.where(allowed, scores, masked_value)
        weight = jnp.exp(scores)
        grad_scores = (weight * shifted[half]).astype(bf16)
        probs.append(weight.astype(bf16))
        grads.append(grad_scores)
        turned.append(dot_nn(key_turned[half * HEAD : (half + 1) * HEAD], grad_scores))
    grad_query = (score_scale * jnp.concatenate(turned, axis=0)).T.astype(bf16)
    grad_turned, scaled_turned = grad.T, scaled.T
    halves = [slice(0, HEAD), slice(HEAD, PAIR)]
    value_turned = jnp.concatenate(
        [dot_nt(grad_turned[h], p) for h, p in zip(halves, probs)], axis=0).astype(bf16)
    keyed_turned = jnp.concatenate(
        [dot_nt(scaled_turned[h], p) for h, p in zip(halves, grads)], axis=0).astype(bf16)
    grad_value, grad_key = value_turned.T, keyed_turned.T
    return grad_query, grad_key, grad_value, keyed_turned, value_turned


def cross_backward_kernel(rider, q_ref, k_ref, v_ref, o_ref, do_ref, lse_ref, qid_ref, kid_ref,
                          c_ref, *refs):
    total_ref = refs[-1]
    dq_ref, dk_ref, dv_ref, sum_ref = rider.board(refs[:-1], 4)
    ones = key_marks(jnp.full((k_ref.shape[1], 1), -1, jnp.int32), True)
    marked = jnp.concatenate([k_ref[0], turned_marks(kid_ref[0]) + ones], axis=1)
    dq_ref[0], grad_key, grad_value, key_t, value_t = backward_pair(
        q_ref[0], k_ref[0], v_ref[0], o_ref[0], do_ref[0], lse_ref[0, 0], marked,
        query_bias(qid_ref[0]), None)
    dk_ref[0], dv_ref[0] = grad_key, grad_value
    row, pair = pl.program_id(0), pl.program_id(1)
    part = dot_nn(jnp.concatenate([key_t, value_t], axis=0), c_ref[0])

    @pl.when(row == 0)
    def _():
        total_ref[pair] = part

    @pl.when(row > 0)
    def _():
        total_ref[pair] = total_ref[pair] + part

    @pl.when(row == pl.num_programs(0) - 1)
    def _():
        at = pl.ds(pl.multiple_of(pair * PAIR, PAIR), PAIR)
        sum_ref[1, at] = total_ref[pair, :PAIR].astype(bf16)
        sum_ref[2, at] = total_ref[pair, PAIR:].astype(bf16)
        sum_ref[0, at] = jnp.zeros((PAIR, D), bf16)
        sum_ref[3, at] = jnp.zeros((PAIR, D), bf16)

    rider.leave()


def self_backward_kernel(q_ref, k_ref, v_ref, o_ref, do_ref, lse_ref, qid_ref, kid_ref,
                         grad_ref):
    length = k_ref.shape[1]
    ones = key_marks(jnp.full((length, 1), -1, jnp.int32), True)
    allowed = causal_mask(qid_ref, kid_ref)
    for pair in range(GROUP):
        lanes = pair_lanes(pair)
        key = k_ref[0, :, lanes]
        parts = backward_pair(
            q_ref[0, :, lanes], key, v_ref[0, :, lanes], o_ref[0, :, lanes],
            do_ref[0, :, lanes], lse_ref[0, pair], jnp.concatenate([key, ones], axis=1),
            jnp.zeros((length, 128), f32), allowed)[:3]
        for part, value in enumerate(parts):
            first = part * D + (pl.program_id(1) * GROUP + pair) * PAIR
            grad_ref[0, :, pl.ds(pl.multiple_of(first, PAIR), PAIR)] = value

    @pl.when(pl.program_id(1) == 0)
    def _():
        grad_ref[0, :, 3 * D :] = jnp.zeros((length, D), bf16)


def pair_spec(length, offset, pairs=1):
    return pl.BlockSpec((1, length, pairs * PAIR), lambda row, step: (row, 0, offset + step))


def row_spec(shape):
    return pl.BlockSpec((1,) + shape, lambda row, step: (row, 0, 0))


def stat_spec(length, pairs=1):
    return pl.BlockSpec((1, pairs, 8, length), lambda row, step: (row, step, 0, 0))


def cost(rows, queries, keys, products):
    elements = rows * HEADS * queries * keys
    return pl.CostEstimate(
        flops=2 * elements * 256 * products // 2,
        transcendentals=elements,
        bytes_accessed=rows * (queries + keys) * D * 2 * 3,
    )


class Rider:
    def __init__(self, sizes, names, kind, number, steps):
        self.sizes, self.names, self.kind, self.number = sizes, names, kind, number
        self.steps = steps

    def board(self, refs, outputs):
        count = len(self.names)
        theirs, mine, scratch = refs[:count], refs[count : count + outputs], refs[count + outputs :]
        if count:
            ends, scratch = scratch[:count], scratch[count:]
            build = gather_stages if self.kind == "gather" else scatter_stages
            stages = build(self.sizes, self.names, theirs, ends, scratch)
            step = pl.program_id(0) * pl.num_programs(1) + pl.program_id(1)
            for number in range(self.steps):
                run_stages(stages, step, number, self.steps)
            self.rest = ([s for time, s in stages if time >= 12], step == self.steps - 1)
        return mine

    def leave(self):
        if self.names and self.rest[0]:
            pl.when(self.rest[1])(functools.partial(in_turn, self.rest[0]))

    def in_specs(self):
        return [VMEM if self.kind == "gather" else HBM] * len(self.names)

    def out_specs(self):
        return [HBM if self.kind == "gather" else VMEM] * len(self.names)

    def out_shape(self):
        if self.kind == "gather":
            return [jax.ShapeDtypeStruct(self.sizes.full(n), bf16) for n in self.names]
        return [jax.ShapeDtypeStruct(self.sizes.owned(n), f32) for n in self.names]

    def scratch(self):
        if not self.names:
            return []
        build = gather_scratch if self.kind == "gather" else scatter_scratch
        return build(self.sizes, self.names)

    def params(self):
        if not self.names:
            return pltpu.CompilerParams()
        return pltpu.CompilerParams(
            collective_id=self.number, has_side_effects=True, vmem_limit_bytes=60 * 1024 * 1024
        )


def self_forward(packed, query_ids, key_ids):
    rows, length = packed.shape[:2]
    steps = PAIRS // GROUP
    return pl.pallas_call(
        self_forward_kernel,
        grid=(rows, steps),
        in_specs=[pair_spec(length, part * steps, GROUP) for part in range(3)]
        + [row_spec((1, length)), row_spec((length, 1))],
        out_specs=[pair_spec(length, 0, GROUP), stat_spec(length, GROUP)],
        out_shape=[
            jax.ShapeDtypeStruct((rows, length, D), bf16),
            jax.ShapeDtypeStruct((rows, PAIRS, 8, length), f32),
        ],
        cost_estimate=cost(rows, length, length, 2),
        name="self_forward",
    )(packed, packed, packed, query_ids, key_ids)


def self_backward(packed, mixed, grad, lse, query_ids, key_ids):
    rows, length = packed.shape[:2]
    steps = PAIRS // GROUP
    plain = pair_spec(length, 0, GROUP)
    return pl.pallas_call(
        self_backward_kernel,
        grid=(rows, steps),
        in_specs=[pair_spec(length, part * steps, GROUP) for part in range(3)]
        + [plain, plain, stat_spec(length, GROUP), row_spec((1, length)), row_spec((length, 1))],
        out_specs=row_spec((length, 4 * D)),
        out_shape=jax.ShapeDtypeStruct((rows, length, 4 * D), bf16),
        cost_estimate=cost(rows, length, length, 5),
        name="self_backward",
    )(packed, packed, packed, mixed, grad, lse, query_ids, key_ids)


def cross_forward(rider, queries, patches, projections, query_ids, key_ids, shards):
    rows, length = queries.shape[:2]
    count = patches.shape[1]

    def slab(which):
        return pl.BlockSpec((1, PAIR, D), lambda row, pair: (which, pair, 0))

    return pl.pallas_call(
        functools.partial(cross_forward_kernel, rider),
        grid=(rows, PAIRS),
        in_specs=[
            pair_spec(length, 0),
            row_spec((count, D)),
            slab(1),
            slab(2),
            row_spec((length, 1)),
            row_spec((1, count)),
        ]
        + rider.in_specs(),
        out_specs=[
            pair_spec(length, 0), stat_spec(length), pair_spec(count, 0), pair_spec(count, 0),
        ]
        + rider.out_specs(),
        out_shape=[
            jax.ShapeDtypeStruct((rows, length, D), bf16),
            jax.ShapeDtypeStruct((rows, PAIRS, 8, length), f32),
            jax.ShapeDtypeStruct((rows, count, D), bf16),
            jax.ShapeDtypeStruct((rows, count, D), bf16),
        ]
        + rider.out_shape(),
        scratch_shapes=rider.scratch(),
        compiler_params=rider.params(),
        cost_estimate=cost(rows, length, count, 4),
        name="cross_forward",
    )(queries, patches, projections, projections, query_ids, key_ids, *shards)


def cross_backward(rider, queries, keys, values, mixed, grad, lse, query_ids, key_ids, patches,
                   fulls):
    rows, length = grad.shape[:2]
    count = keys.shape[1]
    short, tall = pair_spec(length, 0), pair_spec(count, 0)
    return pl.pallas_call(
        functools.partial(cross_backward_kernel, rider),
        grid=(rows, PAIRS),
        in_specs=[
            short, tall, tall, short, short, stat_spec(length), row_spec((length, 1)),
            row_spec((1, count)), row_spec((count, D)),
        ]
        + rider.in_specs(),
        out_specs=[short, tall, tall, VMEM] + rider.out_specs(),
        out_shape=[
            jax.ShapeDtypeStruct((rows, length, D), bf16),
            jax.ShapeDtypeStruct((rows, count, D), bf16),
            jax.ShapeDtypeStruct((rows, count, D), bf16),
            jax.ShapeDtypeStruct((4, D, D), bf16),
        ]
        + rider.out_shape(),
        scratch_shapes=rider.scratch() + [pltpu.VMEM((PAIRS, 2 * PAIR, D), f32)],
        compiler_params=rider.params(),
        cost_estimate=cost(rows, length, count, 7),
        name="cross_backward",
    )(queries, keys, values, mixed, grad, lse, query_ids, key_ids, patches, *fulls)


def gather_weights(attention, inner, outer):
    turned = lax.all_gather(jnp.swapaxes(attention, 1, 2), BOTH, axis=0, tiled=False)
    heads = lax.axis_size("dp"), lax.axis_size("fsdp")
    turned = turned.reshape(heads + turned.shape[1:])
    full_attention = jnp.transpose(turned, (2, 0, 3, 1, 4)).reshape(8, D, D)
    wide = lax.all_gather(inner, BOTH, axis=0, tiled=False)
    wide = wide.reshape(heads + wide.shape[1:])
    full_inner = jnp.transpose(wide, (2, 1, 3, 0, 4)).reshape(2, D, -1)
    tall = lax.all_gather(outer.T, BOTH, axis=0, tiled=False)
    tall = tall.reshape(heads + tall.shape[1:])
    full_outer = jnp.transpose(tall, (0, 2, 1, 3)).reshape(D, -1)
    return full_attention, full_inner, full_outer


def scatter_grads(attention, inner, outer):
    across, within = lax.axis_size("dp"), lax.axis_size("fsdp")
    blocks = attention.reshape(8, across, D // across, within, D // within)
    blocks = jnp.transpose(blocks, (1, 3, 0, 2, 4))
    blocks = blocks.reshape((across * within,) + blocks.shape[2:])
    own_attention = lax.psum_scatter(blocks, BOTH, scatter_dimension=0, tiled=False)
    blocks = inner.reshape(2, within, D // within, across, inner.shape[2] // across)
    blocks = jnp.transpose(blocks, (3, 1, 0, 2, 4))
    blocks = blocks.reshape((across * within,) + blocks.shape[2:])
    own_inner = lax.psum_scatter(blocks, BOTH, scatter_dimension=0, tiled=False)
    blocks = outer.reshape(across, D // across, within, outer.shape[1] // within)
    blocks = jnp.transpose(blocks, (0, 2, 1, 3))
    blocks = blocks.reshape((across * within,) + blocks.shape[2:])
    own_outer = lax.psum_scatter(blocks, BOTH, scatter_dimension=0, tiled=False)
    return (
        jnp.swapaxes(own_attention, 1, 2).astype(f32),
        own_inner.astype(f32),
        own_outer.T.astype(f32),
    )


MESH = pl.DeviceIdType.MESH
RIGHT, LEFT, TO_Y, TO_X, TO_CORE = range(5)


def where_am_i():
    across, within = lax.axis_index("dp"), lax.axis_index("fsdp")
    return across // 2, across % 2, within // 2, within % 2


def device_at(z, y, x, core):
    return (2 * z + y, 2 * x + core)


def aligned(value, unit):
    return pl.multiple_of(value * unit, unit)


class Sizes:
    def __init__(self, down, width, side, deep):
        self.down, self.width, self.side, self.deep = down, width, side, deep
        self.across, self.within = D // down, D // width
        self.depth = self.across // 2
        self.chips = self.across * self.within // 2

    def shard(self, name):
        return {
            "low": (4, self.down, self.width),
            "high": (4, self.down, self.width),
            "inner": (2, self.width, self.side),
            "outer": (self.down, self.deep),
        }[name]

    def owned(self, name):
        if name in ("low", "high"):
            return (4, self.width, self.down)
        return self.shard(name)

    def full(self, name):
        return {
            "low": (4, D, D),
            "high": (4, D, D),
            "inner": (D, 2 * self.across * self.side),
            "outer": (D, self.within * self.deep),
        }[name]

    def piece(self, name):
        return {
            "low": (self.down, 2 * self.width),
            "high": (self.down, 2 * self.width),
            "inner": (self.width, self.side),
            "outer": (self.down // 2, self.deep),
        }[name]

    def part(self, name):
        return {
            "low": (2, self.down, self.width),
            "high": (2, self.down, self.width),
            "inner": (self.width, self.side),
            "outer": (self.down // 2, self.deep),
        }[name]

    def place(self, name, ref, cut, z, y, x, half):
        place = 2 * z + y
        if name == "inner":
            return ref.at[
                pl.ds(aligned(2 * x + cut, self.width), self.width),
                pl.ds(aligned(half * self.across + place, self.side), self.side),
            ]
        if name == "outer":
            return ref.at[
                pl.ds(aligned(2 * place + half, self.down // 2), self.down // 2),
                pl.ds(aligned(2 * x + cut, self.deep), self.deep),
            ]
        return ref.at[
            2 * half + cut,
            pl.ds(aligned(place, self.down), self.down),
            pl.ds(aligned(x, 2 * self.width), 2 * self.width),
        ]

    def share(self, name, ref, half):
        if name == "inner":
            return ref.at[half]
        if name == "outer":
            return ref.at[pl.ds(aligned(half, self.down // 2), self.down // 2)]
        return ref.at[pl.ds(2 * half, 2)]


def greet(depth):
    z, y, x, core = where_am_i()
    barrier = pltpu.get_barrier_semaphore()

    def signal(device):
        pl.semaphore_signal(barrier, inc=1, device_id=device, device_id_type=MESH)

    signal(device_at(z, y, x, 1 - core))
    signal(device_at(z, y, 1 - x, core))
    signal(device_at(z, 1 - y, x, core))
    pl.when(z > 0)(lambda: signal(device_at(z - 1, y, x, core)))
    pl.when(z < depth - 1)(lambda: signal(device_at(z + 1, y, x, core)))
    pl.semaphore_wait(barrier, 3 + jnp.where(z > 0, 1, 0) + jnp.where(z < depth - 1, 1, 0))


def chip_index(bz, by, bx):
    return (2 * bz + by) * 2 + bx


def remote(src, dst, send, recv, device):
    return pltpu.make_async_remote_copy(
        src_ref=src, dst_ref=dst, send_sem=send, recv_sem=recv, device_id=device,
        device_id_type=MESH)


def gather_scratch(sizes, names):
    wave = pltpu.SemaphoreType.DMA
    count, pieces = len(names), 2 * len(names)
    return (
        [pltpu.VMEM((2,) + sizes.piece(name), bf16) for name in names]
        + [pltpu.VMEM(sizes.part(name), bf16) for name in names]
        + [wave((count,)), wave((count,)), wave((pieces,)), wave((pieces, 5, sizes.chips)),
           wave((pieces, 2, sizes.chips))]
    )


def gather_stages(sizes, names, shards, fulls, scratch):
    count, depth = len(names), sizes.depth
    pairs, got = scratch[:count], scratch[count : 2 * count]
    swap_send, swap_recv, own_sem, send_sem, recv_sem = scratch[2 * count :]
    z, y, x, core = where_am_i()
    other = 1 - core
    pieces = [(n, cut) for cut in range(2) for n in range(count)]

    def place(piece, bz, by, bx, half):
        n, cut = pieces[piece]
        return sizes.place(names[n], fulls[n], cut, bz, by, bx, half)

    def swap(n):
        return remote(sizes.share(names[n], shards[n], other), got[n], swap_send.at[n],
                      swap_recv.at[n], device_at(z, y, x, other))

    def merge(n, me):
        if names[n] in ("low", "high"):
            width = sizes.width
            for part, source in ((me, shards[n][2 * me : 2 * me + 2]), (1 - me, got[n][...])):
                pairs[n][:, :, part * width : (part + 1) * width] = source
        else:
            half = sizes.down // 2
            mine = shards[n][me] if names[n] == "inner" else shards[n][me * half : (me + 1) * half]
            pairs[n][me] = mine
            pairs[n][1 - me] = got[n][...]

    def copy(piece, bz, by, bx, kind, own=False):
        target = {
            RIGHT: device_at(z + 1, y, x, core),
            LEFT: device_at(z - 1, y, x, core),
            TO_Y: device_at(z, 1 - y, x, core),
            TO_X: device_at(z, y, 1 - x, core),
            TO_CORE: device_at(z, y, x, other),
        }[kind]
        spot = place(piece, bz, by, bx, core)
        n, cut = pieces[piece]
        slot = chip_index(bz, by, bx)
        return remote(pairs[n].at[cut] if own else spot, spot, send_sem.at[piece, kind, slot],
                      recv_sem.at[piece, 1 if kind == TO_CORE else 0, slot], target)

    def arrive(piece, bz, by, bx, from_core=False):
        spot = place(piece, bz, by, bx, other if from_core else core)
        remote(spot, spot, send_sem.at[piece, 0, 0],
               recv_sem.at[piece, 1 if from_core else 0, chip_index(bz, by, bx)],
               device_at(z, y, x, other)).wait_recv()

    def keep(piece):
        n, cut = pieces[piece]
        return pltpu.make_async_copy(pairs[n].at[cut], place(piece, z, y, x, core),
                                     own_sem.at[piece])

    every = range(len(pieces))
    first, later = every[:count], every[count:]

    def launch(kind):
        for piece in every:
            copy(piece, z, y, x, kind, True).start()

    def begin():
        greet(depth)
        for n in range(count):
            swap(n).start()

    def send_own():
        for n in range(count):
            swap(n).wait_recv()
        for me in range(2):
            @pl.when(core == me)
            def _(me=me):
                for n in range(count):
                    merge(n, me)
        pl.when(z < depth - 1)(lambda: launch(RIGHT))
        pl.when(z > 0)(lambda: launch(LEFT))
        for piece in every:
            copy(piece, z, y, x, TO_Y, True).start()
            copy(piece, z, y, x, TO_X, True).start()
        for piece in every:
            copy(piece, z, y, x, TO_CORE, True).start()
            keep(piece).start()

    def from_z(bz, kind, further):
        for piece in every:
            arrive(piece, bz, y, x)
            pl.when(further)(lambda piece=piece: copy(piece, bz, y, x, kind).start())
            copy(piece, bz, y, x, TO_Y).start()
            copy(piece, bz, y, x, TO_X).start()
            copy(piece, bz, y, x, TO_CORE).start()

    def from_sides(bz):
        for early, late in zip(first, later):
            arrive(early, bz, 1 - y, x)
            copy(early, bz, 1 - y, x, TO_X).start()
            copy(early, bz, 1 - y, x, TO_CORE).start()
            arrive(late, bz, y, 1 - x)
            copy(late, bz, y, 1 - x, TO_Y).start()
            copy(late, bz, y, 1 - x, TO_CORE).start()
        for early, late in zip(first, later):
            arrive(early, bz, y, 1 - x)
            copy(early, bz, y, 1 - x, TO_CORE).start()
            arrive(late, bz, 1 - y, x)
            copy(late, bz, 1 - y, x, TO_CORE).start()

    def from_corner(bz):
        for piece in every:
            arrive(piece, bz, 1 - y, 1 - x)
            copy(piece, bz, 1 - y, 1 - x, TO_CORE).start()

    def both_ways(step, action):
        if step == 0:
            action(z)
            return
        pl.when(z - step >= 0)(lambda: action(z - step))
        pl.when(z + step < depth)(lambda: action(z + step))

    def line(step):
        pl.when(z - step >= 0)(lambda: from_z(z - step, RIGHT, z < depth - 1))
        pl.when(z + step < depth)(lambda: from_z(z + step, LEFT, z > 0))

    def end():
        for n in range(count):
            swap(n).wait_send()
        for piece in every:
            keep(piece).wait()

            @pl.loop(0, depth)
            def _(bz, piece=piece):
                for by in range(2):
                    for bx in range(2):
                        arrive(piece, bz, by, bx, True)
                        copy(piece, bz, by, bx, TO_CORE).wait_send()
                copy(piece, bz, y, x, TO_Y).wait_send()
                copy(piece, bz, y, x, TO_X).wait_send()
                if piece in first:
                    copy(piece, bz, 1 - y, x, TO_X).wait_send()
                else:
                    copy(piece, bz, y, 1 - x, TO_Y).wait_send()
                pl.when((bz <= z) & (z < depth - 1))(
                    lambda: copy(piece, bz, y, x, RIGHT).wait_send())
                pl.when((bz >= z) & (z > 0))(lambda: copy(piece, bz, y, x, LEFT).wait_send())

    timed = [(0, begin), (0, send_own), (12, end)]
    for step in range(1, depth):
        timed.append((2 * step, functools.partial(line, step)))
    for step in range(depth):
        timed.append(((3, 6, 8, 9)[step], functools.partial(both_ways, step, from_sides)))
        timed.append(((10, 10, 11, 11)[step], functools.partial(both_ways, step, from_corner)))
    return sorted(timed, key=lambda item: item[0])


def add_rows(target, sources):
    slab = 48

    def total(k):
        at = pl.ds(aligned(k, slab), slab)
        value = sources[0][at].astype(f32)
        for source in sources[1:]:
            value = value + source[at].astype(f32)
        target[at] = value.astype(target.dtype)

    pl.loop(0, target.shape[0] // slab)(total)


def scatter_scratch(sizes, names):
    wave = pltpu.SemaphoreType.DMA
    count, pieces, depth, chips = len(names), 2 * len(names), sizes.depth, sizes.chips

    def buffers(lead, kind):
        return [pltpu.VMEM(lead + (2,) + sizes.piece(name), kind) for name in names]

    return (
        buffers((chips,), bf16) + buffers((chips,), bf16) + buffers((2 * depth,), bf16)
        + buffers((depth,), bf16) + buffers((2, depth), bf16) + buffers((), f32)
        + [pltpu.VMEM(sizes.part(name), f32) for name in names]
        + [pltpu.VMEM(sizes.part(name), f32) for name in names]
        + [wave((pieces, chips))] * 3 + [wave((pieces, 2 * depth))] * 2
        + [wave((pieces, depth))] * 2 + [wave((pieces, 2, depth))] * 2 + [wave((count,))] * 2
    )


def scatter_stages(sizes, names, fulls, owns, scratch):
    count, depth = len(names), sizes.depth
    acc, swapped, first, second, line, sums, outs, ins = (
        scratch[k * count : (k + 1) * count] for k in range(8)
    )
    (load_sem, swap_send, swap_recv, one_send, one_recv, two_send, two_recv, line_send,
     line_recv, end_send, end_recv) = scratch[8 * count :]
    z, y, x, core = where_am_i()
    other = 1 - core
    partner = device_at(z, y, x, other)
    over_x, over_y = device_at(z, y, 1 - x, core), device_at(z, 1 - y, x, core)
    pieces = [(n, cut) for cut in range(2) for n in range(count)]
    every = range(len(pieces))
    order = sorted(range(depth), key=lambda spot: (-abs(2 * spot - depth + 1), -spot))

    def at(buffers, piece, *index):
        n, cut = pieces[piece]
        return buffers[n].at[(*index, cut)]

    def block(piece, bz, by, bx, half):
        n, cut = pieces[piece]
        return sizes.place(names[n], fulls[n], cut, bz, by, bx, half)

    def load(piece, bz, by, bx):
        slot = chip_index(bz, by, bx)
        return pltpu.make_async_copy(block(piece, bz, by, bx, core), at(acc, piece, slot),
                                     load_sem.at[piece, slot])

    def swap(piece, bz, by, bx):
        slot = chip_index(bz, by, bx)
        return remote(block(piece, bz, by, bx, other), at(swapped, piece, slot),
                      swap_send.at[piece, slot], swap_recv.at[piece, slot], partner)

    def turned(piece):
        return pieces[piece][1] == 1

    def stage_one(piece, bz, spot):
        if turned(piece):
            far, device = chip_index(bz, 1 - y, spot), over_y
        else:
            far, device = chip_index(bz, spot, 1 - x), over_x
        slot = 2 * bz + spot
        return remote(at(acc, piece, far), at(first, piece, slot), one_send.at[piece, slot],
                      one_recv.at[piece, slot], device)

    def stage_two(piece, bz):
        if turned(piece):
            far, device = chip_index(bz, y, 1 - x), over_x
        else:
            far, device = chip_index(bz, 1 - y, x), over_y
        return remote(at(acc, piece, far), at(second, piece, bz), two_send.at[piece, bz],
                      two_recv.at[piece, bz], device)

    def along(piece, bz, way):
        device = device_at(z + 1, y, x, core) if way == 0 else device_at(z - 1, y, x, core)
        return remote(at(acc, piece, chip_index(bz, y, x)), at(line, piece, way, bz),
                      line_send.at[piece, way, bz], line_recv.at[piece, way, bz], device)

    def begin():
        greet(depth)
        for bz in order:
            for flip_y, flip_x in ((1, 1), (0, 1), (1, 0), (0, 0)):
                for piece in every:
                    if turned(piece):
                        flip_y, flip_x = flip_x, flip_y
                    by = 1 - y if flip_y else y
                    bx = 1 - x if flip_x else x
                    swap(piece, bz, by, bx).start()
                    load(piece, bz, by, bx).start()
                    if turned(piece):
                        flip_y, flip_x = flip_x, flip_y

    def join(piece, bz, by, bx, extra=()):
        load(piece, bz, by, bx).wait()
        swap(piece, bz, by, bx).wait_recv()
        mine = at(acc, piece, chip_index(bz, by, bx))
        add_rows(mine, (mine, at(swapped, piece, chip_index(bz, by, bx))) + extra)

    def send_first(bz):
        for far in range(2):
            for piece in every:
                if turned(piece):
                    spot = x if far else 1 - x
                    join(piece, bz, 1 - y, spot)
                else:
                    spot = y if far else 1 - y
                    join(piece, bz, spot, 1 - x)
                stage_one(piece, bz, spot).start()

    def send_second(bz):
        for piece in every:
            spot = 1 - x if turned(piece) else 1 - y
            stage_one(piece, bz, spot).wait_recv()
            arrived = (at(first, piece, 2 * bz + spot),)
            if turned(piece):
                join(piece, bz, y, spot, arrived)
            else:
                join(piece, bz, spot, x, arrived)
            stage_two(piece, bz).start()

    def gathered(piece, bz):
        spot = x if turned(piece) else y
        stage_one(piece, bz, spot).wait_recv()
        stage_two(piece, bz).wait_recv()
        load(piece, bz, y, x).wait()
        swap(piece, bz, y, x).wait_recv()
        mine = at(acc, piece, chip_index(bz, y, x))
        return mine, (mine, at(swapped, piece, chip_index(bz, y, x)),
                      at(first, piece, 2 * bz + spot), at(second, piece, bz))

    def pass_on(bz, level, way):
        for piece in every:
            mine, base = gathered(piece, bz)
            if level > 0:
                along(piece, bz, way).wait_recv()
                base = base + (at(line, piece, way, bz),)
            add_rows(mine, base)
            along(piece, bz, way).start()

    def pass_level(bz, level):
        if level < bz:
            pl.when(z == level)(lambda: pass_on(bz, level, 0))
        if depth - 1 - level > bz:
            pl.when(z == depth - 1 - level)(lambda: pass_on(bz, level, 1))

    def finish(bz):
        @pl.when(z == bz)
        def _():
            ways = ((0,) if bz > 0 else ()) + ((1,) if bz < depth - 1 else ())
            for piece in every:
                n, cut = pieces[piece]
                _, base = gathered(piece, bz)
                for way in ways:
                    along(piece, bz, way).wait_recv()
                add_rows(sums[n].at[cut], base + tuple(at(line, piece, way, bz) for way in ways))

    def exchange(n):
        return remote(outs[n], ins[n], end_send.at[n], end_recv.at[n], partner)

    width, half = sizes.width, sizes.down // 2

    def hand_over():
        for me in range(2):
            @pl.when(core == me)
            def _(me=me):
                far = 1 - me
                for n, name in enumerate(names):
                    if name == "inner":
                        outs[n][...] = sums[n][far]
                        owns[n][me] = sums[n][me]
                    elif name == "outer":
                        outs[n][...] = sums[n][far]
                        owns[n][me * half : (me + 1) * half] = sums[n][me]
                    else:
                        outs[n][...] = sums[n][:, :, far * width : (far + 1) * width]
                        for k in range(2):
                            mine = sums[n][k, :, me * width : (me + 1) * width]
                            owns[n][2 * me + k] = mine.T
        for n in range(count):
            exchange(n).start()

    def end():
        for n in range(count):
            exchange(n).wait_recv()
        for me in range(2):
            @pl.when(core == me)
            def _(me=me):
                far = 1 - me
                for n, name in enumerate(names):
                    if name == "inner":
                        owns[n][far] = ins[n][...]
                    elif name == "outer":
                        owns[n][far * half : (far + 1) * half] = ins[n][...]
                    else:
                        for k in range(2):
                            owns[n][2 * far + k] = ins[n][k].T
        for n in range(count):
            exchange(n).wait_send()
        for piece in every:
            @pl.loop(0, depth)
            def _(bz, piece=piece):
                for by in range(2):
                    for bx in range(2):
                        swap(piece, bz, by, bx).wait_send()
                for spot in range(2):
                    stage_one(piece, bz, spot).wait_send()
                stage_two(piece, bz).wait_send()
                pl.when(z < bz)(lambda: along(piece, bz, 0).wait_send())
                pl.when(z > bz)(lambda: along(piece, bz, 1).wait_send())

    timed = [(0, begin)]
    for turn, bz in enumerate(order):
        timed.append((turn, functools.partial(send_first, bz)))
        timed.append(((2, 4, 5, 7)[turn], functools.partial(send_second, bz)))
        for level in range(depth - 1):
            when = ((4, 6, 8), (8, 10, 12), (9, 11, 12), (9, 12, 12))[turn][level]
            timed.append((when, functools.partial(pass_level, bz, level)))
    ending = [functools.partial(finish, bz) for bz in order] + [hand_over, end]
    timed.append((13, functools.partial(in_turn, ending)))
    return sorted(timed, key=lambda item: item[0])


def in_turn(actions):
    for action in actions:
        action()


def run_stages(timed, step, number, steps):
    mine = [stage for time, stage in timed if time < 12 and time * steps // 12 == number]
    if mine:
        pl.when(step == number)(functools.partial(in_turn, mine))


HBM = pl.BlockSpec(memory_space=pl.ANY)
VMEM = pl.BlockSpec(memory_space=pltpu.VMEM)


def gather_kernel(sizes, names, *refs):
    count = len(names)
    gain_ref, gain_out, send, recv = refs[count], refs[2 * count + 1], *refs[-2:]
    stages = gather_stages(sizes, names, refs[:count], refs[count + 1 : 2 * count + 1],
                           refs[2 * count + 2 : -2])
    z, y, x, core = where_am_i()
    mine, near = 2 * x + core, 2 * x + 1 - core
    far, corner = 2 * (1 - x) + core, 2 * (1 - x) + 1 - core

    def pass_gain(src, slot, kind, device):
        return remote(src, gain_out.at[slot], send.at[kind], recv.at[kind], device)

    partner, beside = device_at(z, y, x, 1 - core), device_at(z, y, 1 - x, core)
    hops = (
        (gain_ref, mine, 0, partner),
        (gain_ref, mine, 1, beside),
        (gain_out.at[near], near, 2, beside),
    )
    stages = [stage for _, stage in stages]
    stages[0]()
    gain_out[mine] = gain_ref[...]
    pass_gain(*hops[0]).start()
    pass_gain(*hops[1]).start()
    stages[1]()
    pass_gain(gain_ref, near, 0, partner).wait_recv()
    pass_gain(*hops[2]).start()
    for stage in stages[2:]:
        stage()
    pass_gain(gain_ref, far, 1, beside).wait_recv()
    pass_gain(gain_ref, corner, 2, beside).wait_recv()
    for hop in hops:
        pass_gain(*hop).wait_send()


def gather_blocks(sizes, names, shards, gain):
    wave = pltpu.SemaphoreType.DMA
    return pl.pallas_call(
        functools.partial(gather_kernel, sizes, names),
        out_shape=[jax.ShapeDtypeStruct(sizes.full(name), bf16) for name in names]
        + [jax.ShapeDtypeStruct((sizes.within,) + gain.shape, f32)],
        in_specs=[VMEM] * (len(names) + 1),
        out_specs=[HBM] * len(names) + [VMEM],
        scratch_shapes=gather_scratch(sizes, names) + [wave((3,)), wave((3,))],
        compiler_params=pltpu.CompilerParams(collective_id=0, has_side_effects=True),
        name="gather_blocks",
    )(*shards, gain)


def gain_stages(depth, gain_ref, gain_out, buf, send, recv):
    z, y, x, core = where_am_i()
    hops = (device_at(z, y, x, 1 - core), device_at(z, y, 1 - x, core),
            device_at(z, 1 - y, x, core))

    def hop(step):
        return remote(buf.at[2 * step], buf.at[2 * step + 1], send.at[step], recv.at[step],
                      hops[step])

    def line(way):
        device = device_at(z + 1, y, x, core) if way == 0 else device_at(z - 1, y, x, core)
        return remote(buf.at[7 + way], buf.at[9 + way], send.at[3 + way], recv.at[3 + way],
                      device)

    def begin():
        buf[0] = gain_ref[...]
        hop(0).start()

    def turn(step):
        hop(step).wait_recv()
        buf[2 * step + 2] = buf[2 * step] + buf[2 * step + 1]
        if step < 2:
            hop(step + 1).start()

    def rightward():
        gain_out[...] = buf[6]

        @pl.when(z > 0)
        def _():
            line(0).wait_recv()
            gain_out[...] = gain_out[...] + buf[9]

        @pl.when(z < depth - 1)
        def _():
            buf[7] = gain_out[...]
            line(0).start()

    def leftward():
        buf[8] = buf[6]

        @pl.when(z < depth - 1)
        def _():
            line(1).wait_recv()
            gain_out[...] = gain_out[...] + buf[10]
            buf[8] = buf[6] + buf[10]

        pl.when(z > 0)(lambda: line(1).start())

    def end():
        for step in range(3):
            hop(step).wait_send()
        pl.when(z < depth - 1)(lambda: line(0).wait_send())
        pl.when(z > 0)(lambda: line(1).wait_send())

    return [begin] + [functools.partial(turn, step) for step in range(3)] + [
        rightward, leftward, end]


def scatter_kernel(sizes, names, k_ref, v_ref, wk_ref, wv_ref, *refs):
    count = len(names)
    fulls, gain_ref, grad_ref = refs[:count], refs[count], refs[count + 1]
    own_ref, gain_out = refs[count + 2 : count + 4]
    owns = [own_ref.at[pl.ds(4 * n, 4)] for n in range(count)]
    gain_scratch, scratch = refs[count + 4 : count + 7], refs[count + 7 :]
    stages = scatter_stages(sizes, names, fulls, owns, scratch)
    gains = gain_stages(sizes.depth, gain_ref, gain_out, *gain_scratch)
    joined = [(0, stages[0][1])]
    for number, (_, stage) in enumerate(stages[1:]):
        both = functools.partial(in_turn, [stage] + gains[number : number + 1])
        joined.append((12 * (number + 1) / len(stages), both))
    steps = pl.num_programs(0)
    for number in range(steps):
        run_stages(joined, pl.program_id(0), number, steps)
    grad_ref[...] = dot_nn(k_ref[...], wk_ref[0]) + dot_nn(v_ref[...], wv_ref[0])


def scatter_blocks(sizes, names, fulls, gains, grad_key, grad_value, projections):
    wave = pltpu.SemaphoreType.DMA
    slab = 256
    rows = pl.BlockSpec((slab, D), lambda step: (step, 0))

    def matrix(which):
        return pl.BlockSpec((1, D, D), lambda step: (which, 0, 0))

    return pl.pallas_call(
        functools.partial(scatter_kernel, sizes, names),
        grid=(grad_key.shape[0] // slab,),
        out_shape=[jax.ShapeDtypeStruct(grad_key.shape, f32)]
        + [jax.ShapeDtypeStruct((4 * len(names),) + sizes.owned("low")[1:], f32)]
        + [jax.ShapeDtypeStruct(gains.shape, f32)],
        in_specs=[rows, rows, matrix(1), matrix(2)] + [HBM] * len(names) + [VMEM],
        out_specs=[rows, VMEM, VMEM],
        scratch_shapes=[pltpu.VMEM((11,) + gains.shape, f32), wave((5,)), wave((5,))]
        + scatter_scratch(sizes, names),
        compiler_params=pltpu.CompilerParams(
            collective_id=1, has_side_effects=True, vmem_limit_bytes=60 * 1024 * 1024
        ),
        name="scatter_blocks",
    )(grad_key, grad_value, projections, projections, *fulls, gains)


def tile_aligned(down, width, side, deep):
    return (
        lax.axis_size("fsdp") == 4
        and lax.axis_size("dp") in (2, 4, 8)
        and down % 96 == 0
        and width % 48 == 0
        and (2 * width) % 128 == 0
        and side % 128 == 0
        and deep % 128 == 0
    )


def adam_update(weight, mean_old, square_old, gradient, step_rate, decay_rate):
    mean_new = beta_one * mean_old + (1.0 - beta_one) * gradient
    square_new = beta_two * square_old + (1.0 - beta_two) * gradient * gradient
    corrected = (
        mean_new
        / (1.0 - beta_one**STEP)
        / (jnp.sqrt(square_new / (1.0 - beta_two**STEP)) + adam_epsilon)
    )
    master = weight - step_rate * (corrected + decay_rate * weight)
    return (mean_new, square_new, master, master.astype(bf16))


def on_device(
    hidden_in,
    patches,
    token_segments,
    patch_segments,
    cotangent,
    attention_weights,
    attention_means,
    attention_squares,
    inner_weights,
    inner_means,
    inner_squares,
    outer_weights,
    outer_means,
    outer_squares,
    norm_gains,
    gain_means,
    gain_squares,
):
    rows, _, length, _ = hidden_in.shape
    count = patches.shape[2]
    tokens = rows * length
    width, down = attention_weights.shape[1:]
    side, deep = inner_weights.shape[2], outer_weights.shape[0]
    direct = tile_aligned(down, width, side, deep)
    low_inner, low_outer = inner_weights.astype(bf16), outer_weights.astype(bf16)
    if direct:
        sizes = Sizes(down, width, side, deep)
        turned = jnp.swapaxes(attention_weights, 1, 2).astype(bf16)
        parts = norm_gains.shape[1]
        gain_block = jnp.pad(
            norm_gains.astype(bf16).astype(f32), ((0, 8 - norm_gains.shape[0]), (0, -parts % 128))
        )
        low, high, gains = gather_blocks(
            sizes, ("low", "high"), (turned[:4], turned[4:]), gain_block
        )
        gains = jnp.swapaxes(gains[:, : norm_gains.shape[0], :parts], 0, 1).reshape(-1, D)
        rest, rest_shards = ("inner", "outer"), (low_inner, low_outer.T)
    else:
        sizes = None
        gains = lax.all_gather(norm_gains.astype(bf16), "fsdp", axis=1, tiled=True)
        weights, inner, outer = gather_weights(
            attention_weights.astype(bf16), low_inner, low_outer
        )
        low, high = weights[:4], weights[4:]
        inner = jnp.concatenate([inner[0], inner[1]], axis=1)
        rest, rest_shards = (), ()

    initial = hidden_in.reshape(tokens, D).astype(f32)
    token_rows = token_segments.reshape(rows, 1, length)
    token_columns = token_segments.reshape(rows, length, 1)
    patch_ids = patch_segments.reshape(rows, 1, count)

    normed_one, unit_one, rms_one = norm_forward(initial, gains[0])
    stacked = low.reshape(4 * D, D)
    packed = dot_nt(normed_one, stacked).astype(bf16).reshape(rows, length, 4 * D)
    mixture_one, lse_one = self_forward(packed, token_rows, token_columns)
    mixed_one = mixture_one.reshape(tokens, D)
    after_one = initial + dot_nt(mixed_one, low[3])
    normed_two, unit_two, rms_two = norm_forward(after_one, gains[1])
    cross_query = dot_nt(normed_two, high[0]).astype(bf16).reshape(rows, length, D)
    mixture_two, lse_two, cross_key, cross_value, *arrived = cross_forward(
        Rider(sizes, rest, "gather", 2, rows * PAIRS), cross_query, patches.reshape(rows, count, D), high,
        token_columns, patch_ids, rest_shards,
    )
    if direct:
        inner, outer = arrived
    mixed_two = mixture_two.reshape(tokens, D)
    after_two = after_one + dot_nt(mixed_two, high[3])
    normed_three, unit_three, rms_three = norm_forward(after_two, gains[2])
    gated = dot_nn(normed_three, inner)
    hidden_units = outer.shape[1]
    gate, up = gated[:, :hidden_units], gated[:, hidden_units:]
    units = (gelu_tanh(gate) * up).astype(bf16)
    hidden_out = (after_two + dot_nt(units, outer)).astype(bf16)

    grad_low = cotangent.reshape(tokens, D)
    grad_final = grad_low.astype(f32)
    grad_outer = dot_tn(grad_low, units).astype(bf16)
    grad_units = dot_nn(grad_low, outer)
    activation, gelu_back = jax.vjp(gelu_tanh, gate)
    grad_gated = jnp.concatenate(
        [gelu_back(grad_units * up)[0], grad_units * activation], axis=1
    ).astype(bf16)
    grad_inner = dot_tn(normed_three, grad_gated).astype(bf16)
    grad_normed = dot_nt(grad_gated, inner)
    grad_from_three, gain_three = norm_backward(grad_normed, gains[2], unit_three, rms_three)
    grad_two = grad_final + grad_from_three
    branch_two = grad_two.astype(bf16)
    grad_mixture_two = dot_nn(branch_two, high[3]).astype(bf16).reshape(rows, length, D)
    grad_cq, grad_ck, grad_cv, grad_pair, *summed_rest = cross_backward(
        Rider(sizes, rest, "scatter", 3, rows * PAIRS), cross_query, cross_key, cross_value,
        mixture_two, grad_mixture_two, lse_two, token_columns, patch_ids,
        patches.reshape(rows, count, D), (grad_inner, grad_outer) if direct else (),
    )
    grad_cq = grad_cq.reshape(tokens, D)
    grad_ck = grad_ck.reshape(rows * count, D)
    grad_cv = grad_cv.reshape(rows * count, D)
    grad_high = grad_pair.at[0].set(dot_tn(grad_cq, normed_two).astype(bf16))
    grad_high = grad_high.at[3].set(dot_tn(branch_two, mixed_two).astype(bf16))
    grad_from_two, gain_two = norm_backward(
        dot_nn(grad_cq, high[0]), gains[1], unit_two, rms_two
    )
    grad_one = grad_two + grad_from_two
    branch_one = grad_one.astype(bf16)
    grad_mixture_one = dot_nn(branch_one, low[3]).astype(bf16).reshape(rows, length, D)
    grad_packed = self_backward(
        packed, mixture_one, grad_mixture_one, lse_one, token_rows, token_columns
    ).reshape(tokens, 4 * D)
    grad_normed_one = dot_nn(grad_packed, stacked)
    grad_from_one, gain_one = norm_backward(grad_normed_one, gains[0], unit_one, rms_one)
    hidden_grad = grad_one + grad_from_one
    grad_first = dot_tn(grad_packed, normed_one).astype(bf16).reshape(4, D, D)
    grad_first = grad_first.at[3].set(dot_tn(branch_one, mixed_one).astype(bf16))
    gain_grads = jnp.stack([gain_one, gain_two, gain_three])
    if direct:
        own_inner, own_outer = summed_rest
        patch_grad, own_attention, gain_totals = scatter_blocks(
            sizes, ("low", "high"), (grad_first, grad_high),
            jnp.pad(gain_grads, ((0, 5), (0, 0))), grad_ck, grad_cv, high,
        )
        own_outer = own_outer.T
        gain_totals = gain_totals[:3]
    else:
        patch_grad = dot_nn(grad_ck, high[1]) + dot_nn(grad_cv, high[2])
        own_attention, own_inner, own_outer = scatter_grads(
            jnp.concatenate([grad_first, grad_high]),
            jnp.stack([grad_inner[:, :hidden_units], grad_inner[:, hidden_units:]]),
            grad_outer,
        )
        gain_totals = lax.psum(gain_grads, BOTH)
    width = norm_gains.shape[1]
    own_gains = lax.dynamic_slice_in_dim(
        gain_totals, lax.axis_index("fsdp") * width, width, axis=1
    )

    attention_new = adam_update(
        attention_weights, attention_means, attention_squares, own_attention,
        rate_matrix, decay_matrix,
    )
    inner_new = adam_update(
        inner_weights, inner_means, inner_squares, own_inner, rate_matrix, decay_matrix
    )
    outer_new = adam_update(
        outer_weights, outer_means, outer_squares, own_outer, rate_matrix, decay_matrix
    )
    gain_new = adam_update(norm_gains, gain_means, gain_squares, own_gains, rate_gain, 0.0)
    return (
        hidden_out.reshape(hidden_in.shape),
        hidden_grad.reshape(hidden_in.shape),
        patch_grad.reshape(patches.shape),
        *attention_new,
        *inner_new,
        *outer_new,
        *gain_new,
    )


def solution(mesh):
    rows = P(None, BOTH, None, None)
    ids = P(None, BOTH, None)
    matrix = P(None, "fsdp", "dp")
    down = P("fsdp", "dp")
    gain = P(None, "fsdp")
    return jax.shard_map(
        on_device,
        mesh=mesh,
        in_specs=(rows, rows, ids, ids, rows) + (matrix,) * 6 + (down,) * 3 + (gain,) * 3,
        out_specs=(rows, rows, rows) + (matrix,) * 8 + (down,) * 4 + (gain,) * 4,
        check_vma=False,
    )
```
